64 devices in a mesh: dp: 4 (over x, y), fsdp: 16 (over z, core).
Axes of the slice: x: 2, y: 2, z: 8, core: 2. Of those that a mesh axis runs over, the one named last changes fastest.
The devices are a block of a 4x4x8 slice.
Arguments:
- tokens: int32 [64, 128], P(('dp', 'fsdp')), parts along dimension 0
- embed_table: bfloat16 [128256, 2048], P('fsdp')
- norm_attn: bfloat16 [2048], P('fsdp')
- w_qkv: bfloat16 [2048, 3072], P('fsdp')
- w_out: bfloat16 [2048, 2048], P('fsdp')
- norm_mlp: bfloat16 [2048], P('fsdp')
- w_gate_up: bfloat16 [2048, 16384], P('fsdp')
- w_down: bfloat16 [8192, 2048], P('fsdp')
- rope_scale: float32 [32], replicated
Outputs:
- output 1: bfloat16 [64, 128, 2048], P(('dp', 'fsdp')), parts along dimension 0
- output 2: bfloat16 [64, 128, 8, 64], P(('dp', 'fsdp')), parts along dimension 0
- output 3: bfloat16 [64, 128, 8, 64], P(('dp', 'fsdp')), parts along dimension 0
There are 4 independent parts. The reference program is written for one: setup_inputs(seed, part) draws one part's arguments, and reference() takes and returns one part's arrays. A program takes and returns all parts, laid end to end along the dimension named above; an argument that names none is the same for every part.
All inputs are finite; a program needn't handle non-finite values.
Results may differ from the reference program's by a relative error of at most 0.0117517.
Values are sent between devices in bfloat16 or wider.
A program may use at most 768 MiB of HBM per device.

```python
import jax
import jax.numpy as jnp
from jax import lax

BATCH = 16
SEQ = 128
D = 2048
HEADS = 32
KV_HEADS = 8
HEAD = 64
FF = 8192
VOCAB = 128256

Q_WIDTH = HEADS * HEAD
KV_WIDTH = KV_HEADS * HEAD
HEAD_GROUP = HEADS // KV_HEADS
HALF_DIM = HEAD // 2
NORM_EPS = 1e-5
ROPE_THETA = 10000.0


def draw_tokens(tok_key):
    level_key, id_key = jax.random.split(tok_key)
    tok_level = jax.random.randint(level_key, (BATCH, SEQ), 0, 4)
    id_limit = VOCAB // jnp.power(8, tok_level)
    tokens = jax.random.randint(id_key, (BATCH, SEQ), 0, id_limit)
    return tokens.at[0, 0].set(VOCAB - 1).astype(jnp.int32)


def setup_inputs(seed: int = 0, part: int = 0) -> dict:
    base_key = jax.random.key(seed)
    sub_keys = jax.random.split(base_key, 9)
    tokens = draw_tokens(jax.random.fold_in(sub_keys[0], part))
    embed_table = jax.random.normal(sub_keys[1], (VOCAB, D), jnp.float32)
    norm_attn = 1.0 + 0.3 * jax.random.normal(sub_keys[2], (D,), jnp.float32)
    w_qkv = 1.5 * D ** -0.5 * jax.random.normal(sub_keys[3], (D, Q_WIDTH + 2 * KV_WIDTH), jnp.float32)
    w_out = Q_WIDTH ** -0.5 * jax.random.normal(sub_keys[4], (Q_WIDTH, D), jnp.float32)
    norm_mlp = 1.0 + 0.3 * jax.random.normal(sub_keys[5], (D,), jnp.float32)
    w_gate_up = D ** -0.5 * jax.random.normal(sub_keys[6], (D, 2 * FF), jnp.float32)
    w_down = FF ** -0.5 * jax.random.normal(sub_keys[7], (FF, D), jnp.float32)
    rope_scale = jax.random.uniform(sub_keys[8], (HALF_DIM,), jnp.float32, 1.0, 4.0)
    return {
        'tokens': tokens,
        'embed_table': embed_table.astype(jnp.bfloat16),
        'norm_attn': norm_attn.astype(jnp.bfloat16),
        'w_qkv': w_qkv.astype(jnp.bfloat16),
        'w_out': w_out.astype(jnp.bfloat16),
        'norm_mlp': norm_mlp.astype(jnp.bfloat16),
        'w_gate_up': w_gate_up.astype(jnp.bfloat16),
        'w_down': w_down.astype(jnp.bfloat16),
        'rope_scale': rope_scale,
    }


def rms_norm(hidden, gain):
    h_f32 = hidden.astype(jnp.float32)
    inv_rms = lax.rsqrt(jnp.mean(h_f32 * h_f32, axis=-1, keepdims=True) + NORM_EPS)
    return (h_f32 * inv_rms * gain.astype(jnp.float32)).astype(jnp.bfloat16)


def reference(tokens, embed_table, norm_attn, w_qkv, w_out, norm_mlp, w_gate_up, w_down, rope_scale):
    freq_expo = jnp.arange(HALF_DIM, dtype=jnp.float32) * (2.0 / HEAD)
    inv_freq = 1.0 / (rope_scale * jnp.power(ROPE_THETA, freq_expo))
    angles = jnp.arange(SEQ, dtype=jnp.float32)[:, None] * inv_freq[None, :]
    cos_tab = jnp.cos(angles)[:, None, :]
    sin_tab = jnp.sin(angles)[:, None, :]
    causal = jnp.arange(SEQ)[:, None] >= jnp.arange(SEQ)[None, :]

    def rotate(proj):
        low_half = proj[..., :HALF_DIM]
        high_half = proj[..., HALF_DIM:]
        return jnp.concatenate([low_half * cos_tab - high_half * sin_tab, high_half * cos_tab + low_half * sin_tab], axis=-1)

    def one_sequence(seq_tokens):
        hidden = jnp.take(embed_table, seq_tokens, axis=0)
        normed = rms_norm(hidden, norm_attn)
        qkv_proj = jnp.dot(normed, w_qkv, preferred_element_type=jnp.float32)
        query_rot = rotate(qkv_proj[:, :Q_WIDTH].reshape(SEQ, HEADS, HEAD)).astype(jnp.bfloat16)
        key_rot = rotate(qkv_proj[:, Q_WIDTH:Q_WIDTH + KV_WIDTH].reshape(SEQ, KV_HEADS, HEAD)).astype(jnp.bfloat16)
        values = qkv_proj[:, Q_WIDTH + KV_WIDTH:].reshape(SEQ, KV_HEADS, HEAD).astype(jnp.bfloat16)
        q_grouped = query_rot.reshape(SEQ, KV_HEADS, HEAD_GROUP, HEAD)
        scores = jnp.einsum('qkgd,skd->kgqs', q_grouped.astype(jnp.float32), key_rot.astype(jnp.float32)) * (HEAD ** -0.5)
        scores = jnp.where(causal, scores, -jnp.inf)
        scores = scores - jnp.max(scores, axis=-1, keepdims=True)
        weights = jnp.exp(scores)
        attn_probs = (weights / jnp.sum(weights, axis=-1, keepdims=True)).astype(jnp.bfloat16)
        context = jnp.einsum('kgqs,skd->qkgd', attn_probs.astype(jnp.float32), values.astype(jnp.float32))
        context = context.astype(jnp.bfloat16).reshape(SEQ, Q_WIDTH)
        attn_proj = jnp.dot(context, w_out, preferred_element_type=jnp.float32)
        resid_mid = (hidden.astype(jnp.float32) + attn_proj).astype(jnp.bfloat16)
        normed_mlp = rms_norm(resid_mid, norm_mlp)
        gate_up = jnp.dot(normed_mlp, w_gate_up, preferred_element_type=jnp.float32)
        mlp_act = (jax.nn.silu(gate_up[:, :FF]) * gate_up[:, FF:]).astype(jnp.bfloat16)
        down_proj = jnp.dot(mlp_act, w_down, preferred_element_type=jnp.float32)
        layer_out = (resid_mid.astype(jnp.float32) + down_proj).astype(jnp.bfloat16)
        return layer_out, key_rot, values

    hidden_out, key_cache, value_cache = lax.map(one_sequence, tokens)
    return hidden_out, key_cache, value_cache
```

```python
import functools
import math

import jax
import jax.numpy as jnp
from jax import lax
from jax.experimental import pallas as pl
from jax.experimental.pallas import tpu as pltpu
from jax.sharding import PartitionSpec as P

NORM_EPS = 1e-5
ROPE_THETA = 10000.0
BATCH = 32
DEPTH = 4


def gather_kernel(n_tok, gid_ref, tgt_ref, table_ref, out_ref, buf, obuf, sems, osem):
    width = table_ref.shape[2]
    n_step = n_tok // BATCH

    def fetch(step, slot):
        def one(i, carry):
            g = gid_ref[step * BATCH + i]

            @pl.when(g >= 0)
            def _():
                pltpu.make_async_copy(table_ref.at[g], buf.at[slot, i], sems.at[slot]).start()
            return carry
        lax.fori_loop(0, BATCH, one, 0, unroll=8)

    def drain(step, slot):
        def one(i, carry):
            @pl.when(gid_ref[step * BATCH + i] >= 0)
            def _():
                pltpu.make_async_copy(table_ref.at[0], buf.at[slot, 0], sems.at[slot]).wait()
            return carry
        lax.fori_loop(0, BATCH, one, 0, unroll=8)

    buf[...] = jnp.zeros_like(buf)
    for j in range(DEPTH - 1):
        fetch(j, j)

    def body(step, carry):
        slot = lax.rem(step, DEPTH)

        @pl.when(step + DEPTH - 1 < n_step)
        def _():
            fetch(step + DEPTH - 1, lax.rem(step + DEPTH - 1, DEPTH))
        drain(step, slot)
        rows = pl.ds(pl.multiple_of(step * BATCH, BATCH), BATCH)
        pick = (lax.broadcasted_iota(jnp.int32, (BATCH, BATCH * 8), 1) == tgt_ref[rows, :]).astype(jnp.bfloat16)
        block = buf[slot].reshape(BATCH * 8, width)
        got = jnp.dot(pick, block, preferred_element_type=jnp.float32)
        out_ref[rows, :] = got.astype(jnp.bfloat16)
        return carry
    lax.fori_loop(0, n_step, body, 0)


def gather_table(ids, owned, table):
    n_tok = ids.shape[0]
    n_rows, width = table.shape
    gid = jnp.where(owned, ids // 8, -1)
    lane = jnp.arange(n_tok, dtype=jnp.int32) % BATCH
    tgt = jnp.where(owned, 8 * lane + ids % 8, -1)[:, None]
    return pl.pallas_call(
        functools.partial(gather_kernel, n_tok),
        out_shape=jax.ShapeDtypeStruct((n_tok, width), jnp.bfloat16),
        in_specs=[pl.BlockSpec(memory_space=pltpu.SMEM), pl.BlockSpec(memory_space=pltpu.VMEM), pl.BlockSpec(memory_space=pl.ANY)],
        out_specs=pl.BlockSpec(memory_space=pltpu.VMEM),
        scratch_shapes=[
            pltpu.VMEM((DEPTH, BATCH, 8, width), jnp.bfloat16),
            pltpu.VMEM((8, 128), jnp.bfloat16),
            pltpu.SemaphoreType.DMA((DEPTH,)),
            pltpu.SemaphoreType.DMA,
        ],
        compiler_params=pltpu.CompilerParams(vmem_limit_bytes=48 * 2**20),
        cost_estimate=pl.CostEstimate(flops=2 * n_tok * BATCH * 8 * width, bytes_accessed=9 * n_tok * width * 2, transcendentals=0),
    )(gid, tgt, table.reshape(n_rows // 8, 8, width))


def rope_tables(seq_len, rope_scale):
    half_dim = rope_scale.shape[0]
    freq_expo = jnp.arange(half_dim, dtype=jnp.float32) * (1.0 / half_dim)
    inv_freq = 1.0 / (rope_scale * jnp.power(ROPE_THETA, freq_expo))
    angles = jnp.arange(seq_len, dtype=jnp.float32)[:, None] * inv_freq[None, :]
    return jnp.cos(angles)[:, None, :], jnp.sin(angles)[:, None, :]


def rotate(proj, cos_tab, sin_tab):
    half_dim = cos_tab.shape[-1]
    low_half = proj[..., :half_dim]
    high_half = proj[..., half_dim:]
    return jnp.concatenate([low_half * cos_tab - high_half * sin_tab, high_half * cos_tab + low_half * sin_tab], axis=-1)


def solution(mesh):
    batch_axes = ('dp', 'fsdp')
    row_spec = P('fsdp', None)
    n_dp = mesh.shape['dp']
    side = math.isqrt(n_dp)
    flip_y = [(i, i ^ 1) for i in range(n_dp)]
    flip_x = [(i, ((i // side) ^ 1) * side + i % side) for i in range(n_dp)]

    def device_step(tokens, embed_table, norm_attn, w_qkv, w_out, norm_mlp, w_gate_up, w_down, rope_scale):
        dp = lax.axis_index('dp')
        me_x = (dp // side) % 2
        me_y = dp % 2
        me = 2 * me_x + me_y
        n_fsdp = mesh.shape['fsdp']
        seq_len = tokens.shape[1]
        width = embed_table.shape[1]
        head_dim = 2 * rope_scale.shape[0]
        q_width = w_out.shape[0] * n_fsdp
        kv_width = (w_qkv.shape[1] - q_width) // 2
        ff_part = w_down.shape[0]
        q4, kv4, w4, f4 = q_width // 4, kv_width // 4, width // 4, ff_part // 4
        n_tok = 4 * seq_len

        def send_x(a):
            return lax.ppermute(a, 'dp', flip_x)

        def send_y(a):
            return lax.ppermute(a, 'dp', flip_y)

        def by_role(mine, dx, dy, dxy):
            stack = jnp.stack([mine, dy, dx, dxy])
            return stack[jnp.arange(4) ^ me]

        def square_gather(a):
            half = a.shape[0] // 2
            top, bot = a[:half], a[half:]
            top_x, bot_y = send_x(top), send_y(bot)
            top2 = send_y(jnp.concatenate([top, top_x]))
            bot2 = send_x(jnp.concatenate([bot, bot_y]))
            dx = jnp.concatenate([top_x, bot2[:half]])
            dy = jnp.concatenate([top2[:half], bot_y])
            dxy = jnp.concatenate([top2[half:], bot2[half:]])
            return by_role(a, dx, dy, dxy)

        def square_scatter(parts):
            half = parts.shape[1] // 2
            ex = parts[jnp.arange(4) ^ me]
            top, bot = ex[:, :half], ex[:, half:]
            top_r = send_x(top[2:])
            bot_r = send_y(bot[jnp.array([1, 3])])
            top1 = top[:2] + top_r
            bot1 = bot[jnp.array([0, 2])] + bot_r
            top2 = top1[0] + send_y(top1[1])
            bot2 = bot1[0] + send_x(bot1[1])
            return jnp.concatenate([top2, bot2])

        def gather_rows(weight):
            return lax.all_gather(weight, 'fsdp', axis=0, tiled=True)

        wqkv_part = jnp.concatenate([
            lax.dynamic_slice_in_dim(w_qkv, me * q4, q4, 1),
            lax.dynamic_slice_in_dim(w_qkv, q_width + me * kv4, kv4, 1),
            lax.dynamic_slice_in_dim(w_qkv, q_width + kv_width + me * kv4, kv4, 1)], axis=1)
        full_qkv = gather_rows(wqkv_part)
        full_out = gather_rows(lax.dynamic_slice_in_dim(w_out, me * w4, w4, 1))
        gains = jnp.concatenate([norm_attn[None], norm_mlp[None]])
        gains = lax.all_gather(gains, 'fsdp', axis=1, tiled=True)
        gain_attn, gain_mlp = gains[0].astype(jnp.float32), gains[1].astype(jnp.float32)

        group_tokens = lax.all_gather(tokens, 'fsdp', axis=0, tiled=True).reshape(-1)
        shard_rows = embed_table.shape[0]
        local_ids = group_tokens - lax.axis_index('fsdp') * shard_rows
        owned = (local_ids >= 0) & (local_ids < shard_rows)
        rows = gather_table(local_ids, owned, embed_table)
        hidden = lax.psum_scatter(rows.reshape(n_fsdp, seq_len, width), 'fsdp', scatter_dimension=0, tiled=False)

        gu = w_gate_up.reshape(w_gate_up.shape[0], 2 * n_fsdp, 4, f4)
        gu = lax.dynamic_index_in_dim(gu, me, 2, keepdims=False).reshape(w_gate_up.shape[0], 2 * n_fsdp * f4)
        full_gate_up = gather_rows(gu)
        full_down = gather_rows(lax.dynamic_slice_in_dim(w_down, me * f4, f4, 0))

        x_all = square_gather(hidden).reshape(n_tok, width)
        x_f32 = x_all.astype(jnp.float32)
        inv = lax.rsqrt(jnp.mean(x_f32 * x_f32, axis=-1, keepdims=True) + NORM_EPS)
        normed = (x_f32 * inv * gain_attn).astype(jnp.bfloat16)
        qkv = jnp.dot(normed, full_qkv, preferred_element_type=jnp.float32).reshape(4, seq_len, -1)
        cos_tab, sin_tab = rope_tables(seq_len, rope_scale)
        n_q, n_kv = q4 // head_dim, kv4 // head_dim
        q = rotate(qkv[..., :q4].reshape(4, seq_len, n_q, head_dim), cos_tab, sin_tab).astype(jnp.bfloat16)
        k = rotate(qkv[..., q4:q4 + kv4].reshape(4, seq_len, n_kv, head_dim), cos_tab, sin_tab).astype(jnp.bfloat16)
        v = qkv[..., q4 + kv4:].reshape(4, seq_len, n_kv, head_dim).astype(jnp.bfloat16)
        qg = q.reshape(4, seq_len, n_kv, n_q // n_kv, head_dim)
        scores = jnp.einsum('bqkgd,bskd->bkgqs', qg, k, preferred_element_type=jnp.float32) * (head_dim ** -0.5)
        causal = jnp.arange(seq_len)[:, None] >= jnp.arange(seq_len)[None, :]
        scores = jnp.where(causal, scores, -jnp.inf)
        scores = scores - jnp.max(scores, axis=-1, keepdims=True)
        weights = jnp.exp(scores)
        probs = (weights / jnp.sum(weights, axis=-1, keepdims=True)).astype(jnp.bfloat16)
        ctx = jnp.einsum('bkgqs,bskd->bqkgd', probs, v, preferred_element_type=jnp.float32)
        ctx = ctx.astype(jnp.bfloat16).reshape(n_tok, q4)

        kv = jnp.concatenate([k.reshape(4, seq_len, kv4), v.reshape(4, seq_len, kv4)], axis=-1)
        kv_ex = kv[jnp.arange(4) ^ me]
        kv_x = send_x(kv_ex[2:])
        kv_y = send_y(jnp.stack([kv_ex[1], kv_x[1]]))
        kv_all = by_role(kv_ex[0], kv_x[0], kv_y[0], kv_y[1])
        k_out = kv_all[..., :kv4].reshape(4, seq_len, n_kv, head_dim).transpose(1, 0, 2, 3).reshape(1, seq_len, 4 * n_kv, head_dim)
        v_out = kv_all[..., kv4:].reshape(4, seq_len, n_kv, head_dim).transpose(1, 0, 2, 3).reshape(1, seq_len, 4 * n_kv, head_dim)

        ctx_full = square_gather(ctx).transpose(1, 0, 2).reshape(n_tok, q_width)
        attn = jnp.dot(ctx_full, full_out, preferred_element_type=jnp.float32)
        x_cols = lax.dynamic_slice_in_dim(x_all, me * w4, w4, 1)
        mid = (x_cols.astype(jnp.float32) + attn).astype(jnp.bfloat16)
        mid_f32 = mid.astype(jnp.float32)
        ss = jnp.sum(mid_f32 * mid_f32, axis=-1, keepdims=True)
        ss = ss.reshape(4, seq_len)
        ss = ss + send_x(ss)
        ss = (ss + send_y(ss)).reshape(n_tok, 1)
        inv2 = lax.rsqrt(ss / width + NORM_EPS)
        gain_cols = lax.dynamic_slice_in_dim(gain_mlp, me * w4, w4, 0)
        h2 = (mid_f32 * inv2 * gain_cols).astype(jnp.bfloat16)
        h2_full = square_gather(h2).transpose(1, 0, 2).reshape(n_tok, width)
        gate_up = jnp.dot(h2_full, full_gate_up, preferred_element_type=jnp.float32)
        half_ff = gate_up.shape[1] // 2
        act = (jax.nn.silu(gate_up[:, :half_ff]) * gate_up[:, half_ff:]).astype(jnp.bfloat16)
        down = jnp.dot(act, full_down, preferred_element_type=jnp.float32)
        cols = lax.broadcasted_iota(jnp.int32, (1, width), 1) // w4 == me
        down = down + jnp.where(cols, jnp.tile(mid_f32, (1, 4)), 0.0)
        out = square_scatter(down.reshape(4, seq_len, width))
        return out.astype(jnp.bfloat16)[None], k_out, v_out

    return jax.shard_map(
        device_step,
        mesh=mesh,
        in_specs=(P(batch_axes, None), row_spec, P('fsdp'), row_spec, row_spec, P('fsdp'), row_spec, row_spec, P(None)),
        out_specs=(P(batch_axes, None, None), P(batch_axes, None, None, None), P(batch_axes, None, None, None)),
        check_vma=False,
    )
```

```python
import functools
import math

import jax
import jax.numpy as jnp
from jax import lax
from jax.experimental import pallas as pl
from jax.experimental.pallas import tpu as pltpu
from jax.sharding import PartitionSpec as P

NORM_EPS = 1e-5
ROPE_THETA = 10000.0
PICK = 32
DEPTH = 4
LANES = 128
MESH = pl.DeviceIdType.MESH
BF16 = jnp.bfloat16
F32 = jnp.float32


def aligned(start, size, step):
    return pl.ds(pl.multiple_of(start, step), size)


class Where:
    def __init__(self, side, n_fsdp):
        self.side = side
        self.nz = n_fsdp // 2
        self.dp = lax.axis_index('dp')
        self.f = lax.axis_index('fsdp')
        self.z = self.f // 2
        self.c = self.f % 2
        self.px = self.dp // side
        self.py = self.dp % side
        self.me = 2 * (self.px % 2) + self.py % 2

    def chip(self, dz):
        return lax.rem(self.z + dz + self.nz, self.nz)

    def along_z(self, dz, core):
        return (self.dp, 2 * self.chip(dz) + core)

    def partner(self):
        return (self.dp, 2 * self.z + 1 - self.c)

    def square(self, rel, core):
        px = self.px + (1 - 2 * (self.px % 2)) if rel & 2 else self.px
        py = self.py + (1 - 2 * (self.py % 2)) if rel & 1 else self.py
        return (px * self.side + py, 2 * self.z + core)


def greet(devices):
    barrier = pltpu.get_barrier_semaphore()
    for dev in devices:
        pl.semaphore_signal(barrier, inc=1, device_id=dev, device_id_type=MESH)
    pl.semaphore_wait(barrier, len(devices))


def remote(src, dst, ssem, rsem, dev):
    return pltpu.make_async_remote_copy(src_ref=src, dst_ref=dst, send_sem=ssem, recv_sem=rsem, device_id=dev, device_id_type=MESH)


def arrived(ref, sem):
    pltpu.make_async_copy(ref, ref, sem).wait()


def ids_kernel(side, n_fsdp, tok_ref, gain_ref, ids_ref, gains_ref, lsem, ssem, rsem):
    w = Where(side, n_fsdp)
    greet([(w.dp, lax.rem(w.f + k, n_fsdp)) for k in range(1, n_fsdp)])
    own = [pltpu.make_async_copy(tok_ref, ids_ref.at[w.f], lsem.at[0]),
           pltpu.make_async_copy(gain_ref, gains_ref.at[w.f], lsem.at[1])]
    for cp in own:
        cp.start()
    sent = []
    for k in range(1, n_fsdp):
        dev = (w.dp, lax.rem(w.f + k, n_fsdp))
        for j, (src, dst) in enumerate(((tok_ref, ids_ref), (gain_ref, gains_ref))):
            cp = remote(src, dst.at[w.f], ssem.at[j, k], rsem.at[j, k], dev)
            cp.start()
            sent.append(cp)
    for cp in own:
        cp.wait()
    for cp in sent:
        cp.wait_send()
    for k in range(1, n_fsdp):
        src = lax.rem(w.f - k + n_fsdp, n_fsdp)
        arrived(ids_ref.at[src], rsem.at[0, k])
        arrived(gains_ref.at[src], rsem.at[1, k])


def gather_ids(side, n_fsdp, tokens, gains):
    return pl.pallas_call(
        functools.partial(ids_kernel, side, n_fsdp),
        out_shape=(jax.ShapeDtypeStruct((n_fsdp,) + tokens.shape, tokens.dtype), jax.ShapeDtypeStruct((n_fsdp,) + gains.shape, gains.dtype)),
        in_specs=[pl.BlockSpec(memory_space=pltpu.VMEM)] * 2,
        out_specs=(pl.BlockSpec(memory_space=pltpu.VMEM), pl.BlockSpec(memory_space=pltpu.VMEM)),
        scratch_shapes=[pltpu.SemaphoreType.DMA((2,)), pltpu.SemaphoreType.DMA((2, n_fsdp)), pltpu.SemaphoreType.DMA((2, n_fsdp))],
        compiler_params=pltpu.CompilerParams(collective_id=0, has_side_effects=True),
        name='ids',
    )(tokens, gains)


class Pieces:
    def __init__(self, rows, q4, kv4, w4, f4, n_fsdp, width):
        self.rows = rows
        self.q4, self.kv4, self.w4, self.f4 = q4, kv4, w4, f4
        self.n_fsdp = n_fsdp
        self.width = width
        self.qkv = q4 + 2 * kv4
        self.gu0 = self.qkv + w4
        self.gu_w = 2 * f4 * n_fsdp // 4
        self.dn0 = self.gu0 + 4 * self.gu_w
        self.dn_w = width // 4
        self.total = self.dn0 + width
        self.late = self.total - self.qkv
        self.chunks = [(0, self.qkv), (self.qkv, w4)]
        self.chunks += [(self.gu0 + b * self.gu_w, self.gu_w) for b in range(4)]
        self.chunks += [(self.dn0 + n * self.dn_w, self.dn_w) for n in range(4)]
        self.early = 3


def pack_copies(pc, me, pk, w_qkv, w_out, w_gu, w_dn, sem_a, sem_b):
    q4, kv4, w4, f4 = pc.q4, pc.kv4, pc.w4, pc.f4
    first = [
        (w_qkv.at[:, aligned(me * q4, q4, LANES)], pk.at[:, pl.ds(0, q4)]),
        (w_qkv.at[:, aligned(4 * q4 + me * kv4, kv4, LANES)], pk.at[:, pl.ds(q4, kv4)]),
        (w_qkv.at[:, aligned(4 * q4 + 4 * kv4 + me * kv4, kv4, LANES)], pk.at[:, pl.ds(q4 + kv4, kv4)]),
    ]
    for src, dst in first:
        pltpu.make_async_copy(src, dst, sem_a).start()
    pltpu.make_async_copy(w_out.at[:, aligned(me * w4, w4, LANES)], pk.at[:, pl.ds(pc.qkv, w4)], sem_b).start()
    ff = 4 * f4 * pc.n_fsdp
    for d in range(pc.n_fsdp):
        b, k = d // 4, d % 4
        for part in range(2):
            src = w_gu.at[:, aligned(part * ff + d * 4 * f4 + me * f4, f4, LANES)]
            dst = pk.at[:, pl.ds(pc.gu0 + b * pc.gu_w + part * (pc.gu_w // 2) + k * f4, f4)]
            pltpu.make_async_copy(src, dst, sem_b).start()
    pltpu.make_async_copy(w_dn.at[aligned(me * f4, f4, LANES), :], pk.at[:, pl.ds(pc.dn0, pc.width)], sem_b).start()


def gather_kernel(n_tok, gid_ref, tgt_ref, table_ref, out_ref, buf, obuf, sems, osem):
    width = table_ref.shape[2]
    n_step = n_tok // PICK

    def fetch(step, slot):
        def one(i, carry):
            g = gid_ref[step * PICK + i]

            @pl.when(g >= 0)
            def _():
                pltpu.make_async_copy(table_ref.at[g], buf.at[slot, i], sems.at[slot]).start()
            return carry
        lax.fori_loop(0, PICK, one, 0, unroll=8)

    def drain(step, slot):
        def one(i, carry):
            @pl.when(gid_ref[step * PICK + i] >= 0)
            def _():
                pltpu.make_async_copy(table_ref.at[0], buf.at[slot, 0], sems.at[slot]).wait()
            return carry
        lax.fori_loop(0, PICK, one, 0, unroll=8)

    buf[...] = jnp.zeros_like(buf)
    for j in range(DEPTH - 1):
        fetch(j, j)

    def body(step, carry):
        slot = lax.rem(step, DEPTH)

        @pl.when(step + DEPTH - 1 < n_step)
        def _():
            fetch(step + DEPTH - 1, lax.rem(step + DEPTH - 1, DEPTH))
        drain(step, slot)
        rows = pl.ds(pl.multiple_of(step * PICK, PICK), PICK)
        pick = (lax.broadcasted_iota(jnp.int32, (PICK, PICK * 8), 1) == tgt_ref[rows, :]).astype(jnp.bfloat16)
        block = buf[slot].reshape(PICK * 8, width)
        got = jnp.dot(pick, block, preferred_element_type=jnp.float32)
        out_ref[rows, :] = got.astype(jnp.bfloat16)
        return carry
    lax.fori_loop(0, n_step, body, 0)


def gather_table(ids, owned, table):
    n_tok = ids.shape[0]
    n_rows, width = table.shape
    gid = jnp.where(owned, ids // 8, -1)
    lane = jnp.arange(n_tok, dtype=jnp.int32) % PICK
    tgt = jnp.where(owned, 8 * lane + ids % 8, -1)[:, None]
    return pl.pallas_call(
        functools.partial(gather_kernel, n_tok),
        out_shape=jax.ShapeDtypeStruct((n_tok, width), jnp.bfloat16),
        in_specs=[pl.BlockSpec(memory_space=pltpu.SMEM), pl.BlockSpec(memory_space=pltpu.VMEM), pl.BlockSpec(memory_space=pl.ANY)],
        out_specs=pl.BlockSpec(memory_space=pltpu.VMEM),
        scratch_shapes=[
            pltpu.VMEM((DEPTH, PICK, 8, width), jnp.bfloat16),
            pltpu.VMEM((8, 128), jnp.bfloat16),
            pltpu.SemaphoreType.DMA((DEPTH,)),
            pltpu.SemaphoreType.DMA,
        ],
        compiler_params=pltpu.CompilerParams(vmem_limit_bytes=48 * 2**20),
        cost_estimate=pl.CostEstimate(flops=2 * n_tok * PICK * 8 * width, bytes_accessed=9 * n_tok * width * 2, transcendentals=0),
    )(gid, tgt, table.reshape(n_rows // 8, 8, width))


def embed_kernel(side, pc, rows_ref, w_qkv, w_out, w_gu, w_dn, x_ref, q_ref, own_ref, early_ref,
                 got, peer, rp, sb, pk, xo,
                 got_sem, pack_sem, own_sem, d2d_s, d2d_r, z_s, z_r, f_s, f_r, push_s, push_r,
                 peer_s, peer_r, rs_s, rs_r, x_s, x_r):
    n_fsdp = pc.n_fsdp
    w = Where(side, n_fsdp)
    nz = w.nz
    far = nz // 2
    seq = got.shape[2]
    hw = got.shape[3]
    width = 2 * hw
    order = [far]
    for o in range(far - 1, 0, -1):
        order += [o, -o]
    order += [0]
    mine = aligned(w.c * hw, hw, LANES)
    other = aligned((1 - w.c) * hw, hw, LANES)
    for k in range(len(order)):
        dest = w.chip(order[k])
        pltpu.make_async_copy(rows_ref.at[dest, :, :, mine], got.at[dest], got_sem.at[k]).start()
    pack_copies(pc, w.me, pk, w_qkv, w_out, w_gu, w_dn, pack_sem.at[0], pack_sem.at[1])
    greet([w.partner()] + [w.along_z(dz, core) for dz in (1, -1) for core in (0, 1)])
    dirs = (1, -1)

    for k in range(len(order)):
        dest = w.chip(order[k])
        remote(rows_ref.at[dest, :, :, other], peer.at[dest], peer_s.at[k], peer_r.at[k], w.partner()).start()

    sends = []
    arrived(pk.at[:, pl.ds(0, pc.qkv)], pack_sem.at[0])
    arrived(pk.at[:, pl.ds(pc.qkv, pc.total - pc.qkv)], pack_sem.at[1])

    def first_hop(t):
        off, cw = pc.chunks[t]
        for i, dz in enumerate(dirs):
            dst = q_ref.at[w.f] if t == 0 else early_ref.at[i, w.c, :, pl.ds(off - pc.qkv, cw)]
            cp = remote(pk.at[:, pl.ds(off, cw)], dst, z_s.at[t, i], z_r.at[t, i, w.c], w.along_z(dz, 1))
            cp.start()
            sends.append(cp)

    pk_q, pk_rest = pk.at[:, pl.ds(0, pc.qkv)], pk.at[:, pl.ds(pc.qkv, pc.late)]
    own = []
    for j, (src, dst) in enumerate(((pk_q, q_ref.at[w.f]), (pk_rest, own_ref.at[w.c]))):
        own += [pltpu.make_async_copy(src, dst, own_sem.at[j]), remote(src, dst, d2d_s.at[j], d2d_r.at[j], w.partner())]
    for cp in own:
        cp.start()


    def pair(dz):
        return q_ref.at[pl.ds(2 * w.chip(dz), 2)]

    def single(dz, i):
        return q_ref.at[pl.ds(2 * w.chip(dz) + i, 1)]

    def push(ref, i, h):
        remote(ref, ref, push_s.at[i, h], push_r, w.partner()).start()

    def forward(h):
        @pl.when(w.c == 1)
        def _():
            for i, dz in enumerate(dirs):
                if h == 1:
                    for core in range(2):
                        arrived(q_ref.at[2 * w.chip(-dz) + core], z_r.at[0, i, core])
                elif h < far:
                    arrived(pair(-dz * h), f_r.at[i, h])
                else:
                    arrived(single(-dz * h, i), f_r.at[i, h])
                if h < far - 1:
                    remote(pair(-dz * h), pair(-dz * h), f_s.at[i, h + 1], f_r.at[i, h + 1], w.along_z(dz, 1)).start()
                elif h == far - 1:
                    remote(single(-dz * h, i), single(-dz * h, i), f_s.at[i, h + 1], f_r.at[i, h + 1], w.along_z(dz, 1)).start()
                push(pair(-dz * h) if h < far else single(-dz * h, i), i, h)

    def addto(dst, terms):
        def one(r, carry):
            rows = aligned(r * 32, 32, 32)
            val = terms[0](rows)
            for term in terms[1:]:
                val = val + term(rows)
            dst(rows, val)
            return carry
        lax.fori_loop(0, seq // 32, one, 0)

    def rs_stage(k):
        o = order[k]
        dest = w.chip(o)
        arrived(got.at[dest], got_sem.at[k])
        arrived(peer.at[dest], peer_r.at[k])
        if o == 0:
            return
        for i, dz in enumerate(dirs):
            if o * dz < 0 and o != far:
                continue
            dist = abs(o)
            halves = (i,) if dist == far else (1 - i, i)
            for h in halves:
                terms = [lambda r, h=h: got[dest, h, r, :], lambda r, h=h: peer[dest, h, r, :]]
                if dist < far - 1 or (dist == far - 1 and h == i):
                    arrived(rp.at[i, dist, h], rs_r.at[i, dist, h])
                    terms.append(lambda r, h=h: rp[i, dist, h, r, :])

                def put(r, val, h=h):
                    sb[i, dist - 1, h, r, :] = val
                addto(put, terms)
                remote(sb.at[i, dist - 1, h], rp.at[i, dist - 1, h], rs_s.at[i, dist - 1, h], rs_r.at[i, dist - 1, h], w.along_z(dz, w.c)).start()

    for k in range(len(order) - 1):
        rs_stage(k)
        if k < pc.early:
            first_hop(k)
        if k >= 3:
            forward(k - 2)
    rs_stage(len(order) - 1)
    for h in range(2):
        terms = [lambda r: got[w.z, h, r, :], lambda r: peer[w.z, h, r, :]]
        for i in range(2):
            arrived(rp.at[i, 0, h], rs_r.at[i, 0, h])
            terms.append(lambda r, i=i: rp[i, 0, h, r, :])

        def put(r, val):
            xo[h, r, :] = val
        addto(put, terms)
    home = pltpu.make_async_copy(xo, x_ref.at[:, :, mine], x_s.at[1])
    away = remote(xo, x_ref.at[:, :, mine], x_s.at[0], x_r, w.partner())
    home.start()
    away.start()

    for cp in sends:
        cp.wait_send()
    for cp in own:
        cp.wait()
    for k in range(len(order)):
        dest = w.chip(order[k])
        arrived(peer.at[dest], peer_s.at[k])
    for i in range(2):
        for dist in range(1, far + 1):
            for h in ((i,) if dist == far else (0, 1)):
                arrived(sb.at[i, dist - 1, h], rs_s.at[i, dist - 1, h])

    @pl.when(w.c == 1)
    def _():
        for i, dz in enumerate(dirs):
            for t in range(1, pc.early):
                off, cw = pc.chunks[t]
                for core in range(2):
                    arrived(early_ref.at[i, core, :, pl.ds(off - pc.qkv, cw)], z_r.at[t, i, core])
            for h in range(1, far + 1):
                ref = pair(-dz * h) if h < far else single(-dz * h, i)
                arrived(ref, push_s.at[i, h])
                if h < far:
                    arrived(pair(-dz * h) if h < far - 1 else single(-dz * h, i), f_s.at[i, h + 1])

    @pl.when(w.c == 0)
    def _():
        arrived(q_ref.at[pl.ds(0, n_fsdp - 2)], push_r)
    home.wait()
    away.wait()


def embed(side, pc, rows, w_qkv, w_out, w_gu, w_dn):
    seq, width = rows.shape[2], rows.shape[3]
    nz = pc.n_fsdp // 2
    far = nz // 2
    hbm = pl.BlockSpec(memory_space=pl.ANY)
    dma = pltpu.SemaphoreType.DMA
    return pl.pallas_call(
        functools.partial(embed_kernel, side, pc),
        out_shape=(
            jax.ShapeDtypeStruct((2, seq, width), BF16),
            jax.ShapeDtypeStruct((pc.n_fsdp, pc.rows, pc.qkv), BF16),
            jax.ShapeDtypeStruct((2, pc.rows, pc.late), BF16),
            jax.ShapeDtypeStruct((2, 2, pc.rows, sum(cw for _, cw in pc.chunks[1:pc.early])), BF16)),
        in_specs=[hbm] * 5,
        out_specs=(hbm, hbm, hbm, hbm),
        scratch_shapes=[
            pltpu.VMEM((nz, 2, seq, width // 2), BF16),
            pltpu.VMEM((nz, 2, seq, width // 2), BF16),
            pltpu.VMEM((2, far, 2, seq, width // 2), BF16),
            pltpu.VMEM((2, far, 2, seq, width // 2), BF16),
            pltpu.VMEM((pc.rows, pc.total), BF16),
            pltpu.VMEM((2, seq, width // 2), BF16),
            dma((nz,)), dma((2,)), dma((2,)), dma((2,)), dma((2,)),
            dma((pc.early, 2)), dma((pc.early, 2, 2)),
            dma((2, far + 1)), dma((2, far + 1)), dma((2, far + 1)), dma,
            dma((nz,)), dma((nz,)),
            dma((2, far, 2)), dma((2, far, 2)),
            dma((2,)), dma,
        ],
        compiler_params=pltpu.CompilerParams(collective_id=1, has_side_effects=True, vmem_limit_bytes=67043328),
        name='embed',
    )(rows, w_qkv, w_out, w_gu, w_dn)


def layer_kernel(side, pc, head_dim, x_ref, q_ref, own_ref, early_ref, g1_ref, g2_ref, cos_ref, sin_ref, out_ref, k_ref, v_ref, w_ref,
                 xa, ca, xm, wg, wd, mm, pp, r1, r2, qf, kvb,
                 lsem, xs_s, xs_r, cs_s, cs_r, ms_s, ms_r, kv_s, kv_r, p1_s, p1_r, p2_s, p2_r, o_s, o_l, o_r,
                 zs, zr, ps, wch):
    h2 = ca
    n_fsdp = pc.n_fsdp
    w = Where(side, n_fsdp)
    far = w.nz // 2
    seq, width = xa.shape[2], xa.shape[3]
    rows_b = 2 * seq
    half = pc.dn_w // 2
    n_chunk = len(pc.chunks)
    last_gu = 5
    greet([w.partner(), w.along_z(1, w.c), w.along_z(-1, w.c)] + [w.square(rel, core) for rel in (1, 2, 3) for core in (0, 1)])
    dirs = (1, -1)

    def stream():
        def cols(t):
            off, cw = pc.chunks[t]
            return pl.ds(off - pc.qkv, cw)

        def pair(t, dz):
            return w_ref.at[pl.ds(2 * w.chip(dz), 2), :, cols(t)]

        def single(t, dz, i):
            return w_ref.at[pl.ds(2 * w.chip(dz) + i, 1), :, cols(t)]

        def piece(t, h, i):
            dz = dirs[i]
            return pair(t, -dz * h) if h < far else single(t, -dz * h, i)

        def source(t, h, i, ref):
            if h == 0:
                return own_ref.at[:, :, cols(t)]
            if h == 1 and t < pc.early:
                return early_ref.at[i, :, :, cols(t)]
            return ref

        sent = []

        def hop(t, h):
            if t < 1 or t >= n_chunk or (h == 0 and t < pc.early):
                return
            for i in range(2):
                dz = dirs[i]
                if h > 1 or (h == 1 and t >= pc.early):
                    arrived(piece(t, h, i), zr.at[t, i, h])
                if h < far:
                    ref = pair(t, -dz * h) if h < far - 1 else single(t, -dz * h, i)
                    remote(source(t, h, i, ref), ref, zs.at[t, i, h], zr.at[t, i, h + 1], w.along_z(dz, 1)).start()
                    sent.append((ref, zs.at[t, i, h]))
            if h > 0:
                for i in range(2):
                    ref = piece(t, h, i)
                    remote(source(t, h, i, ref), ref, ps.at[t, i, h], wch.at[t], w.partner()).start()
                    sent.append((ref, ps.at[t, i, h]))

        for s in range(pc.early - 1, n_chunk + far):
            for h in range(far + 1):
                hop(s - h, h)
        for ref, sem in sent:
            arrived(ref, sem)
        kvw = 2 * (kvb.shape[2] // 4)
        for rel in range(4):
            arrived(k_ref.at[:, pl.ds(0, kvw)], kv_r.at[rel, 0])
            arrived(v_ref.at[:, pl.ds(0, kvw)], kv_r.at[rel, 1])
        for n in range(4):
            arrived(out_ref.at[:, pl.ds(n * pc.dn_w, pc.dn_w)], o_r.at[n])

    def compute():
        y, x = w.square(1, 0), w.square(2, 0)
        q4, kv4 = pc.q4, pc.kv4
        cols = {q: aligned((w.me ^ q) * pc.w4, pc.w4, LANES) for q in range(4)}
        sent = []

        def go(cp):
            cp.start()
            sent.append(cp)

        def load(t, dst, sem):
            off, cw = pc.chunks[t]
            c = pl.ds(off - pc.qkv, cw)
            arrived(w_ref.at[pl.ds(0, n_fsdp - 2), :, c], wch.at[t])
            for dz in range(w.nz):
                two = pl.ds(2 * w.chip(dz), 2)
                src = own_ref.at[:, :, c] if dz == 0 else w_ref.at[two, :, c]
                pltpu.make_async_copy(src, dst.at[two], sem).start()

        own = pltpu.make_async_copy(x_ref, xa.at[0], lsem.at[0])
        own.start()
        first = pltpu.make_async_copy(q_ref, wg.at[:, :, pl.ds(0, pc.qkv)], lsem.at[1])
        first.start()
        go(remote(x_ref.at[0], xa.at[2, 0], xs_s.at[0], xs_r.at[2, 0], x))
        go(remote(x_ref.at[1], xa.at[1, 1], xs_s.at[1], xs_r.at[1, 1], y))
        go(remote(x_ref.at[1], xa.at[2, 1], xs_s.at[2], xs_r.at[2, 1], x))
        go(remote(x_ref.at[0], xa.at[1, 0], xs_s.at[3], xs_r.at[1, 0], y))
        own.wait()
        first.wait()

        def norm_into(dst, slot, load_rows, gain_ref):
            def one(i, carry):
                rows = aligned(i * 16, 16, 16)
                val = load_rows(rows, i).astype(F32)
                inv = lax.rsqrt(jnp.mean(val * val, axis=-1, keepdims=True) + NORM_EPS)
                dst[slot, rows, :] = (val * inv * gain_ref[...]).astype(BF16)
                return carry
            lax.fori_loop(0, rows_b // 16, one, 0)

        per = seq // 16
        lane = lax.broadcasted_iota(jnp.int32, (seq, LANES), 1)
        low_head = (lane % head_dim) < head_dim // 2
        first_head = lane < head_dim
        n_pair = q4 // LANES
        pair_per_kv = n_pair // 2

        def rope(t):
            swapped = jnp.where(low_head, pltpu.roll(t, LANES - head_dim // 2, 1), pltpu.roll(t, head_dim // 2, 1))
            return t * cos_ref[...] + swapped * sin_ref[...]

        def attend(slot):
            norm_into(mm, slot, lambda rows, i: xa[slot, i // per, aligned((i % per) * 16, 16, 16), :], g1_ref)
            def proj(nt, carry):
                c = aligned(nt * 256, 256, LANES)
                qf[:, c] = jnp.dot(mm[slot], wg[:, :, c].reshape(width, 256), preferred_element_type=F32)
                return carry
            lax.fori_loop(0, pc.qkv // 256, proj, 0)

            def one_seq(u, carry):
                rows = aligned(u * seq, seq, seq)
                k_f = rope(qf[rows, pl.ds(q4, LANES)])
                v_f = qf[rows, pl.ds(q4 + kv4, LANES)]
                kvb[slot, rows, pl.ds(0, LANES)] = k_f.astype(BF16)
                kvb[slot, rows, pl.ds(LANES, LANES)] = v_f.astype(BF16)
                k_r, v_r = pltpu.roll(k_f, head_dim, 1), pltpu.roll(v_f, head_dim, 1)
                zero = jnp.zeros_like(k_f)
                row = lax.broadcasted_iota(jnp.int32, (pair_per_kv * seq, seq), 0) % seq
                causal = row >= lax.broadcasted_iota(jnp.int32, (pair_per_kv * seq, seq), 1)
                for g in range(2):
                    k_lo, k_hi = (k_f, k_r) if g == 0 else (k_r, k_f)
                    v_lo, v_hi = (v_f, v_r) if g == 0 else (v_r, v_f)
                    kk = jnp.concatenate([jnp.where(first_head, k_lo, zero), jnp.where(first_head, zero, k_hi)], axis=0).astype(BF16)
                    vv = jnp.concatenate([jnp.where(first_head, v_lo, zero), jnp.where(first_head, zero, v_hi)], axis=0).astype(BF16)
                    qs = jnp.concatenate([rope(qf[rows, pl.ds((g * pair_per_kv + p) * LANES, LANES)]).astype(BF16) for p in range(pair_per_kv)], axis=0)
                    sc = lax.dot_general(qs, kk, (((1,), (1,)), ((), ())), preferred_element_type=F32) * (head_dim ** -0.5)
                    probs = []
                    for e in range(2):
                        part = jnp.where(causal, sc[:, e * seq:(e + 1) * seq], -jnp.inf)
                        part = jnp.exp(part - jnp.max(part, axis=-1, keepdims=True))
                        probs.append((part / jnp.sum(part, axis=-1, keepdims=True)).astype(BF16))
                    ctx = jnp.dot(jnp.concatenate(probs, axis=1), vv, preferred_element_type=F32).astype(BF16)
                    for p in range(pair_per_kv):
                        lanes = aligned(w.me * pc.w4 + (g * pair_per_kv + p) * LANES, LANES, LANES)
                        ca[slot, rows, lanes] = ctx[p * seq:(p + 1) * seq]
                return carry
            lax.fori_loop(0, 2, one_seq, 0)

        def spread(buf, slot, ss, rs):
            mine = buf.at[slot, :, cols[0]]
            go(remote(mine, buf.at[slot ^ 2, :, cols[0]], ss.at[slot, 1], rs.at[slot ^ 2, 1], x))
            go(remote(mine, buf.at[slot ^ 1, :, cols[0]], ss.at[slot, 0], rs.at[slot ^ 1, 0], y))

        def take(buf, slot, q, rs):
            arrived(buf.at[slot, :, cols[q]], rs.at[slot, q - 1 if q < 3 else 2])

        def relay(buf, slot, q, ss, rs):
            take(buf, slot, q, rs)
            ref = buf.at[slot, :, cols[q]]
            to, dev = (slot ^ 1, y) if q == 2 else (slot ^ 2, x)
            go(remote(ref, buf.at[to, :, cols[q]], ss.at[to, 2], rs.at[to, 2], dev))

        def send_kv(slot):
            mine = aligned(w.me * kv4, kv4, LANES)
            for core in range(2):
                for j, dst in enumerate((k_ref, v_ref)):
                    src = kvb.at[slot, pl.ds(core * seq, seq), pl.ds(j * kv4, kv4)]
                    if slot == 0 and core == 0:
                        cp = pltpu.make_async_copy(src, dst.at[:, mine], kv_s.at[slot, core, j])
                        cp.start()
                        local_kv.append(cp)
                    else:
                        go(remote(src, dst.at[:, mine], kv_s.at[slot, core, j], kv_r.at[slot, j], w.square(slot, core)))
        local_kv = []

        def here(slot, h):
            arrived(xa.at[slot, h], xs_r.at[slot, h])

        attend(0)
        here(2, 0)
        go(remote(xa.at[2, 0], xa.at[3, 0], xs_s.at[4], xs_r.at[3, 0], y))
        here(1, 1)
        go(remote(xa.at[1, 1], xa.at[3, 1], xs_s.at[5], xs_r.at[3, 1], x))
        spread(ca, 0, cs_s, cs_r)
        here(2, 1)
        attend(2)
        spread(ca, 2, cs_s, cs_r)
        here(1, 0)
        attend(1)
        spread(ca, 1, cs_s, cs_r)
        relay(ca, 2, 2, cs_s, cs_r)
        here(3, 0)
        here(3, 1)
        attend(3)
        spread(ca, 3, cs_s, cs_r)
        relay(ca, 0, 2, cs_s, cs_r)
        relay(ca, 0, 1, cs_s, cs_r)
        relay(ca, 2, 1, cs_s, cs_r)
        load(1, wd, lsem.at[0])
        for slot in range(4):
            send_kv(slot)
        arrived(wd, lsem.at[0])
        n_ctx = len(sent)

        def mid(slot):
            for q in (1, 2, 3):
                if q == 3 or slot in (1, 3):
                    take(ca, slot, q, cs_r)

            def one(nt, carry):
                c = aligned(nt * 256, 256, LANES)
                o = aligned(w.me * pc.w4 + nt * 256, 256, LANES)
                got = jnp.dot(ca[slot], wd[:, :, c].reshape(width, 256), preferred_element_type=F32)
                res = xa[slot, :, :, o].reshape(rows_b, 256).astype(F32)
                xm[slot, :, o] = (res + got).astype(BF16)
                return carry
            lax.fori_loop(0, pc.w4 // 256, one, 0)
            spread(xm, slot, ms_s, ms_r)

        mid(3)
        mid(1)
        mid(2)
        relay(xm, 1, 2, ms_s, ms_r)
        mid(0)
        relay(xm, 3, 2, ms_s, ms_r)
        relay(xm, 3, 1, ms_s, ms_r)
        relay(xm, 1, 1, ms_s, ms_r)
        for cp in sent[:n_ctx]:
            cp.wait_send()
        del sent[:n_ctx]
        for slot in (0, 2, 1, 3):
            for q in (1, 2, 3):
                if q == 3 or slot in (0, 2):
                    take(xm, slot, q, ms_r)
            norm_into(h2, slot, lambda rows, i, slot=slot: xm[slot, rows, :], g2_ref)

        gate_w = pc.gu_w // 2
        for b in range(4):
            load(2 + b, wg, lsem.at[b % 2])
            arrived(wg, lsem.at[b % 2])

            def one(j, carry):
                s, nt = j // (gate_w // 256), j % (gate_w // 256)
                act = h2[pl.ds(2 * s, 2)].reshape(2 * rows_b, width)
                gate = jnp.dot(act, wg[:, :, aligned(nt * 256, 256, LANES)].reshape(width, 256), preferred_element_type=F32)
                up = jnp.dot(act, wg[:, :, aligned(gate_w + nt * 256, 256, LANES)].reshape(width, 256), preferred_element_type=F32)
                val = (jax.nn.silu(gate) * up).astype(BF16)
                mm[pl.ds(2 * s, 2), :, aligned(b * gate_w + nt * 256, 256, LANES)] = val.reshape(2, rows_b, 256)
                return carry
            lax.fori_loop(0, 2 * (gate_w // 256), one, 0)

        h0, h1 = pl.ds(0, half), pl.ds(half, half)
        first_sends, home = {}, []

        def phase1(n):
            load(last_gu + 1 + n, wd, lsem.at[n % 2])
            for old in first_sends.get(n - 2, ()):
                old.wait_send()
            arrived(wd, lsem.at[n % 2])
            par = n % 2

            def one(j, carry):
                s, nt = j // (pc.dn_w // 256), j % (pc.dn_w // 256)
                c = aligned(nt * 256, 256, LANES)
                act = mm[pl.ds(2 * s, 2)].reshape(2 * rows_b, mm.shape[2])
                got = jnp.dot(act, wd[:, :, c].reshape(mm.shape[2], 256), preferred_element_type=F32)
                pp[par, pl.ds(2 * s, 2), :, c] = got.reshape(2, rows_b, 256)
                return carry
            lax.fori_loop(0, 2 * (pc.dn_w // 256), one, 0)
            first_sends[n] = []
            for path, dev, cc, rels in ((0, x, h0, (2, 3)), (1, y, h1, (1, 3))):
                for j, rel in enumerate(rels):
                    cp = remote(pp.at[par, rel, :, cc], r1.at[n, path, j], p1_s.at[n, path, j], p1_r.at[n, path, j], dev)
                    cp.start()
                    first_sends[n].append(cp)

        def phase2(n):
            par = n % 2
            for path, dev, cc, rel in ((0, y, h0, 1), (1, x, h1, 2)):
                arrived(r1.at[n, path, 1], p1_r.at[n, path, 1])
                r1[n, path, 1] = pp[par, rel, :, cc] + r1[n, path, 1]
                go(remote(r1.at[n, path, 1], r2.at[n, path], p2_s.at[n, path], p2_r.at[n, path], dev))
            for path, cc in ((0, h0), (1, h1)):
                arrived(r1.at[n, path, 0], p1_r.at[n, path, 0])
                r1[n, path, 0] = pp[par, 0, :, cc] + r1[n, path, 0]

        def phase3(n):
            for path in range(2):
                arrived(r2.at[n, path], p2_r.at[n, path])
                c = pl.ds(n * pc.dn_w + path * half, half)
                total = xm[0, :, c].astype(F32) + (r1[n, path, 0] + r2[n, path])
                xm[0, :, c] = total.astype(BF16)
            c = pl.ds(n * pc.dn_w, pc.dn_w)
            go(remote(xm.at[0, pl.ds(seq, seq), c], out_ref.at[:, c], o_s.at[n], o_r.at[n], w.partner()))
            cp = pltpu.make_async_copy(xm.at[0, pl.ds(0, seq), c], out_ref.at[:, c], o_l.at[n])
            cp.start()
            home.append(cp)

        for cp in sent:
            cp.wait_send()
        sent.clear()
        for n in range(4):
            phase1(n)
            if n >= 1:
                phase2(n - 1)
            if n >= 2:
                phase3(n - 2)
        phase2(3)
        phase3(2)
        phase3(3)

        for cp in sent:
            cp.wait_send()
        for n in (2, 3):
            for cp in first_sends[n]:
                cp.wait_send()
        for cp in local_kv + home:
            cp.wait()
        for rel in (1, 2, 3):
            arrived(k_ref.at[:, pl.ds(0, kv4)], kv_r.at[rel, 0])
            arrived(v_ref.at[:, pl.ds(0, kv4)], kv_r.at[rel, 1])

    pl.when(w.c == 1)(stream)
    pl.when(w.c == 0)(compute)


def layer(side, pc, head_dim, x, q_all, own2, early, g1, g2, cos_tab, sin_tab):
    _, seq, width = x.shape
    rows_b = 2 * seq
    kv_width = 4 * pc.kv4
    n_chunk = len(pc.chunks)
    far = pc.n_fsdp // 4
    ff4 = pc.f4 * pc.n_fsdp
    half = pc.dn_w // 2
    hbm = pl.BlockSpec(memory_space=pl.ANY)
    vmem = pl.BlockSpec(memory_space=pltpu.VMEM)
    dma = pltpu.SemaphoreType.DMA
    return pl.pallas_call(
        functools.partial(layer_kernel, side, pc, head_dim),
        out_shape=(
            jax.ShapeDtypeStruct((seq, width), BF16),
            jax.ShapeDtypeStruct((seq, kv_width), BF16),
            jax.ShapeDtypeStruct((seq, kv_width), BF16),
            jax.ShapeDtypeStruct((pc.n_fsdp, pc.rows, pc.late), BF16)),
        in_specs=[hbm, hbm, hbm, hbm, vmem, vmem, vmem, vmem],
        out_specs=(hbm, hbm, hbm, hbm),
        scratch_shapes=[
            pltpu.VMEM((4, 2, seq, width), BF16),
            pltpu.VMEM((4, rows_b, width), BF16),
            pltpu.VMEM((4, rows_b, width), BF16),
            pltpu.VMEM((pc.n_fsdp, pc.rows, pc.gu_w), BF16),
            pltpu.VMEM((pc.n_fsdp, pc.rows, pc.dn_w), BF16),
            pltpu.VMEM((4, rows_b, max(ff4, width)), BF16),
            pltpu.VMEM((2, 4, rows_b, pc.dn_w), F32),
            pltpu.VMEM((4, 2, 2, rows_b, half), F32),
            pltpu.VMEM((4, 2, rows_b, half), F32),
            pltpu.VMEM((rows_b, pc.qkv), F32),
            pltpu.VMEM((4, rows_b, 2 * pc.kv4), BF16),
            dma((2,)),
            dma((6,)), dma((4, 2)),
            dma((4, 3)), dma((4, 3)),
            dma((4, 3)), dma((4, 3)),
            dma((4, 2, 2)), dma((4, 2)),
            dma((4, 2, 2)), dma((4, 2, 2)),
            dma((4, 2)), dma((4, 2)),
            dma((4,)), dma((4,)), dma((4,)),
            dma((n_chunk, 2, far + 1)), dma((n_chunk, 2, far + 1)), dma((n_chunk, 2, far + 1)), dma((n_chunk,)),
        ],
        compiler_params=pltpu.CompilerParams(collective_id=2, has_side_effects=True, vmem_limit_bytes=67043328),
        name='layer',
    )(x, q_all, own2, early, g1, g2, cos_tab, sin_tab)


def solution(mesh):
    batch_axes = ('dp', 'fsdp')
    row_spec = P('fsdp', None)
    n_dp = mesh.shape['dp']
    n_fsdp = mesh.shape['fsdp']
    side = math.isqrt(n_dp)

    def device_step(tokens, embed_table, norm_attn, w_qkv, w_out, norm_mlp, w_gate_up, w_down, rope_scale):
        seq = tokens.shape[1]
        shard_rows, width = embed_table.shape
        head_dim = 2 * rope_scale.shape[0]
        rows = w_out.shape[0]
        q_width = rows * n_fsdp
        kv_width = (w_qkv.shape[1] - q_width) // 2
        pc = Pieces(rows, q_width // 4, kv_width // 4, width // 4, w_down.shape[0] // 4, n_fsdp, width)

        gains = jnp.stack([norm_attn, norm_mlp]).astype(F32)
        ids, gains = gather_ids(side, n_fsdp, tokens, gains)
        ids = ids.reshape(-1) - lax.axis_index('fsdp') * shard_rows
        owned = (ids >= 0) & (ids < shard_rows)
        table_rows = gather_table(ids, owned, embed_table)
        g1 = gains[:, 0].reshape(1, width)
        g2 = gains[:, 1].reshape(1, width)

        freq_expo = jnp.arange(head_dim // 2, dtype=F32) * (2.0 / head_dim)
        inv_freq = 1.0 / (rope_scale * jnp.power(ROPE_THETA, freq_expo))
        angles = jnp.arange(seq, dtype=F32)[:, None] * inv_freq[None, :]
        cos_tab, sin_tab = jnp.cos(angles), jnp.sin(angles)
        reps = LANES // head_dim
        cos_tab = jnp.concatenate([cos_tab, cos_tab] * reps, axis=1)
        sin_tab = jnp.concatenate([-sin_tab, sin_tab] * reps, axis=1)

        x, q_all, own2, early = embed(side, pc, table_rows.reshape(n_fsdp // 2, 2, seq, width), w_qkv, w_out, w_gate_up, w_down)
        out, k, v, _ = layer(side, pc, head_dim, x, q_all, own2, early, g1, g2, cos_tab, sin_tab)
        heads = (1, seq, kv_width // head_dim, head_dim)
        return out[None], k.reshape(heads), v.reshape(heads)

    return jax.shard_map(
        device_step,
        mesh=mesh,
        in_specs=(P(batch_axes, None), row_spec, P('fsdp'), row_spec, row_spec, P('fsdp'), row_spec, row_spec, P(None)),
        out_specs=(P(batch_axes, None, None), P(batch_axes, None, None, None), P(batch_axes, None, None, None)),
        check_vma=False,
    )
```

```python
import functools
import math

import jax
import jax.numpy as jnp
from jax import lax
from jax.experimental import pallas as pl
from jax.experimental.pallas import tpu as pltpu
from jax.sharding import PartitionSpec as P

NORM_EPS = 1e-5
ROPE_THETA = 10000.0
PICK = 32
DEPTH = 4
LANES = 128
MESH = pl.DeviceIdType.MESH
BF16 = jnp.bfloat16
F32 = jnp.float32


def aligned(start, size, step):
    return pl.ds(pl.multiple_of(start, step), size)


class Where:
    def __init__(self, side, n_fsdp):
        self.side = side
        self.nz = n_fsdp // 2
        self.dp = lax.axis_index('dp')
        self.f = lax.axis_index('fsdp')
        self.z = self.f // 2
        self.c = self.f % 2
        self.px = self.dp // side
        self.py = self.dp % side
        self.me = 2 * (self.px % 2) + self.py % 2

    def chip(self, dz):
        return lax.rem(self.z + dz + self.nz, self.nz)

    def along_z(self, dz, core):
        return (self.dp, 2 * self.chip(dz) + core)

    def partner(self):
        return (self.dp, 2 * self.z + 1 - self.c)

    def square(self, rel, core):
        px = self.px + (1 - 2 * (self.px % 2)) if rel & 2 else self.px
        py = self.py + (1 - 2 * (self.py % 2)) if rel & 1 else self.py
        return (px * self.side + py, 2 * self.z + core)


def greet(devices):
    barrier = pltpu.get_barrier_semaphore()
    for dev in devices:
        pl.semaphore_signal(barrier, inc=1, device_id=dev, device_id_type=MESH)
    pl.semaphore_wait(barrier, len(devices))


def remote(src, dst, ssem, rsem, dev):
    return pltpu.make_async_remote_copy(src_ref=src, dst_ref=dst, send_sem=ssem, recv_sem=rsem, device_id=dev, device_id_type=MESH)


def arrived(ref, sem):
    pltpu.make_async_copy(ref, ref, sem).wait()


def ids_kernel(side, pc, tok_ref, gain_ref, w_qkv, w_out, w_gu, w_dn, ids_ref, gains_ref, pq_ref, pe_ref, pd_ref,
               pk, lsem, ssem, rsem, pack_sem, store_sem):
    n_fsdp = pc.n_fsdp
    w = Where(side, n_fsdp)
    pack_copies(pc, w.me, pk, w_qkv, w_out, w_gu, w_dn, pack_sem)
    greet([(w.dp, lax.rem(w.f + k, n_fsdp)) for k in range(1, n_fsdp)])
    own = [pltpu.make_async_copy(tok_ref, ids_ref.at[w.f], lsem.at[0]),
           pltpu.make_async_copy(gain_ref, gains_ref.at[w.f], lsem.at[1])]
    for cp in own:
        cp.start()
    sent = []
    for k in range(1, n_fsdp):
        dev = (w.dp, lax.rem(w.f + k, n_fsdp))
        for j, (src, dst) in enumerate(((tok_ref, ids_ref), (gain_ref, gains_ref))):
            cp = remote(src, dst.at[w.f], ssem.at[j, k], rsem.at[j, k], dev)
            cp.start()
            sent.append(cp)
    arrived(pk, pack_sem)
    lo = 0
    stores = []
    for j, ref in enumerate((pq_ref, pe_ref, pd_ref)):
        stores.append(pltpu.make_async_copy(pk.at[:, pl.ds(lo, ref.shape[1])], ref, store_sem.at[j]))
        stores[-1].start()
        lo += ref.shape[1]
    for cp in own + stores:
        cp.wait()
    for cp in sent:
        cp.wait_send()
    for k in range(1, n_fsdp):
        src = lax.rem(w.f - k + n_fsdp, n_fsdp)
        arrived(ids_ref.at[src], rsem.at[0, k])
        arrived(gains_ref.at[src], rsem.at[1, k])


class Pieces:
    def __init__(self, rows, q4, kv4, w4, f4, n_fsdp, width):
        self.rows = rows
        self.q4, self.kv4, self.w4, self.f4 = q4, kv4, w4, f4
        self.n_fsdp = n_fsdp
        self.width = width
        self.qkv = q4 + 2 * kv4
        self.gu0 = self.qkv + w4
        self.gu_w = 2 * f4 * n_fsdp // 4
        self.dn0 = self.gu0 + 4 * self.gu_w
        self.dn_w = width // 4
        self.total = self.dn0 + width
        self.late = self.total - self.qkv
        self.chunks = [(0, self.qkv), (self.qkv, w4)]
        self.chunks += [(self.gu0 + b * self.gu_w, self.gu_w) for b in range(4)]
        self.chunks += [(self.dn0 + n * self.dn_w, self.dn_w) for n in range(4)]
        self.early = 6


def pack_copies(pc, me, pk, w_qkv, w_out, w_gu, w_dn, sem):
    q4, kv4, w4, f4 = pc.q4, pc.kv4, pc.w4, pc.f4
    first = [
        (w_qkv.at[:, aligned(me * q4, q4, LANES)], pk.at[:, pl.ds(0, q4)]),
        (w_qkv.at[:, aligned(4 * q4 + me * kv4, kv4, LANES)], pk.at[:, pl.ds(q4, kv4)]),
        (w_qkv.at[:, aligned(4 * q4 + 4 * kv4 + me * kv4, kv4, LANES)], pk.at[:, pl.ds(q4 + kv4, kv4)]),
    ]
    for src, dst in first:
        pltpu.make_async_copy(src, dst, sem).start()
    pltpu.make_async_copy(w_out.at[:, aligned(me * w4, w4, LANES)], pk.at[:, pl.ds(pc.qkv, w4)], sem).start()
    ff = 4 * f4 * pc.n_fsdp
    for d in range(pc.n_fsdp):
        b, k = d // 4, d % 4
        for part in range(2):
            src = w_gu.at[:, aligned(part * ff + d * 4 * f4 + me * f4, f4, LANES)]
            dst = pk.at[:, pl.ds(pc.gu0 + b * pc.gu_w + part * (pc.gu_w // 2) + k * f4, f4)]
            pltpu.make_async_copy(src, dst, sem).start()
    pltpu.make_async_copy(w_dn.at[aligned(me * f4, f4, LANES), :], pk.at[:, pl.ds(pc.dn0, pc.width)], sem).start()


def gather_ids(side, pc, tokens, gains, w_qkv, w_out, w_gu, w_dn):
    n_fsdp = pc.n_fsdp
    vmem, hbm = pl.BlockSpec(memory_space=pltpu.VMEM), pl.BlockSpec(memory_space=pl.ANY)
    dma = pltpu.SemaphoreType.DMA
    return pl.pallas_call(
        functools.partial(ids_kernel, side, pc),
        out_shape=(
            jax.ShapeDtypeStruct((n_fsdp,) + tokens.shape, tokens.dtype),
            jax.ShapeDtypeStruct((n_fsdp,) + gains.shape, gains.dtype),
            jax.ShapeDtypeStruct((pc.rows, pc.qkv), BF16),
            jax.ShapeDtypeStruct((pc.rows, pc.dn0 - pc.qkv), BF16),
            jax.ShapeDtypeStruct((pc.rows, pc.width), BF16)),
        in_specs=[vmem, vmem, hbm, hbm, hbm, hbm],
        out_specs=(vmem, vmem, hbm, hbm, hbm),
        scratch_shapes=[pltpu.VMEM((pc.rows, pc.total), BF16), dma((2,)), dma((2, n_fsdp)), dma((2, n_fsdp)), dma, dma((3,))],
        compiler_params=pltpu.CompilerParams(collective_id=0, has_side_effects=True),
        name='ids',
    )(tokens, gains, w_qkv, w_out, w_gu, w_dn)


def gather_kernel(n_tok, gid_ref, tgt_ref, table_ref, out_ref, buf, sems):
    width = table_ref.shape[2]
    n_step = n_tok // PICK

    def fetch(step, slot):
        for i in range(PICK):
            pltpu.make_async_copy(table_ref.at[gid_ref[step * PICK + i]], buf.at[slot, i], sems.at[slot]).start()

    for j in range(DEPTH - 1):
        fetch(j, j)

    def body(step, carry):
        slot = lax.rem(step, DEPTH)

        @pl.when(step + DEPTH - 1 < n_step)
        def _():
            fetch(step + DEPTH - 1, lax.rem(step + DEPTH - 1, DEPTH))
        arrived(buf.at[slot], sems.at[slot])
        rows = aligned(step * PICK, PICK, PICK)
        hot = (lax.broadcasted_iota(jnp.int32, (PICK, PICK * 8), 1) == tgt_ref[rows, :]).astype(BF16)
        got = jnp.dot(hot, buf[slot].reshape(PICK * 8, width), preferred_element_type=F32)
        out_ref[rows, :] = got.astype(BF16)
        return carry
    lax.fori_loop(0, n_step, body, 0)


def gather_table(ids, owned, table):
    n_tok = ids.shape[0]
    n_rows, width = table.shape
    gid = jnp.clip(ids, 0, n_rows - 1) // 8
    place = jnp.arange(n_tok, dtype=jnp.int32) % PICK
    tgt = jnp.where(owned, 8 * place + ids % 8, -1)[:, None]
    return pl.pallas_call(
        functools.partial(gather_kernel, n_tok),
        out_shape=jax.ShapeDtypeStruct((n_tok, width), BF16),
        in_specs=[pl.BlockSpec(memory_space=pltpu.SMEM), pl.BlockSpec(memory_space=pltpu.VMEM), pl.BlockSpec(memory_space=pl.ANY)],
        out_specs=pl.BlockSpec(memory_space=pltpu.VMEM),
        scratch_shapes=[pltpu.VMEM((DEPTH, PICK, 8, width), BF16), pltpu.SemaphoreType.DMA((DEPTH,))],
        compiler_params=pltpu.CompilerParams(vmem_limit_bytes=48 * 2**20),
        cost_estimate=pl.CostEstimate(flops=80 * 10**9, bytes_accessed=9 * n_tok * width * 2, transcendentals=0),
        name='rows',
    )(gid, tgt, table.reshape(n_rows // 8, 8, width))


def embed_kernel(side, pc, rows_ref, pq_ref, pe_ref, pd_ref, f0_ref, f1_ref, x_ref, q_ref, te_ref, td_ref, tf_ref,
                 got, peer, rp, sb, pk, xo,
                 got_sem, pack_sem, own_sem, d2d_s, d2d_r, z_s, z_r, f_s, f_r, push_s, push_r,
                 peer_s, peer_r, rs_s, rs_r, x_s, x_r):
    n_fsdp = pc.n_fsdp
    w = Where(side, n_fsdp)
    nz = w.nz
    far = nz // 2
    seq = got.shape[2]
    hw = got.shape[3]
    width = 2 * hw
    order = [far]
    for o in range(far - 1, 0, -1):
        order += [o, -o]
    order += [0]
    mine = aligned(w.c * hw, hw, LANES)
    other = aligned((1 - w.c) * hw, hw, LANES)
    for k in range(len(order)):
        dest = w.chip(order[k])
        pltpu.make_async_copy(rows_ref.at[dest, :, :, mine], got.at[dest], got_sem.at[k]).start()
    pltpu.make_async_copy(pq_ref, pk, pack_sem).start()
    greet([w.partner()] + [w.along_z(dz, core) for dz in (1, -1) for core in (0, 1)])
    dirs = (1, -1)

    for k in range(len(order)):
        dest = w.chip(order[k])
        remote(rows_ref.at[dest, :, :, other], peer.at[dest], peer_s.at[k], peer_r.at[k], w.partner()).start()

    sends = []
    arrived(pk, pack_sem)

    def first_hop():
        for i, dz in enumerate(dirs):
            cp = remote(pk, q_ref.at[w.f], z_s.at[i], z_r.at[i, w.c], w.along_z(dz, 1))
            cp.start()
            sends.append(cp)

    swaps = ((pk, q_ref.at[w.f]), (pe_ref, te_ref), (pd_ref, td_ref), (f0_ref, tf_ref.at[0]), (f1_ref, tf_ref.at[1]))
    own = [pltpu.make_async_copy(pk, q_ref.at[w.f], own_sem)]
    own += [remote(src, dst, d2d_s.at[j], d2d_r.at[j], w.partner()) for j, (src, dst) in enumerate(swaps)]


    def pair(dz):
        return q_ref.at[pl.ds(2 * w.chip(dz), 2)]

    def single(dz, i):
        return q_ref.at[pl.ds(2 * w.chip(dz) + i, 1)]

    def push(ref, i, h):
        remote(ref, ref, push_s.at[i, h], push_r, w.partner()).start()

    def forward(h):
        @pl.when(w.c == 1)
        def _():
            for i, dz in enumerate(dirs):
                if h == 1:
                    for core in range(2):
                        arrived(q_ref.at[2 * w.chip(-dz) + core], z_r.at[i, core])
                elif h < far:
                    arrived(pair(-dz * h), f_r.at[i, h])
                else:
                    arrived(single(-dz * h, i), f_r.at[i, h])
                if h < far - 1:
                    remote(pair(-dz * h), pair(-dz * h), f_s.at[i, h + 1], f_r.at[i, h + 1], w.along_z(dz, 1)).start()
                elif h == far - 1:
                    remote(single(-dz * h, i), single(-dz * h, i), f_s.at[i, h + 1], f_r.at[i, h + 1], w.along_z(dz, 1)).start()
                push(pair(-dz * h) if h < far else single(-dz * h, i), i, h)

    def addto(dst, terms):
        def one(r, carry):
            rows = aligned(r * 32, 32, 32)
            val = terms[0](rows)
            for term in terms[1:]:
                val = val + term(rows)
            dst(rows, val)
            return carry
        lax.fori_loop(0, seq // 32, one, 0)

    def rs_stage(k):
        o = order[k]
        dest = w.chip(o)
        arrived(got.at[dest], got_sem.at[k])
        arrived(peer.at[dest], peer_r.at[k])
        if o == 0:
            return
        for i, dz in enumerate(dirs):
            if o * dz < 0 and o != far:
                continue
            dist = abs(o)
            halves = (i,) if dist == far else (1 - i, i)
            for h in halves:
                terms = [lambda r, h=h: got[dest, h, r, :], lambda r, h=h: peer[dest, h, r, :]]
                if dist < far - 1 or (dist == far - 1 and h == i):
                    arrived(rp.at[i, dist, h], rs_r.at[i, dist, h])
                    terms.append(lambda r, h=h: rp[i, dist, h, r, :])

                def put(r, val, h=h):
                    sb[i, dist - 1, h, r, :] = val
                addto(put, terms)
                remote(sb.at[i, dist - 1, h], rp.at[i, dist - 1, h], rs_s.at[i, dist - 1, h], rs_r.at[i, dist - 1, h], w.along_z(dz, w.c)).start()

    for k in range(len(order) - 1):
        rs_stage(k)
        if k == 0:
            first_hop()
            for cp in own:
                cp.start()
        if k >= 2 and k - 1 <= far:
            forward(k - 1)
    rs_stage(len(order) - 1)
    for h in range(2):
        terms = [lambda r: got[w.z, h, r, :], lambda r: peer[w.z, h, r, :]]
        for i in range(2):
            arrived(rp.at[i, 0, h], rs_r.at[i, 0, h])
            terms.append(lambda r, i=i: rp[i, 0, h, r, :])

        def put(r, val):
            xo[h, r, :] = val
        addto(put, terms)
    home = pltpu.make_async_copy(xo, x_ref.at[:, :, mine], x_s.at[1])
    away = remote(xo, x_ref.at[:, :, mine], x_s.at[0], x_r, w.partner())
    home.start()
    away.start()

    for cp in sends:
        cp.wait_send()
    for cp in own:
        cp.wait()
    for k in range(len(order)):
        dest = w.chip(order[k])
        arrived(peer.at[dest], peer_s.at[k])
    for i in range(2):
        for dist in range(1, far + 1):
            for h in ((i,) if dist == far else (0, 1)):
                arrived(sb.at[i, dist - 1, h], rs_s.at[i, dist - 1, h])

    @pl.when(w.c == 1)
    def _():
        for i, dz in enumerate(dirs):
            for h in range(1, far + 1):
                ref = pair(-dz * h) if h < far else single(-dz * h, i)
                arrived(ref, push_s.at[i, h])
                if h < far:
                    arrived(pair(-dz * h) if h < far - 1 else single(-dz * h, i), f_s.at[i, h + 1])

    @pl.when(w.c == 0)
    def _():
        arrived(q_ref.at[pl.ds(0, n_fsdp - 2)], push_r)
    home.wait()
    away.wait()


def embed(side, pc, rows, pq, pe, pd, f0, f1):
    seq, width = rows.shape[2], rows.shape[3]
    nz = pc.n_fsdp // 2
    far = nz // 2
    hbm = pl.BlockSpec(memory_space=pl.ANY)
    dma = pltpu.SemaphoreType.DMA
    return pl.pallas_call(
        functools.partial(embed_kernel, side, pc),
        out_shape=(
            jax.ShapeDtypeStruct((2, seq, width), BF16),
            jax.ShapeDtypeStruct((pc.n_fsdp, pc.rows, pc.qkv), BF16),
            jax.ShapeDtypeStruct(pe.shape, BF16),
            jax.ShapeDtypeStruct(pd.shape, BF16),
            jax.ShapeDtypeStruct((2,) + f0.shape, BF16)),
        in_specs=[hbm] * 6,
        out_specs=(hbm,) * 5,
        scratch_shapes=[
            pltpu.VMEM((nz, 2, seq, width // 2), BF16),
            pltpu.VMEM((nz, 2, seq, width // 2), BF16),
            pltpu.VMEM((2, far, 2, seq, width // 2), BF16),
            pltpu.VMEM((2, far, 2, seq, width // 2), BF16),
            pltpu.VMEM((pc.rows, pc.qkv), BF16),
            pltpu.VMEM((2, seq, width // 2), BF16),
            dma((nz,)), dma, dma, dma((5,)), dma((5,)),
            dma((2,)), dma((2, 2)),
            dma((2, far + 1)), dma((2, far + 1)), dma((2, far + 1)), dma,
            dma((nz,)), dma((nz,)),
            dma((2, far, 2)), dma((2, far, 2)),
            dma((2,)), dma,
        ],
        compiler_params=pltpu.CompilerParams(collective_id=1, has_side_effects=True, vmem_limit_bytes=67043328),
        name='embed',
    )(rows, pq, pe, pd, f0, f1)


def layer_kernel(side, pc, head_dim, x_ref, q_ref, pe_ref, pd_ref, f0_ref, f1_ref, te_ref, td_ref, tf_ref, g1_ref, g2_ref, cos_ref, sin_ref, out_ref, k_ref, v_ref, w_ref,
                 xa, ca, xm, wg, wd, mm, pp, r1, r2, qf, kvb,
                 lsem, xs_s, xs_r, cs_s, cs_r, ms_s, ms_r, kv_s, kv_r, p1_s, p1_r, p2_s, p2_r, o_s, o_l, o_r,
                 zs, zr, ps, wch):
    h2 = ca
    n_fsdp = pc.n_fsdp
    w = Where(side, n_fsdp)
    far = w.nz // 2
    seq, width = xa.shape[2], xa.shape[3]
    rows_b = 2 * seq
    half = pc.dn_w // 2
    n_chunk = len(pc.chunks)
    last_gu = 5
    greet([w.partner(), w.along_z(1, w.c), w.along_z(-1, w.c)] + [w.square(rel, core) for rel in (1, 2, 3) for core in (0, 1)])
    dirs = (1, -1)

    def slim(t):
        off, cw = pc.chunks[t]
        return pl.ds(off - (pc.qkv if t < pc.early else pc.dn0), cw)

    def own_pieces(t):
        refs = (pe_ref, te_ref) if t < pc.early else (pd_ref, td_ref)
        return [ref.at[:, slim(t)] for ref in refs]

    def near_pieces(t, i):
        return [(f0_ref, f1_ref)[i].at[:, slim(t)], tf_ref.at[i, :, slim(t)]]

    def stream():
        def cols(t):
            off, cw = pc.chunks[t]
            return pl.ds(off - pc.qkv, cw)

        def pair(t, dz):
            return w_ref.at[pl.ds(2 * w.chip(dz), 2), :, cols(t)]

        def single(t, dz, i):
            return w_ref.at[pl.ds(2 * w.chip(dz) + i, 1), :, cols(t)]

        def piece(t, h, i):
            dz = dirs[i]
            return pair(t, -dz * h) if h < far else single(t, -dz * h, i)

        sent = []

        def hop(t, h):
            if t < 1 or t >= n_chunk or (h == 0 and t < pc.early):
                return
            ready = h == 1 and t < pc.early
            for i in range(2):
                dz = dirs[i]
                if h > 0 and not ready:
                    arrived(piece(t, h, i), zr.at[t, i, h])
                if h == far:
                    continue
                ref = pair(t, -dz * h) if h < far - 1 else single(t, -dz * h, i)
                sems = (zs.at[t, i, h], zr.at[t, i, h + 1], w.along_z(dz, 1))
                if h == 0 or ready:
                    pieces = near_pieces(t, i) if ready else own_pieces(t)
                    for src, core in zip(pieces, (1, 0)):
                        remote(src, w_ref.at[2 * w.chip(-dz * h) + core, :, cols(t)], *sems).start()
                else:
                    remote(ref, ref, *sems).start()
                sent.append((ref, zs.at[t, i, h]))
            if h > 0 and not ready:
                for i in range(2):
                    ref = piece(t, h, i)
                    remote(ref, ref, ps.at[t, i, h], wch.at[t], w.partner()).start()
                    sent.append((ref, ps.at[t, i, h]))

        for s in range(2, n_chunk + far):
            for h in range(far + 1):
                hop(s - h, h)
        for ref, sem in sent:
            arrived(ref, sem)
        kvw = 2 * (kvb.shape[2] // 4)
        for rel in range(4):
            arrived(k_ref.at[:, pl.ds(0, kvw)], kv_r.at[rel, 0])
            arrived(v_ref.at[:, pl.ds(0, kvw)], kv_r.at[rel, 1])
        for n in range(4):
            arrived(out_ref.at[:, pl.ds(n * pc.dn_w, pc.dn_w)], o_r.at[n])

    def compute():
        y, x = w.square(1, 0), w.square(2, 0)
        q4, kv4 = pc.q4, pc.kv4
        cols = {q: aligned((w.me ^ q) * pc.w4, pc.w4, LANES) for q in range(4)}
        sent = []

        def go(cp):
            cp.start()
            sent.append(cp)

        def load(t, dst, sem):
            off, cw = pc.chunks[t]
            c = pl.ds(off - pc.qkv, cw)
            near = t < pc.early
            arrived(w_ref.at[pl.ds(0, n_fsdp - (6 if near else 2)), :, c], wch.at[t])
            for dz in range(-1, w.nz - 1):
                two = pl.ds(2 * w.chip(dz), 2)
                if dz == 0 or (near and dz in (1, -1)):
                    pieces = own_pieces(t) if dz == 0 else near_pieces(t, 0 if dz == -1 else 1)
                    for core, src in enumerate(pieces):
                        pltpu.make_async_copy(src, dst.at[2 * w.chip(dz) + core], sem).start()
                else:
                    pltpu.make_async_copy(w_ref.at[two, :, c], dst.at[two], sem).start()

        own = pltpu.make_async_copy(x_ref, xa.at[0], lsem.at[0])
        own.start()
        first = pltpu.make_async_copy(q_ref, wg.at[:, :, pl.ds(0, pc.qkv)], lsem.at[1])
        first.start()
        go(remote(x_ref.at[0], xa.at[2, 0], xs_s.at[0], xs_r.at[2, 0], x))
        go(remote(x_ref.at[1], xa.at[1, 1], xs_s.at[1], xs_r.at[1, 1], y))
        go(remote(x_ref.at[1], xa.at[2, 1], xs_s.at[2], xs_r.at[2, 1], x))
        go(remote(x_ref.at[0], xa.at[1, 0], xs_s.at[3], xs_r.at[1, 0], y))
        own.wait()
        first.wait()

        def norm_into(dst, slot, load_rows, gain_ref):
            def one(i, carry):
                rows = aligned(i * 16, 16, 16)
                val = load_rows(rows, i).astype(F32)
                inv = lax.rsqrt(jnp.mean(val * val, axis=-1, keepdims=True) + NORM_EPS)
                dst[slot, rows, :] = (val * inv * gain_ref[...]).astype(BF16)
                return carry
            lax.fori_loop(0, rows_b // 16, one, 0)

        per = seq // 16
        lane = lax.broadcasted_iota(jnp.int32, (seq, LANES), 1)
        low_head = (lane % head_dim) < head_dim // 2
        first_head = lane < head_dim
        n_pair = q4 // LANES
        pair_per_kv = n_pair // 2

        def rope(t):
            swapped = jnp.where(low_head, pltpu.roll(t, LANES - head_dim // 2, 1), pltpu.roll(t, head_dim // 2, 1))
            return t * cos_ref[...] + swapped * sin_ref[...]

        def attend(slot):
            norm_into(mm, slot, lambda rows, i: xa[slot, i // per, aligned((i % per) * 16, 16, 16), :], g1_ref)
            def proj(nt, carry):
                c = aligned(nt * 256, 256, LANES)
                qf[:, c] = jnp.dot(mm[slot], wg[:, :, c].reshape(width, 256), preferred_element_type=F32)
                return carry
            lax.fori_loop(0, pc.qkv // 256, proj, 0)

            def one_seq(u, carry):
                rows = aligned(u * seq, seq, seq)
                k_f = rope(qf[rows, pl.ds(q4, LANES)])
                v_f = qf[rows, pl.ds(q4 + kv4, LANES)]
                kvb[slot, rows, pl.ds(0, LANES)] = k_f.astype(BF16)
                kvb[slot, rows, pl.ds(LANES, LANES)] = v_f.astype(BF16)
                k_r, v_r = pltpu.roll(k_f, head_dim, 1), pltpu.roll(v_f, head_dim, 1)
                zero = jnp.zeros_like(k_f)
                row = lax.broadcasted_iota(jnp.int32, (pair_per_kv * seq, seq), 0) % seq
                causal = row >= lax.broadcasted_iota(jnp.int32, (pair_per_kv * seq, seq), 1)
                for g in range(2):
                    k_lo, k_hi = (k_f, k_r) if g == 0 else (k_r, k_f)
                    v_lo, v_hi = (v_f, v_r) if g == 0 else (v_r, v_f)
                    kk = jnp.concatenate([jnp.where(first_head, k_lo, zero), jnp.where(first_head, zero, k_hi)], axis=0).astype(BF16)
                    vv = jnp.concatenate([jnp.where(first_head, v_lo, zero), jnp.where(first_head, zero, v_hi)], axis=0).astype(BF16)
                    qs = jnp.concatenate([rope(qf[rows, pl.ds((g * pair_per_kv + p) * LANES, LANES)]).astype(BF16) for p in range(pair_per_kv)], axis=0)
                    sc = lax.dot_general(qs, kk, (((1,), (1,)), ((), ())), preferred_element_type=F32) * (head_dim ** -0.5)
                    probs = []
                    for e in range(2):
                        part = jnp.where(causal, sc[:, e * seq:(e + 1) * seq], -jnp.inf)
                        part = jnp.exp(part - jnp.max(part, axis=-1, keepdims=True))
                        probs.append((part / jnp.sum(part, axis=-1, keepdims=True)).astype(BF16))
                    ctx = jnp.dot(jnp.concatenate(probs, axis=1), vv, preferred_element_type=F32).astype(BF16)
                    for p in range(pair_per_kv):
                        lanes = aligned(w.me * pc.w4 + (g * pair_per_kv + p) * LANES, LANES, LANES)
                        ca[slot, rows, lanes] = ctx[p * seq:(p + 1) * seq]
                return carry
            lax.fori_loop(0, 2, one_seq, 0)

        def spread(buf, slot, ss, rs):
            mine = buf.at[slot, :, cols[0]]
            go(remote(mine, buf.at[slot ^ 2, :, cols[0]], ss.at[slot, 1], rs.at[slot ^ 2, 1], x))
            go(remote(mine, buf.at[slot ^ 1, :, cols[0]], ss.at[slot, 0], rs.at[slot ^ 1, 0], y))

        def take(buf, slot, q, rs):
            arrived(buf.at[slot, :, cols[q]], rs.at[slot, q - 1 if q < 3 else 2])

        def relay(buf, slot, q, ss, rs):
            take(buf, slot, q, rs)
            ref = buf.at[slot, :, cols[q]]
            to, dev = (slot ^ 1, y) if q == 2 else (slot ^ 2, x)
            go(remote(ref, buf.at[to, :, cols[q]], ss.at[to, 2], rs.at[to, 2], dev))

        def send_kv(slot):
            mine = aligned(w.me * kv4, kv4, LANES)
            for core in range(2):
                for j, dst in enumerate((k_ref, v_ref)):
                    src = kvb.at[slot, pl.ds(core * seq, seq), pl.ds(j * kv4, kv4)]
                    if slot == 0 and core == 0:
                        cp = pltpu.make_async_copy(src, dst.at[:, mine], kv_s.at[slot, core, j])
                        cp.start()
                        local_kv.append(cp)
                    else:
                        go(remote(src, dst.at[:, mine], kv_s.at[slot, core, j], kv_r.at[slot, j], w.square(slot, core)))
        local_kv = []

        def here(slot, h):
            arrived(xa.at[slot, h], xs_r.at[slot, h])

        attend(0)
        here(2, 0)
        go(remote(xa.at[2, 0], xa.at[3, 0], xs_s.at[4], xs_r.at[3, 0], y))
        here(1, 1)
        go(remote(xa.at[1, 1], xa.at[3, 1], xs_s.at[5], xs_r.at[3, 1], x))
        spread(ca, 0, cs_s, cs_r)
        here(2, 1)
        attend(2)
        spread(ca, 2, cs_s, cs_r)
        here(1, 0)
        attend(1)
        spread(ca, 1, cs_s, cs_r)
        relay(ca, 2, 2, cs_s, cs_r)
        here(3, 0)
        here(3, 1)
        attend(3)
        spread(ca, 3, cs_s, cs_r)
        relay(ca, 0, 2, cs_s, cs_r)
        relay(ca, 0, 1, cs_s, cs_r)
        relay(ca, 2, 1, cs_s, cs_r)
        load(1, wd, lsem.at[0])
        for slot in range(4):
            send_kv(slot)
        arrived(wd, lsem.at[0])
        n_ctx = len(sent)

        def mid(slot):
            for q in (1, 2, 3):
                if q == 3 or slot in (1, 3):
                    take(ca, slot, q, cs_r)

            def one(nt, carry):
                c = aligned(nt * 256, 256, LANES)
                o = aligned(w.me * pc.w4 + nt * 256, 256, LANES)
                got = jnp.dot(ca[slot], wd[:, :, c].reshape(width, 256), preferred_element_type=F32)
                res = xa[slot, :, :, o].reshape(rows_b, 256).astype(F32)
                xm[slot, :, o] = (res + got).astype(BF16)
                return carry
            lax.fori_loop(0, pc.w4 // 256, one, 0)
            spread(xm, slot, ms_s, ms_r)

        mid(3)
        mid(1)
        mid(2)
        relay(xm, 1, 2, ms_s, ms_r)
        mid(0)
        relay(xm, 3, 2, ms_s, ms_r)
        relay(xm, 3, 1, ms_s, ms_r)
        relay(xm, 1, 1, ms_s, ms_r)
        for cp in sent[:n_ctx]:
            cp.wait_send()
        del sent[:n_ctx]
        for slot in (0, 2, 1, 3):
            for q in (1, 2, 3):
                if q == 3 or slot in (0, 2):
                    take(xm, slot, q, ms_r)
            norm_into(h2, slot, lambda rows, i, slot=slot: xm[slot, rows, :], g2_ref)

        gate_w = pc.gu_w // 2
        for b in range(4):
            load(2 + b, wg, lsem.at[b % 2])
            arrived(wg, lsem.at[b % 2])

            def one(j, carry):
                s, nt = j // (gate_w // 256), j % (gate_w // 256)
                act = h2[pl.ds(2 * s, 2)].reshape(2 * rows_b, width)
                gate = jnp.dot(act, wg[:, :, aligned(nt * 256, 256, LANES)].reshape(width, 256), preferred_element_type=F32)
                up = jnp.dot(act, wg[:, :, aligned(gate_w + nt * 256, 256, LANES)].reshape(width, 256), preferred_element_type=F32)
                val = (jax.nn.silu(gate) * up).astype(BF16)
                mm[pl.ds(2 * s, 2), :, aligned(b * gate_w + nt * 256, 256, LANES)] = val.reshape(2, rows_b, 256)
                return carry
            lax.fori_loop(0, 2 * (gate_w // 256), one, 0)

        h0, h1 = pl.ds(0, half), pl.ds(half, half)
        first_sends, home = {}, []

        def phase1(n):
            load(last_gu + 1 + n, wd, lsem.at[n % 2])
            for old in first_sends.get(n - 2, ()):
                old.wait_send()
            arrived(wd, lsem.at[n % 2])
            par = n % 2

            def one(j, carry):
                s, nt = j // (pc.dn_w // 256), j % (pc.dn_w // 256)
                c = aligned(nt * 256, 256, LANES)
                act = mm[pl.ds(2 * s, 2)].reshape(2 * rows_b, mm.shape[2])
                got = jnp.dot(act, wd[:, :, c].reshape(mm.shape[2], 256), preferred_element_type=F32)
                pp[par, pl.ds(2 * s, 2), :, c] = got.reshape(2, rows_b, 256)
                return carry
            lax.fori_loop(0, 2 * (pc.dn_w // 256), one, 0)
            first_sends[n] = []
            for path, dev, cc, rels in ((0, x, h0, (2, 3)), (1, y, h1, (1, 3))):
                for j, rel in enumerate(rels):
                    cp = remote(pp.at[par, rel, :, cc], r1.at[n, path, j], p1_s.at[n, path, j], p1_r.at[n, path, j], dev)
                    cp.start()
                    first_sends[n].append(cp)

        def phase2(n):
            par = n % 2
            for path, dev, cc, rel in ((0, y, h0, 1), (1, x, h1, 2)):
                arrived(r1.at[n, path, 1], p1_r.at[n, path, 1])
                r1[n, path, 1] = pp[par, rel, :, cc] + r1[n, path, 1]
                go(remote(r1.at[n, path, 1], r2.at[n, path], p2_s.at[n, path], p2_r.at[n, path], dev))
            for path, cc in ((0, h0), (1, h1)):
                arrived(r1.at[n, path, 0], p1_r.at[n, path, 0])
                r1[n, path, 0] = pp[par, 0, :, cc] + r1[n, path, 0]

        def phase3(n):
            for path in range(2):
                arrived(r2.at[n, path], p2_r.at[n, path])
                c = pl.ds(n * pc.dn_w + path * half, half)
                total = xm[0, :, c].astype(F32) + (r1[n, path, 0] + r2[n, path])
                xm[0, :, c] = total.astype(BF16)
            c = pl.ds(n * pc.dn_w, pc.dn_w)
            go(remote(xm.at[0, pl.ds(seq, seq), c], out_ref.at[:, c], o_s.at[n], o_r.at[n], w.partner()))
            cp = pltpu.make_async_copy(xm.at[0, pl.ds(0, seq), c], out_ref.at[:, c], o_l.at[n])
            cp.start()
            home.append(cp)

        for cp in sent:
            cp.wait_send()
        sent.clear()
        for n in range(4):
            phase1(n)
            if n >= 1:
                phase2(n - 1)
            if n >= 2:
                phase3(n - 2)
        phase2(3)
        phase3(2)
        phase3(3)

        for cp in sent:
            cp.wait_send()
        for n in (2, 3):
            for cp in first_sends[n]:
                cp.wait_send()
        for cp in local_kv + home:
            cp.wait()
        for rel in (1, 2, 3):
            arrived(k_ref.at[:, pl.ds(0, kv4)], kv_r.at[rel, 0])
            arrived(v_ref.at[:, pl.ds(0, kv4)], kv_r.at[rel, 1])

    pl.when(w.c == 1)(stream)
    pl.when(w.c == 0)(compute)


def layer(side, pc, head_dim, x, q_all, near, g1, g2, cos_tab, sin_tab):
    _, seq, width = x.shape
    rows_b = 2 * seq
    kv_width = 4 * pc.kv4
    n_chunk = len(pc.chunks)
    far = pc.n_fsdp // 4
    ff4 = pc.f4 * pc.n_fsdp
    half = pc.dn_w // 2
    hbm = pl.BlockSpec(memory_space=pl.ANY)
    vmem = pl.BlockSpec(memory_space=pltpu.VMEM)
    dma = pltpu.SemaphoreType.DMA
    return pl.pallas_call(
        functools.partial(layer_kernel, side, pc, head_dim),
        out_shape=(
            jax.ShapeDtypeStruct((seq, width), BF16),
            jax.ShapeDtypeStruct((seq, kv_width), BF16),
            jax.ShapeDtypeStruct((seq, kv_width), BF16),
            jax.ShapeDtypeStruct((pc.n_fsdp, pc.rows, pc.late), BF16)),
        in_specs=[hbm] * (2 + len(near)) + [vmem, vmem, vmem, vmem],
        out_specs=(hbm, hbm, hbm, hbm),
        scratch_shapes=[
            pltpu.VMEM((4, 2, seq, width), BF16),
            pltpu.VMEM((4, rows_b, width), BF16),
            pltpu.VMEM((4, rows_b, width), BF16),
            pltpu.VMEM((pc.n_fsdp, pc.rows, pc.gu_w), BF16),
            pltpu.VMEM((pc.n_fsdp, pc.rows, pc.dn_w), BF16),
            pltpu.VMEM((4, rows_b, max(ff4, width)), BF16),
            pltpu.VMEM((2, 4, rows_b, pc.dn_w), F32),
            pltpu.VMEM((4, 2, 2, rows_b, half), F32),
            pltpu.VMEM((4, 2, rows_b, half), F32),
            pltpu.VMEM((rows_b, pc.qkv), F32),
            pltpu.VMEM((4, rows_b, 2 * pc.kv4), BF16),
            dma((2,)),
            dma((6,)), dma((4, 2)),
            dma((4, 3)), dma((4, 3)),
            dma((4, 3)), dma((4, 3)),
            dma((4, 2, 2)), dma((4, 2)),
            dma((4, 2, 2)), dma((4, 2, 2)),
            dma((4, 2)), dma((4, 2)),
            dma((4,)), dma((4,)), dma((4,)),
            dma((n_chunk, 2, far + 1)), dma((n_chunk, 2, far + 1)), dma((n_chunk, 2, far + 1)), dma((n_chunk,)),
        ],
        compiler_params=pltpu.CompilerParams(collective_id=2, has_side_effects=True, vmem_limit_bytes=67043328),
        name='layer',
    )(x, q_all, *near, g1, g2, cos_tab, sin_tab)


def solution(mesh):
    batch_axes = ('dp', 'fsdp')
    row_spec = P('fsdp', None)
    n_dp = mesh.shape['dp']
    n_fsdp = mesh.shape['fsdp']
    side = math.isqrt(n_dp)

    def device_step(tokens, embed_table, norm_attn, w_qkv, w_out, norm_mlp, w_gate_up, w_down, rope_scale):
        seq = tokens.shape[1]
        shard_rows, width = embed_table.shape
        head_dim = 2 * rope_scale.shape[0]
        rows = w_out.shape[0]
        q_width = rows * n_fsdp
        kv_width = (w_qkv.shape[1] - q_width) // 2
        pc = Pieces(rows, q_width // 4, kv_width // 4, width // 4, w_down.shape[0] // 4, n_fsdp, width)

        gains = jnp.stack([norm_attn, norm_mlp]).astype(F32)
        ids, gains, pq, pe, pd = gather_ids(side, pc, tokens, gains, w_qkv, w_out, w_gate_up, w_down)
        f0, f1 = [lax.ppermute(pe, 'fsdp', [(i, (i + 2 * dz) % n_fsdp) for i in range(n_fsdp)]) for dz in (1, -1)]
        ids = ids.reshape(-1) - lax.axis_index('fsdp') * shard_rows
        owned = (ids >= 0) & (ids < shard_rows)
        table_rows = gather_table(ids, owned, embed_table)
        g1 = gains[:, 0].reshape(1, width)
        g2 = gains[:, 1].reshape(1, width)

        freq_expo = jnp.arange(head_dim // 2, dtype=F32) * (2.0 / head_dim)
        inv_freq = 1.0 / (rope_scale * jnp.power(ROPE_THETA, freq_expo))
        angles = jnp.arange(seq, dtype=F32)[:, None] * inv_freq[None, :]
        cos_tab, sin_tab = jnp.cos(angles), jnp.sin(angles)
        reps = LANES // head_dim
        cos_tab = jnp.concatenate([cos_tab, cos_tab] * reps, axis=1)
        sin_tab = jnp.concatenate([-sin_tab, sin_tab] * reps, axis=1)

        x, q_all, te, td, tf = embed(side, pc, table_rows.reshape(n_fsdp // 2, 2, seq, width), pq, pe, pd, f0, f1)
        out, k, v, _ = layer(side, pc, head_dim, x, q_all, (pe, pd, f0, f1, te, td, tf), g1, g2, cos_tab, sin_tab)
        heads = (1, seq, kv_width // head_dim, head_dim)
        return out[None], k.reshape(heads), v.reshape(heads)

    return jax.shard_map(
        device_step,
        mesh=mesh,
        in_specs=(P(batch_axes, None), row_spec, P('fsdp'), row_spec, row_spec, P('fsdp'), row_spec, row_spec, P(None)),
        out_specs=(P(batch_axes, None, None), P(batch_axes, None, None, None), P(batch_axes, None, None, None)),
        check_vma=False,
    )
```

```python
import functools
import math

import jax
import jax.numpy as jnp
from jax import lax
from jax.experimental import pallas as pl
from jax.experimental.pallas import tpu as pltpu
from jax.sharding import PartitionSpec as P

NORM_EPS = 1e-5
ROPE_THETA = 10000.0
PICK = 32
DEPTH = 4
LANES = 128
MESH = pl.DeviceIdType.MESH
BF16 = jnp.bfloat16
F32 = jnp.float32


def aligned(start, size, step):
    return pl.ds(pl.multiple_of(start, step), size)


class Where:
    def __init__(self, side, n_fsdp):
        self.side = side
        self.nz = n_fsdp // 2
        self.dp = lax.axis_index('dp')
        self.f = lax.axis_index('fsdp')
        self.z = self.f // 2
        self.c = self.f % 2
        self.px = self.dp // side
        self.py = self.dp % side
        self.me = 2 * (self.px % 2) + self.py % 2

    def chip(self, dz):
        return lax.rem(self.z + dz + self.nz, self.nz)

    def along_z(self, dz, core):
        return (self.dp, 2 * self.chip(dz) + core)

    def partner(self):
        return (self.dp, 2 * self.z + 1 - self.c)

    def square(self, rel, core):
        px = self.px + (1 - 2 * (self.px % 2)) if rel & 2 else self.px
        py = self.py + (1 - 2 * (self.py % 2)) if rel & 1 else self.py
        return (px * self.side + py, 2 * self.z + core)


def greet(devices):
    barrier = pltpu.get_barrier_semaphore()
    for dev in devices:
        pl.semaphore_signal(barrier, inc=1, device_id=dev, device_id_type=MESH)
    pl.semaphore_wait(barrier, len(devices))


def remote(src, dst, ssem, rsem, dev):
    return pltpu.make_async_remote_copy(src_ref=src, dst_ref=dst, send_sem=ssem, recv_sem=rsem, device_id=dev, device_id_type=MESH)


def arrived(ref, sem):
    pltpu.make_async_copy(ref, ref, sem).wait()


def ids_kernel(side, pc, tok_ref, gain_ref, w_qkv, w_out, w_gu, w_dn, ids_ref, gains_ref, pq_ref, pe_ref, pd_ref,
               pk, lsem, ssem, rsem, pack_sem, store_sem):
    n_fsdp = pc.n_fsdp
    w = Where(side, n_fsdp)
    pack_copies(pc, w.me, pk, w_qkv, w_out, w_gu, w_dn, pack_sem)
    greet([(w.dp, lax.rem(w.f + k, n_fsdp)) for k in range(1, n_fsdp)])
    own = [pltpu.make_async_copy(tok_ref, ids_ref.at[w.f], lsem.at[0]),
           pltpu.make_async_copy(gain_ref, gains_ref.at[w.f], lsem.at[1])]
    for cp in own:
        cp.start()
    sent = []
    for k in range(1, n_fsdp):
        dev = (w.dp, lax.rem(w.f + k, n_fsdp))
        for j, (src, dst) in enumerate(((tok_ref, ids_ref), (gain_ref, gains_ref))):
            cp = remote(src, dst.at[w.f], ssem.at[j, k], rsem.at[j, k], dev)
            cp.start()
            sent.append(cp)
    arrived(pk, pack_sem)
    lo = 0
    stores = []
    for j, ref in enumerate((pq_ref, pe_ref, pd_ref)):
        stores.append(pltpu.make_async_copy(pk.at[:, pl.ds(lo, ref.shape[1])], ref, store_sem.at[j]))
        stores[-1].start()
        lo += ref.shape[1]
    for cp in own + stores:
        cp.wait()
    for cp in sent:
        cp.wait_send()
    for k in range(1, n_fsdp):
        src = lax.rem(w.f - k + n_fsdp, n_fsdp)
        arrived(ids_ref.at[src], rsem.at[0, k])
        arrived(gains_ref.at[src], rsem.at[1, k])


class Pieces:
    def __init__(self, rows, q4, kv4, w4, f4, n_fsdp, width):
        self.rows = rows
        self.q4, self.kv4, self.w4, self.f4 = q4, kv4, w4, f4
        self.n_fsdp = n_fsdp
        self.width = width
        self.qkv = q4 + 2 * kv4
        self.gu0 = self.qkv + w4
        self.gu_w = 2 * f4 * n_fsdp // 4
        self.dn0 = self.gu0 + 4 * self.gu_w
        self.dn_w = width // 4
        self.total = self.dn0 + width
        self.late = self.total - self.qkv
        self.chunks = [(0, self.qkv), (self.qkv, w4)]
        self.chunks += [(self.gu0 + b * self.gu_w, self.gu_w) for b in range(4)]
        self.chunks += [(self.dn0 + n * self.dn_w, self.dn_w) for n in range(4)]
        self.early = 6


def pack_copies(pc, me, pk, w_qkv, w_out, w_gu, w_dn, sem):
    q4, kv4, w4, f4 = pc.q4, pc.kv4, pc.w4, pc.f4
    first = [
        (w_qkv.at[:, aligned(me * q4, q4, LANES)], pk.at[:, pl.ds(0, q4)]),
        (w_qkv.at[:, aligned(4 * q4 + me * kv4, kv4, LANES)], pk.at[:, pl.ds(q4, kv4)]),
        (w_qkv.at[:, aligned(4 * q4 + 4 * kv4 + me * kv4, kv4, LANES)], pk.at[:, pl.ds(q4 + kv4, kv4)]),
    ]
    for src, dst in first:
        pltpu.make_async_copy(src, dst, sem).start()
    pltpu.make_async_copy(w_out.at[:, aligned(me * w4, w4, LANES)], pk.at[:, pl.ds(pc.qkv, w4)], sem).start()
    ff = 4 * f4 * pc.n_fsdp
    for d in range(pc.n_fsdp):
        b, k = d // 4, d % 4
        for part in range(2):
            src = w_gu.at[:, aligned(part * ff + d * 4 * f4 + me * f4, f4, LANES)]
            dst = pk.at[:, pl.ds(pc.gu0 + b * pc.gu_w + part * (pc.gu_w // 2) + k * f4, f4)]
            pltpu.make_async_copy(src, dst, sem).start()
    pltpu.make_async_copy(w_dn.at[aligned(me * f4, f4, LANES), :], pk.at[:, pl.ds(pc.dn0, pc.width)], sem).start()


def gather_ids(side, pc, tokens, gains, w_qkv, w_out, w_gu, w_dn):
    n_fsdp = pc.n_fsdp
    vmem, hbm = pl.BlockSpec(memory_space=pltpu.VMEM), pl.BlockSpec(memory_space=pl.ANY)
    dma = pltpu.SemaphoreType.DMA
    return pl.pallas_call(
        functools.partial(ids_kernel, side, pc),
        out_shape=(
            jax.ShapeDtypeStruct((n_fsdp,) + tokens.shape, tokens.dtype),
            jax.ShapeDtypeStruct((n_fsdp,) + gains.shape, gains.dtype),
            jax.ShapeDtypeStruct((pc.rows, pc.qkv), BF16),
            jax.ShapeDtypeStruct((pc.rows, pc.dn0 - pc.qkv), BF16),
            jax.ShapeDtypeStruct((pc.rows, pc.width), BF16)),
        in_specs=[vmem, vmem, hbm, hbm, hbm, hbm],
        out_specs=(vmem, vmem, hbm, hbm, hbm),
        scratch_shapes=[pltpu.VMEM((pc.rows, pc.total), BF16), dma((2,)), dma((2, n_fsdp)), dma((2, n_fsdp)), dma, dma((3,))],
        compiler_params=pltpu.CompilerParams(collective_id=0, has_side_effects=True),
        name='ids',
    )(tokens, gains, w_qkv, w_out, w_gu, w_dn)


def gather_kernel(n_tok, gid_ref, tgt_ref, table_ref, out_ref, buf, sems):
    width = table_ref.shape[2]
    n_step = n_tok // PICK

    def fetch(step, slot):
        for i in range(PICK):
            pltpu.make_async_copy(table_ref.at[gid_ref[step * PICK + i]], buf.at[slot, i], sems.at[slot]).start()

    for j in range(DEPTH - 1):
        fetch(j, j)

    def body(step, carry):
        slot = lax.rem(step, DEPTH)

        @pl.when(step + DEPTH - 1 < n_step)
        def _():
            fetch(step + DEPTH - 1, lax.rem(step + DEPTH - 1, DEPTH))
        arrived(buf.at[slot], sems.at[slot])
        rows = aligned(step * PICK, PICK, PICK)
        hot = (lax.broadcasted_iota(jnp.int32, (PICK, PICK * 8), 1) == tgt_ref[rows, :]).astype(BF16)
        got = jnp.dot(hot, buf[slot].reshape(PICK * 8, width), preferred_element_type=F32)
        out_ref[rows, :] = got.astype(BF16)
        return carry
    lax.fori_loop(0, n_step, body, 0)


def gather_table(ids, owned, table):
    n_tok = ids.shape[0]
    n_rows, width = table.shape
    gid = jnp.where(owned, ids // 8, jnp.arange(n_tok, dtype=jnp.int32) % (n_rows // 8))
    place = jnp.arange(n_tok, dtype=jnp.int32) % PICK
    tgt = jnp.where(owned, 8 * place + ids % 8, -1)[:, None]
    return pl.pallas_call(
        functools.partial(gather_kernel, n_tok),
        out_shape=jax.ShapeDtypeStruct((n_tok, width), BF16),
        in_specs=[pl.BlockSpec(memory_space=pltpu.SMEM), pl.BlockSpec(memory_space=pltpu.VMEM), pl.BlockSpec(memory_space=pl.ANY)],
        out_specs=pl.BlockSpec(memory_space=pltpu.VMEM),
        scratch_shapes=[pltpu.VMEM((DEPTH, PICK, 8, width), BF16), pltpu.SemaphoreType.DMA((DEPTH,))],
        compiler_params=pltpu.CompilerParams(vmem_limit_bytes=48 * 2**20),
        cost_estimate=pl.CostEstimate(flops=80 * 10**9, bytes_accessed=9 * n_tok * width * 2, transcendentals=0),
        name='rows',
    )(gid, tgt, table.reshape(n_rows // 8, 8, width))


def embed_kernel(side, pc, rows_ref, pq_ref, n0_ref, n1_ref, pe_ref, pd_ref, f0_ref, f1_ref, xa_ref, xb_ref, q_ref, te_ref, td_ref, tf_ref,
                 got, peer, rp, sb, pk, xo,
                 got_sem, pack_sem, own_sem, d2d_s, d2d_r, f_s, f_r, push_s, push_r,
                 peer_s, peer_r, rs_s, rs_r, home_sem, x_s, x_r):
    n_fsdp = pc.n_fsdp
    w = Where(side, n_fsdp)
    nz = w.nz
    far = nz // 2
    seq = got.shape[2]
    hw = got.shape[3]
    width = 2 * hw
    order = [far]
    for o in range(far - 1, 0, -1):
        order += [o, -o]
    order += [0]
    mine = aligned(w.c * hw, hw, LANES)
    other = aligned((1 - w.c) * hw, hw, LANES)
    for k in range(len(order)):
        dest = w.chip(order[k])
        pltpu.make_async_copy(rows_ref.at[dest, :, :, mine], got.at[dest], got_sem.at[k]).start()
    for j, src in enumerate((pq_ref, n0_ref, n1_ref)):
        pltpu.make_async_copy(src, pk.at[j], pack_sem.at[j]).start()
    greet([w.partner()] + [w.along_z(dz, core) for dz in (1, -1) for core in (0, 1)] + [w.square(rel, core) for rel in (1, 2) for core in (0, 1)])
    dirs = (1, -1)

    for k in range(len(order)):
        dest = w.chip(order[k])
        remote(rows_ref.at[dest, :, :, other], peer.at[dest], peer_s.at[k], peer_r.at[k], w.partner()).start()

    here_q = (2 * w.z + w.c, 2 * w.chip(-1) + w.c, 2 * w.chip(1) + w.c)
    swaps = [(src, q_ref.at[here_q[j]]) for j, src in enumerate((pq_ref, n0_ref, n1_ref))]
    swaps += [(pe_ref, te_ref), (pd_ref, td_ref), (f0_ref, tf_ref.at[0]), (f1_ref, tf_ref.at[1])]
    own = [remote(src, dst, d2d_s.at[j], d2d_r.at[j], w.partner()) for j, (src, dst) in enumerate(swaps)]


    def pair(dz):
        return q_ref.at[pl.ds(2 * w.chip(dz), 2)]

    def single(dz, i):
        return q_ref.at[pl.ds(2 * w.chip(dz) + i, 1)]

    def push(ref, i, h):
        remote(ref, ref, push_s.at[i, h], push_r, w.partner()).start()

    local = []

    def forward(h):
        @pl.when(w.c == 1)
        def _():
            for i, dz in enumerate(dirs):
                if h == 1:
                    local[1 + i].wait()
                    own[1 + i].wait_recv()
                elif h < far:
                    arrived(pair(-dz * h), f_r.at[i, h])
                else:
                    arrived(single(-dz * h, i), f_r.at[i, h])
                if h < far - 1:
                    remote(pair(-dz * h), pair(-dz * h), f_s.at[i, h + 1], f_r.at[i, h + 1], w.along_z(dz, 1)).start()
                elif h == far - 1:
                    remote(single(-dz * h, i), single(-dz * h, i), f_s.at[i, h + 1], f_r.at[i, h + 1], w.along_z(dz, 1)).start()
                if h > 1:
                    push(pair(-dz * h) if h < far else single(-dz * h, i), i, h)

    def addto(dst, terms, q):
        def one(r, carry):
            rows = aligned(q * (seq // 2) + r * 32, 32, 32)
            val = terms[0](rows)
            for term in terms[1:]:
                val = val + term(rows)
            dst(rows, val)
            return carry
        lax.fori_loop(0, seq // 64, one, 0)

    def part(ref, q):
        return ref.at[pl.ds(q * (seq // 2), seq // 2)]

    def rs_stage(k, h):
        o = order[k]
        dest = w.chip(o)
        if h == 0:
            arrived(got.at[dest], got_sem.at[k])
            arrived(peer.at[dest], peer_r.at[k])
        if o == 0:
            return
        dist = abs(o)
        for i, dz in enumerate(dirs):
            if (o * dz < 0 and o != far) or (dist == far and h != i):
                continue
            for q in range(2):
                terms = [lambda r: got[dest, h, r, :], lambda r: peer[dest, h, r, :]]
                if dist < far - 1 or (dist == far - 1 and h == i):
                    arrived(part(rp.at[i, dist, h], q), rs_r.at[i, dist, h, q])
                    terms.append(lambda r, i=i: rp[i, dist, h, r, :])

                def put(r, val, i=i):
                    sb[i, dist - 1, h, r, :] = val
                addto(put, terms, q)
                remote(part(sb.at[i, dist - 1, h], q), part(rp.at[i, dist - 1, h], q), rs_s.at[i, dist - 1, h, q],
                       rs_r.at[i, dist - 1, h, q], w.along_z(dz, w.c)).start()

    def finish(h):
        for q in range(2):
            terms = [lambda r: got[w.z, h, r, :], lambda r: peer[w.z, h, r, :]]
            for i in range(2):
                arrived(part(rp.at[i, 0, h], q), rs_r.at[i, 0, h, q])
                terms.append(lambda r, i=i: rp[i, 0, h, r, :])

            def put(r, val):
                xo[h, r, :] = val
            addto(put, terms, q)
        dst = (xa_ref.at[0] if h == 0 else xb_ref).at[:, mine]

        @pl.when(w.c == 0)
        def _():
            pltpu.make_async_copy(xo.at[h], dst, home_sem.at[h]).start()

        @pl.when(w.c == 1)
        def _():
            remote(xo.at[h], dst, home_sem.at[h], x_r.at[0, h], w.partner()).start()

    sides = ((2, w.square(2, 0)), (1, w.square(1, 0)))
    spread = [remote(xo.at[0], xa_ref.at[rel, :, mine], x_s.at[j], x_r.at[rel, w.c], dev) for j, (rel, dev) in enumerate(sides)]
    col = [pl.ds(j * hw, hw) for j in range(2)]
    relay = [remote(xa_ref.at[rel, :, col[j]], xa_ref.at[3, :, col[j]], x_s.at[2 + j], x_r.at[3, j], sides[1 - j][1]) for j, (rel, _) in enumerate(sides)]

    for j in range(3):
        arrived(pk.at[j], pack_sem.at[j])
        local.append(pltpu.make_async_copy(pk.at[j], q_ref.at[here_q[j]], own_sem.at[j]))
    last = len(order) - 1
    for k in range(last + 1):
        rs_stage(k, 0)
        if k == 0:
            for cp in own[:3] + local:
                cp.start()
        if k == 2:
            for cp in own[3:]:
                cp.start()
            forward(1)
        if k == 5:
            forward(2)
    for k in range(3):
        rs_stage(k, 1)
    finish(0)
    for cp in spread:
        cp.start()
    for k in range(3, last + 1):
        rs_stage(k, 1)
        if k == 4:
            forward(3)
        if k == last - 1:
            @pl.when(w.c == 0)
            def _():
                for j, (rel, _) in enumerate(sides):
                    arrived(xa_ref.at[rel, :, col[j]], x_r.at[rel, j])
                    relay[j].start()
    forward(4)
    finish(1)

    for cp in own[:1] + own[3:]:
        cp.wait()
    for cp in own[1:3]:
        cp.wait_send()
    local[0].wait()
    for cp in spread:
        cp.wait_send()
    for k in range(len(order)):
        dest = w.chip(order[k])
        arrived(peer.at[dest], peer_s.at[k])
    for i in range(2):
        for dist in range(1, far + 1):
            for h in ((i,) if dist == far else (0, 1)):
                for q in range(2):
                    arrived(part(sb.at[i, dist - 1, h], q), rs_s.at[i, dist - 1, h, q])

    @pl.when(w.c == 1)
    def _():
        for i, dz in enumerate(dirs):
            for h in range(1, far + 1):
                ref = pair(-dz * h) if h < far else single(-dz * h, i)
                if h > 1:
                    arrived(ref, push_s.at[i, h])
                if h < far:
                    arrived(pair(-dz * h) if h < far - 1 else single(-dz * h, i), f_s.at[i, h + 1])

    @pl.when(w.c == 0)
    def _():
        arrived(q_ref.at[pl.ds(0, n_fsdp - 6)], push_r)
        for j in (1, 2):
            local[j].wait()
            own[j].wait_recv()
        arrived(xa_ref.at[0, :, col[1]], x_r.at[0, 0])
        arrived(xb_ref.at[:, col[1]], x_r.at[0, 1])
        arrived(xa_ref.at[2, :, col[1]], x_r.at[2, 1])
        arrived(xa_ref.at[1, :, col[0]], x_r.at[1, 0])
        for j in range(2):
            arrived(xa_ref.at[3, :, col[j]], x_r.at[3, j])
            relay[j].wait_send()
    for h in range(2):
        arrived(xo.at[h], home_sem.at[h])


def embed(side, pc, rows, pq, n0, n1, pe, pd, f0, f1):
    seq, width = rows.shape[2], rows.shape[3]
    nz = pc.n_fsdp // 2
    far = nz // 2
    hbm = pl.BlockSpec(memory_space=pl.ANY)
    dma = pltpu.SemaphoreType.DMA
    return pl.pallas_call(
        functools.partial(embed_kernel, side, pc),
        out_shape=(
            jax.ShapeDtypeStruct((4, seq, width), BF16),
            jax.ShapeDtypeStruct((seq, width), BF16),
            jax.ShapeDtypeStruct((pc.n_fsdp, pc.rows, pc.qkv), BF16),
            jax.ShapeDtypeStruct(pe.shape, BF16),
            jax.ShapeDtypeStruct(pd.shape, BF16),
            jax.ShapeDtypeStruct((2,) + f0.shape, BF16)),
        in_specs=[hbm] * 8,
        out_specs=(hbm,) * 6,
        scratch_shapes=[
            pltpu.VMEM((nz, 2, seq, width // 2), BF16),
            pltpu.VMEM((nz, 2, seq, width // 2), BF16),
            pltpu.VMEM((2, far, 2, seq, width // 2), BF16),
            pltpu.VMEM((2, far, 2, seq, width // 2), BF16),
            pltpu.VMEM((3, pc.rows, pc.qkv), BF16),
            pltpu.VMEM((2, seq, width // 2), BF16),
            dma((nz,)), dma((3,)), dma((3,)), dma((7,)), dma((7,)),
            dma((2, far + 1)), dma((2, far + 1)), dma((2, far + 1)), dma,
            dma((nz,)), dma((nz,)),
            dma((2, far, 2, 2)), dma((2, far, 2, 2)),
            dma((2,)), dma((4,)), dma((4, 2)),
        ],
        compiler_params=pltpu.CompilerParams(collective_id=1, has_side_effects=True, vmem_limit_bytes=67043328),
        name='embed',
    )(rows, pq, n0, n1, pe, pd, f0, f1)


def layer_kernel(side, pc, head_dim, x_ref, xb_ref, q_ref, pe_ref, pd_ref, f0_ref, f1_ref, te_ref, td_ref, tf_ref, g1_ref, g2_ref, cos_ref, sin_ref, out_ref, k_ref, v_ref, w_ref,
                 xa, ca, xm, wg, wd, mm, pp, r1, r2, qf, kvb,
                 lsem, xs_s, xs_r, cs_s, cs_r, ms_s, ms_r, kv_s, kv_r, p1_s, p1_r, p2_s, p2_r, o_s, o_l, o_r,
                 zs, zr, ps, wch):
    h2 = ca
    n_fsdp = pc.n_fsdp
    w = Where(side, n_fsdp)
    far = w.nz // 2
    seq, width = xa.shape[2], xa.shape[3]
    rows_b = 2 * seq
    half = pc.dn_w // 2
    n_chunk = len(pc.chunks)
    last_gu = 5
    greet([w.partner(), w.along_z(1, w.c), w.along_z(-1, w.c)] + [w.square(rel, core) for rel in (1, 2, 3) for core in (0, 1)])
    dirs = (1, -1)

    def slim(t):
        off, cw = pc.chunks[t]
        return pl.ds(off - (pc.qkv if t < pc.early else pc.dn0), cw)

    def own_pieces(t):
        refs = (pe_ref, te_ref) if t < pc.early else (pd_ref, td_ref)
        return [ref.at[:, slim(t)] for ref in refs]

    def near_pieces(t, i):
        return [(f0_ref, f1_ref)[i].at[:, slim(t)], tf_ref.at[i, :, slim(t)]]

    def stream():
        def cols(t):
            off, cw = pc.chunks[t]
            return pl.ds(off - pc.qkv, cw)

        def pair(t, dz):
            return w_ref.at[pl.ds(2 * w.chip(dz), 2), :, cols(t)]

        def single(t, dz, i):
            return w_ref.at[pl.ds(2 * w.chip(dz) + i, 1), :, cols(t)]

        def piece(t, h, i):
            dz = dirs[i]
            return pair(t, -dz * h) if h < far else single(t, -dz * h, i)

        sent = []

        def hop(t, h):
            if t < 1 or t >= n_chunk or (h == 0 and t < pc.early):
                return
            ready = h == 1 and t < pc.early
            for i in range(2):
                dz = dirs[i]
                if h > 0 and not ready:
                    arrived(piece(t, h, i), zr.at[t, i, h])
                if h == far:
                    continue
                ref = pair(t, -dz * h) if h < far - 1 else single(t, -dz * h, i)
                sems = (zs.at[t, i, h], zr.at[t, i, h + 1], w.along_z(dz, 1))
                if h == 0 or ready:
                    pieces = near_pieces(t, i) if ready else own_pieces(t)
                    for src, core in zip(pieces, (1, 0)):
                        remote(src, w_ref.at[2 * w.chip(-dz * h) + core, :, cols(t)], *sems).start()
                else:
                    remote(ref, ref, *sems).start()
                sent.append((ref, zs.at[t, i, h]))
            if h > 0 and not ready:
                for i in range(2):
                    ref = piece(t, h, i)
                    remote(ref, ref, ps.at[t, i, h], wch.at[t], w.partner()).start()
                    sent.append((ref, ps.at[t, i, h]))

        for s in range(2, n_chunk + far):
            for h in range(far + 1):
                hop(s - h, h)
        for ref, sem in sent:
            arrived(ref, sem)
        kvw = 2 * (kvb.shape[2] // 4)
        for rel in range(4):
            arrived(k_ref.at[:, pl.ds(0, kvw)], kv_r.at[rel, 0])
            arrived(v_ref.at[:, pl.ds(0, kvw)], kv_r.at[rel, 1])
        for n in range(4):
            arrived(out_ref.at[:, pl.ds(n * pc.dn_w, pc.dn_w)], o_r.at[n])

    def compute():
        y, x = w.square(1, 0), w.square(2, 0)
        q4, kv4 = pc.q4, pc.kv4
        cols = {q: aligned((w.me ^ q) * pc.w4, pc.w4, LANES) for q in range(4)}
        sent = []

        def go(cp):
            cp.start()
            sent.append(cp)

        def load(t, dst, sem):
            off, cw = pc.chunks[t]
            c = pl.ds(off - pc.qkv, cw)
            near = t < pc.early
            arrived(w_ref.at[pl.ds(0, n_fsdp - (6 if near else 2)), :, c], wch.at[t])
            for dz in range(-1, w.nz - 1):
                two = pl.ds(2 * w.chip(dz), 2)
                if dz == 0 or (near and dz in (1, -1)):
                    pieces = own_pieces(t) if dz == 0 else near_pieces(t, 0 if dz == -1 else 1)
                    for core, src in enumerate(pieces):
                        pltpu.make_async_copy(src, dst.at[2 * w.chip(dz) + core], sem).start()
                else:
                    pltpu.make_async_copy(w_ref.at[two, :, c], dst.at[two], sem).start()

        own = [pltpu.make_async_copy(x_ref, xa.at[:, 0], lsem.at[0]),
               pltpu.make_async_copy(xb_ref, xa.at[0, 1], lsem.at[2]),
               pltpu.make_async_copy(q_ref, wg.at[:, :, pl.ds(0, pc.qkv)], lsem.at[1])]
        for cp in own:
            cp.start()
        bits = [pl.ds(j * (seq // 2), seq // 2) for j in range(2)]
        for j, (rel, dev, q) in enumerate(((2, x, 0), (1, y, 1), (2, x, 1), (1, y, 0))):
            go(remote(xb_ref.at[bits[q]], xa.at[rel, 1, bits[q]], xs_s.at[j], xs_r.at[rel, q], dev))
        for cp in own:
            cp.wait()

        def norm_into(dst, slot, load_rows, gain_ref):
            def one(i, carry):
                rows = aligned(i * 16, 16, 16)
                val = load_rows(rows, i).astype(F32)
                inv = lax.rsqrt(jnp.mean(val * val, axis=-1, keepdims=True) + NORM_EPS)
                dst[slot, rows, :] = (val * inv * gain_ref[...]).astype(BF16)
                return carry
            lax.fori_loop(0, rows_b // 16, one, 0)

        per = seq // 16
        lane = lax.broadcasted_iota(jnp.int32, (seq, LANES), 1)
        low_head = (lane % head_dim) < head_dim // 2
        first_head = lane < head_dim
        n_pair = q4 // LANES
        pair_per_kv = n_pair // 2

        def rope(t):
            swapped = jnp.where(low_head, pltpu.roll(t, LANES - head_dim // 2, 1), pltpu.roll(t, head_dim // 2, 1))
            return t * cos_ref[...] + swapped * sin_ref[...]

        def attend(base, h):
            norm_into(mm, 0, lambda rows, i: xa[base + 2 * (i // per), h, aligned((i % per) * 16, 16, 16), :], g1_ref)

            def proj(nt, carry):
                c = aligned(nt * 256, 256, LANES)
                qf[:, c] = jnp.dot(mm[0], wg[:, :, c].reshape(width, 256), preferred_element_type=F32)
                return carry
            lax.fori_loop(0, pc.qkv // 256, proj, 0)

            def one_seq(u, carry):
                slot = base + 2 * u
                rows = aligned(u * seq, seq, seq)
                place = pl.ds(h * seq, seq)
                k_f = rope(qf[rows, pl.ds(q4, LANES)])
                v_f = qf[rows, pl.ds(q4 + kv4, LANES)]
                kvb[slot, place, pl.ds(0, LANES)] = k_f.astype(BF16)
                kvb[slot, place, pl.ds(LANES, LANES)] = v_f.astype(BF16)
                k_r, v_r = pltpu.roll(k_f, head_dim, 1), pltpu.roll(v_f, head_dim, 1)
                zero = jnp.zeros_like(k_f)
                row = lax.broadcasted_iota(jnp.int32, (pair_per_kv * seq, seq), 0) % seq
                causal = row >= lax.broadcasted_iota(jnp.int32, (pair_per_kv * seq, seq), 1)
                for g in range(2):
                    k_lo, k_hi = (k_f, k_r) if g == 0 else (k_r, k_f)
                    v_lo, v_hi = (v_f, v_r) if g == 0 else (v_r, v_f)
                    kk = jnp.concatenate([jnp.where(first_head, k_lo, zero), jnp.where(first_head, zero, k_hi)], axis=0).astype(BF16)
                    vv = jnp.concatenate([jnp.where(first_head, v_lo, zero), jnp.where(first_head, zero, v_hi)], axis=0).astype(BF16)
                    qs = jnp.concatenate([rope(qf[rows, pl.ds((g * pair_per_kv + p) * LANES, LANES)]).astype(BF16) for p in range(pair_per_kv)], axis=0)
                    sc = lax.dot_general(qs, kk, (((1,), (1,)), ((), ())), preferred_element_type=F32) * (head_dim ** -0.5)
                    probs = []
                    for e in range(2):
                        part = jnp.where(causal, sc[:, e * seq:(e + 1) * seq], -jnp.inf)
                        part = jnp.exp(part - jnp.max(part, axis=-1, keepdims=True))
                        probs.append((part / jnp.sum(part, axis=-1, keepdims=True)).astype(BF16))
                    ctx = jnp.dot(jnp.concatenate(probs, axis=1), vv, preferred_element_type=F32).astype(BF16)
                    for p in range(pair_per_kv):
                        lanes = aligned(w.me * pc.w4 + (g * pair_per_kv + p) * LANES, LANES, LANES)
                        ca[slot, place, lanes] = ctx[p * seq:(p + 1) * seq]
                return carry
            lax.fori_loop(0, 2, one_seq, 0)

        whole = pl.ds(0, rows_b)

        def spread(buf, slot, ss, rs, rows=whole, idx=()):
            mine = buf.at[slot, rows, cols[0]]
            go(remote(mine, buf.at[slot ^ 2, rows, cols[0]], ss.at[(slot,) + idx + (1,)], rs.at[(slot ^ 2,) + idx + (1,)], x))
            go(remote(mine, buf.at[slot ^ 1, rows, cols[0]], ss.at[(slot,) + idx + (0,)], rs.at[(slot ^ 1,) + idx + (0,)], y))

        def take(buf, slot, q, rs, rows=whole, idx=()):
            arrived(buf.at[slot, rows, cols[q]], rs.at[(slot,) + idx + (q - 1 if q < 3 else 2,)])

        def relay(buf, slot, q, ss, rs, rows=whole, idx=()):
            take(buf, slot, q, rs, rows, idx)
            ref = buf.at[slot, rows, cols[q]]
            to, dev = (slot ^ 1, y) if q == 2 else (slot ^ 2, x)
            go(remote(ref, buf.at[to, rows, cols[q]], ss.at[(to,) + idx + (2,)], rs.at[(to,) + idx + (2,)], dev))

        def send_kv(slot):
            mine = aligned(w.me * kv4, kv4, LANES)
            for core in range(2):
                for j, dst in enumerate((k_ref, v_ref)):
                    src = kvb.at[slot, pl.ds(core * seq, seq), pl.ds(j * kv4, kv4)]
                    if slot == 0 and core == 0:
                        cp = pltpu.make_async_copy(src, dst.at[:, mine], kv_s.at[slot, core, j])
                        cp.start()
                        local_kv.append(cp)
                    else:
                        go(remote(src, dst.at[:, mine], kv_s.at[slot, core, j], kv_r.at[slot, j], w.square(slot, core)))
        local_kv = []

        def here(slot, q):
            arrived(xa.at[slot, 1, bits[q]], xs_r.at[slot, q])

        seqs = [pl.ds(h * seq, seq) for h in range(2)]

        def send_ctx(base, h):
            for slot in (base, base + 2):
                spread(ca, slot, cs_s, cs_r, seqs[h], (h,))

        def relay_ctx(q, h):
            for slot in ((2, 0) if q == 2 else (0, 2)):
                relay(ca, slot, q, cs_s, cs_r, seqs[h], (h,))

        attend(0, 0)
        send_ctx(0, 0)
        here(2, 0)
        go(remote(xa.at[2, 1, bits[0]], xa.at[3, 1, bits[0]], xs_s.at[4], xs_r.at[3, 0], y))
        here(1, 1)
        go(remote(xa.at[1, 1, bits[1]], xa.at[3, 1, bits[1]], xs_s.at[5], xs_r.at[3, 1], x))
        attend(1, 0)
        send_ctx(1, 0)
        relay_ctx(2, 0)
        here(2, 1)
        attend(0, 1)
        send_ctx(0, 1)
        relay_ctx(1, 0)
        for slot, q in ((1, 0), (3, 0), (3, 1)):
            here(slot, q)
        attend(1, 1)
        send_ctx(1, 1)
        relay_ctx(2, 1)
        relay_ctx(1, 1)
        load(1, wd, lsem.at[0])
        for slot in range(4):
            send_kv(slot)
        arrived(wd, lsem.at[0])
        n_ctx = len(sent)

        def mid(slot):
            for q in (1, 2, 3):
                if q == 3 or slot in (1, 3):
                    for h in range(2):
                        take(ca, slot, q, cs_r, seqs[h], (h,))

            def one(nt, carry):
                c = aligned(nt * 256, 256, LANES)
                o = aligned(w.me * pc.w4 + nt * 256, 256, LANES)
                got = jnp.dot(ca[slot], wd[:, :, c].reshape(width, 256), preferred_element_type=F32)
                res = xa[slot, :, :, o].reshape(rows_b, 256).astype(F32)
                xm[slot, :, o] = (res + got).astype(BF16)
                return carry
            lax.fori_loop(0, pc.w4 // 256, one, 0)
            spread(xm, slot, ms_s, ms_r)

        mid(3)
        mid(1)
        mid(2)
        relay(xm, 1, 2, ms_s, ms_r)
        mid(0)
        relay(xm, 3, 2, ms_s, ms_r)
        relay(xm, 3, 1, ms_s, ms_r)
        relay(xm, 1, 1, ms_s, ms_r)
        for cp in sent[:n_ctx]:
            cp.wait_send()
        del sent[:n_ctx]
        for slot in (0, 2, 1, 3):
            for q in (1, 2, 3):
                if q == 3 or slot in (0, 2):
                    take(xm, slot, q, ms_r)
            norm_into(h2, slot, lambda rows, i, slot=slot: xm[slot, rows, :], g2_ref)

        gate_w = pc.gu_w // 2
        for b in range(4):
            load(2 + b, wg, lsem.at[b % 2])
            arrived(wg, lsem.at[b % 2])

            def one(j, carry):
                s, nt = j // (gate_w // 256), j % (gate_w // 256)
                act = h2[pl.ds(2 * s, 2)].reshape(2 * rows_b, width)
                gate = jnp.dot(act, wg[:, :, aligned(nt * 256, 256, LANES)].reshape(width, 256), preferred_element_type=F32)
                up = jnp.dot(act, wg[:, :, aligned(gate_w + nt * 256, 256, LANES)].reshape(width, 256), preferred_element_type=F32)
                val = (jax.nn.silu(gate) * up).astype(BF16)
                mm[pl.ds(2 * s, 2), :, aligned(b * gate_w + nt * 256, 256, LANES)] = val.reshape(2, rows_b, 256)
                return carry
            lax.fori_loop(0, 2 * (gate_w // 256), one, 0)

        h0, h1 = pl.ds(0, half), pl.ds(half, half)
        first_sends, home = {}, []

        def phase1(n):
            load(last_gu + 1 + n, wd, lsem.at[n % 2])
            for old in first_sends.get(n - 2, ()):
                old.wait_send()
            arrived(wd, lsem.at[n % 2])
            par = n % 2

            def one(j, carry):
                s, nt = j // (pc.dn_w // 256), j % (pc.dn_w // 256)
                c = aligned(nt * 256, 256, LANES)
                act = mm[pl.ds(2 * s, 2)].reshape(2 * rows_b, mm.shape[2])
                got = jnp.dot(act, wd[:, :, c].reshape(mm.shape[2], 256), preferred_element_type=F32)
                pp[par, pl.ds(2 * s, 2), :, c] = got.reshape(2, rows_b, 256)
                return carry
            lax.fori_loop(0, 2 * (pc.dn_w // 256), one, 0)
            first_sends[n] = []
            for path, dev, cc, rels in ((0, x, h0, (2, 3)), (1, y, h1, (1, 3))):
                for j, rel in enumerate(rels):
                    cp = remote(pp.at[par, rel, :, cc], r1.at[n, path, j], p1_s.at[n, path, j], p1_r.at[n, path, j], dev)
                    cp.start()
                    first_sends[n].append(cp)

        def phase2(n):
            par = n % 2
            for path, dev, cc, rel in ((0, y, h0, 1), (1, x, h1, 2)):
                arrived(r1.at[n, path, 1], p1_r.at[n, path, 1])
                r1[n, path, 1] = pp[par, rel, :, cc] + r1[n, path, 1]
                go(remote(r1.at[n, path, 1], r2.at[n, path], p2_s.at[n, path], p2_r.at[n, path], dev))
            for path, cc in ((0, h0), (1, h1)):
                arrived(r1.at[n, path, 0], p1_r.at[n, path, 0])
                r1[n, path, 0] = pp[par, 0, :, cc] + r1[n, path, 0]

        def phase3(n):
            for path in range(2):
                arrived(r2.at[n, path], p2_r.at[n, path])
                c = pl.ds(n * pc.dn_w + path * half, half)
                total = xm[0, :, c].astype(F32) + (r1[n, path, 0] + r2[n, path])
                xm[0, :, c] = total.astype(BF16)
            c = pl.ds(n * pc.dn_w, pc.dn_w)
            go(remote(xm.at[0, pl.ds(seq, seq), c], out_ref.at[:, c], o_s.at[n], o_r.at[n], w.partner()))
            cp = pltpu.make_async_copy(xm.at[0, pl.ds(0, seq), c], out_ref.at[:, c], o_l.at[n])
            cp.start()
            home.append(cp)

        for cp in sent:
            cp.wait_send()
        sent.clear()
        for n in range(4):
            phase1(n)
            if n >= 1:
                phase2(n - 1)
            if n >= 2:
                phase3(n - 2)
        phase2(3)
        phase3(2)
        phase3(3)

        for cp in sent:
            cp.wait_send()
        for n in (2, 3):
            for cp in first_sends[n]:
                cp.wait_send()
        for cp in local_kv + home:
            cp.wait()
        for rel in (1, 2, 3):
            arrived(k_ref.at[:, pl.ds(0, kv4)], kv_r.at[rel, 0])
            arrived(v_ref.at[:, pl.ds(0, kv4)], kv_r.at[rel, 1])

    pl.when(w.c == 1)(stream)
    pl.when(w.c == 0)(compute)


def layer(side, pc, head_dim, x, xb, q_all, near, g1, g2, cos_tab, sin_tab):
    _, seq, width = x.shape
    rows_b = 2 * seq
    kv_width = 4 * pc.kv4
    n_chunk = len(pc.chunks)
    far = pc.n_fsdp // 4
    ff4 = pc.f4 * pc.n_fsdp
    half = pc.dn_w // 2
    hbm = pl.BlockSpec(memory_space=pl.ANY)
    vmem = pl.BlockSpec(memory_space=pltpu.VMEM)
    dma = pltpu.SemaphoreType.DMA
    return pl.pallas_call(
        functools.partial(layer_kernel, side, pc, head_dim),
        out_shape=(
            jax.ShapeDtypeStruct((seq, width), BF16),
            jax.ShapeDtypeStruct((seq, kv_width), BF16),
            jax.ShapeDtypeStruct((seq, kv_width), BF16),
            jax.ShapeDtypeStruct((pc.n_fsdp, pc.rows, pc.late), BF16)),
        in_specs=[hbm] * (3 + len(near)) + [vmem, vmem, vmem, vmem],
        out_specs=(hbm, hbm, hbm, hbm),
        scratch_shapes=[
            pltpu.VMEM((4, 2, seq, width), BF16),
            pltpu.VMEM((4, rows_b, width), BF16),
            pltpu.VMEM((4, rows_b, width), BF16),
            pltpu.VMEM((pc.n_fsdp, pc.rows, pc.gu_w), BF16),
            pltpu.VMEM((pc.n_fsdp, pc.rows, pc.dn_w), BF16),
            pltpu.VMEM((4, rows_b, max(ff4, width)), BF16),
            pltpu.VMEM((2, 4, rows_b, pc.dn_w), F32),
            pltpu.VMEM((4, 2, 2, rows_b, half), F32),
            pltpu.VMEM((4, 2, rows_b, half), F32),
            pltpu.VMEM((rows_b, pc.qkv), F32),
            pltpu.VMEM((4, rows_b, 2 * pc.kv4), BF16),
            dma((3,)),
            dma((6,)), dma((4, 2)),
            dma((4, 2, 3)), dma((4, 2, 3)),
            dma((4, 3)), dma((4, 3)),
            dma((4, 2, 2)), dma((4, 2)),
            dma((4, 2, 2)), dma((4, 2, 2)),
            dma((4, 2)), dma((4, 2)),
            dma((4,)), dma((4,)), dma((4,)),
            dma((n_chunk, 2, far + 1)), dma((n_chunk, 2, far + 1)), dma((n_chunk, 2, far + 1)), dma((n_chunk,)),
        ],
        compiler_params=pltpu.CompilerParams(collective_id=2, has_side_effects=True, vmem_limit_bytes=67043328),
        name='layer',
    )(x, xb, q_all, *near, g1, g2, cos_tab, sin_tab)


def solution(mesh):
    batch_axes = ('dp', 'fsdp')
    row_spec = P('fsdp', None)
    n_dp = mesh.shape['dp']
    n_fsdp = mesh.shape['fsdp']
    side = math.isqrt(n_dp)

    def device_step(tokens, embed_table, norm_attn, w_qkv, w_out, norm_mlp, w_gate_up, w_down, rope_scale):
        seq = tokens.shape[1]
        shard_rows, width = embed_table.shape
        head_dim = 2 * rope_scale.shape[0]
        rows = w_out.shape[0]
        q_width = rows * n_fsdp
        kv_width = (w_qkv.shape[1] - q_width) // 2
        pc = Pieces(rows, q_width // 4, kv_width // 4, width // 4, w_down.shape[0] // 4, n_fsdp, width)

        gains = jnp.stack([norm_attn, norm_mlp]).astype(F32)
        ids, gains, pq, pe, pd = gather_ids(side, pc, tokens, gains, w_qkv, w_out, w_gate_up, w_down)
        def first_hop(piece, dz):
            return lax.ppermute(piece, 'fsdp', [(i, (i + 2 * dz) % n_fsdp) for i in range(n_fsdp)])

        n0, n1 = first_hop(pq, 1), first_hop(pq, -1)
        f0, f1 = first_hop(pe, 1), first_hop(pe, -1)
        ids = ids.reshape(-1) - lax.axis_index('fsdp') * shard_rows
        owned = (ids >= 0) & (ids < shard_rows)
        table_rows = gather_table(ids, owned, embed_table)
        g1 = gains[:, 0].reshape(1, width)
        g2 = gains[:, 1].reshape(1, width)

        freq_expo = jnp.arange(head_dim // 2, dtype=F32) * (2.0 / head_dim)
        inv_freq = 1.0 / (rope_scale * jnp.power(ROPE_THETA, freq_expo))
        angles = jnp.arange(seq, dtype=F32)[:, None] * inv_freq[None, :]
        cos_tab, sin_tab = jnp.cos(angles), jnp.sin(angles)
        reps = LANES // head_dim
        cos_tab = jnp.concatenate([cos_tab, cos_tab] * reps, axis=1)
        sin_tab = jnp.concatenate([-sin_tab, sin_tab] * reps, axis=1)

        table_rows = table_rows.reshape(n_fsdp // 2, 2, seq, width)
        x, xb, q_all, te, td, tf = embed(side, pc, table_rows, pq, n0, n1, pe, pd, f0, f1)
        out, k, v, _ = layer(side, pc, head_dim, x, xb, q_all, (pe, pd, f0, f1, te, td, tf), g1, g2, cos_tab, sin_tab)
        heads = (1, seq, kv_width // head_dim, head_dim)
        return out[None], k.reshape(heads), v.reshape(heads)

    return jax.shard_map(
        device_step,
        mesh=mesh,
        in_specs=(P(batch_axes, None), row_spec, P('fsdp'), row_spec, row_spec, P('fsdp'), row_spec, row_spec, P(None)),
        out_specs=(P(batch_axes, None, None), P(batch_axes, None, None, None), P(batch_axes, None, None, None)),
        check_vma=False,
    )
```

```python
import functools
import math

import jax
import jax.numpy as jnp
from jax import lax
from jax.experimental import pallas as pl
from jax.experimental.pallas import tpu as pltpu
from jax.sharding import PartitionSpec as P

NORM_EPS = 1e-5
ROPE_THETA = 10000.0
PICK = 32
DEPTH = 4
LANES = 128
MESH = pl.DeviceIdType.MESH
BF16 = jnp.bfloat16
F32 = jnp.float32


def aligned(start, size, step):
    return pl.ds(pl.multiple_of(start, step), size)


class Where:
    def __init__(self, side, n_fsdp):
        self.side = side
        self.nz = n_fsdp // 2
        self.dp = lax.axis_index('dp')
        self.f = lax.axis_index('fsdp')
        self.z = self.f // 2
        self.c = self.f % 2
        self.px = self.dp // side
        self.py = self.dp % side
        self.me = 2 * (self.px % 2) + self.py % 2

    def chip(self, dz):
        return lax.rem(self.z + dz + self.nz, self.nz)

    def along_z(self, dz, core):
        return (self.dp, 2 * self.chip(dz) + core)

    def partner(self):
        return (self.dp, 2 * self.z + 1 - self.c)

    def square(self, rel, core):
        px = self.px + (1 - 2 * (self.px % 2)) if rel & 2 else self.px
        py = self.py + (1 - 2 * (self.py % 2)) if rel & 1 else self.py
        return (px * self.side + py, 2 * self.z + core)


def greet(devices):
    barrier = pltpu.get_barrier_semaphore()
    for dev in devices:
        pl.semaphore_signal(barrier, inc=1, device_id=dev, device_id_type=MESH)
    pl.semaphore_wait(barrier, len(devices))


def remote(src, dst, ssem, rsem, dev):
    return pltpu.make_async_remote_copy(src_ref=src, dst_ref=dst, send_sem=ssem, recv_sem=rsem, device_id=dev, device_id_type=MESH)


def arrived(ref, sem):
    pltpu.make_async_copy(ref, ref, sem).wait()


def ids_kernel(side, pc, tok_ref, gain_ref, w_qkv, w_out, w_gu, w_dn, ids_ref, gains_ref, pe_ref, pd_ref,
               pk, lsem, ssem, rsem, pack_sem, store_sem):
    n_fsdp = pc.n_fsdp
    w = Where(side, n_fsdp)
    pack_copies(pc, w.me, pk, w_qkv, w_out, w_gu, w_dn, pack_sem)
    greet([(w.dp, lax.rem(w.f + k, n_fsdp)) for k in range(1, n_fsdp)])
    own = [pltpu.make_async_copy(tok_ref, ids_ref.at[w.f], lsem.at[0]),
           pltpu.make_async_copy(gain_ref, gains_ref.at[w.f], lsem.at[1])]
    for cp in own:
        cp.start()
    sent = []
    for k in range(1, n_fsdp):
        dev = (w.dp, lax.rem(w.f + k, n_fsdp))
        for j, (src, dst) in enumerate(((tok_ref, ids_ref), (gain_ref, gains_ref))):
            cp = remote(src, dst.at[w.f], ssem.at[j, k], rsem.at[j, k], dev)
            cp.start()
            sent.append(cp)
    arrived(pk, pack_sem)
    lo = 0
    stores = []
    for j, ref in enumerate((pe_ref, pd_ref)):
        stores.append(pltpu.make_async_copy(pk.at[:, pl.ds(lo, ref.shape[1])], ref, store_sem.at[j]))
        stores[-1].start()
        lo += ref.shape[1]
    for cp in own + stores:
        cp.wait()
    for cp in sent:
        cp.wait_send()
    for k in range(1, n_fsdp):
        src = lax.rem(w.f - k + n_fsdp, n_fsdp)
        arrived(ids_ref.at[src], rsem.at[0, k])
        arrived(gains_ref.at[src], rsem.at[1, k])


class Pieces:
    def __init__(self, rows, q4, kv4, w4, f4, n_fsdp, width):
        self.rows = rows
        self.q4, self.kv4, self.w4, self.f4 = q4, kv4, w4, f4
        self.n_fsdp = n_fsdp
        self.width = width
        self.qkv = q4 + 2 * kv4
        self.gu0 = self.qkv + w4
        self.gu_w = 2 * f4 * n_fsdp // 4
        self.dn0 = self.gu0 + 4 * self.gu_w
        self.dn_w = width // 4
        self.total = self.dn0 + width
        self.late = self.total - self.qkv
        self.chunks = [(0, self.qkv), (self.qkv, w4)]
        self.chunks += [(self.gu0 + b * self.gu_w, self.gu_w) for b in range(4)]
        self.chunks += [(self.dn0 + n * self.dn_w, self.dn_w) for n in range(4)]
        self.early = 6


def pack_copies(pc, me, pk, w_qkv, w_out, w_gu, w_dn, sem):
    q4, kv4, w4, f4 = pc.q4, pc.kv4, pc.w4, pc.f4
    first = [
        (w_qkv.at[:, aligned(me * q4, q4, LANES)], pk.at[:, pl.ds(0, q4)]),
        (w_qkv.at[:, aligned(4 * q4 + me * kv4, kv4, LANES)], pk.at[:, pl.ds(q4, kv4)]),
        (w_qkv.at[:, aligned(4 * q4 + 4 * kv4 + me * kv4, kv4, LANES)], pk.at[:, pl.ds(q4 + kv4, kv4)]),
    ]
    for src, dst in first:
        pltpu.make_async_copy(src, dst, sem).start()
    pltpu.make_async_copy(w_out.at[:, aligned(me * w4, w4, LANES)], pk.at[:, pl.ds(pc.qkv, w4)], sem).start()
    ff = 4 * f4 * pc.n_fsdp
    for d in range(pc.n_fsdp):
        b, k = d // 4, d % 4
        for part in range(2):
            src = w_gu.at[:, aligned(part * ff + d * 4 * f4 + me * f4, f4, LANES)]
            dst = pk.at[:, pl.ds(pc.gu0 + b * pc.gu_w + part * (pc.gu_w // 2) + k * f4, f4)]
            pltpu.make_async_copy(src, dst, sem).start()
    pltpu.make_async_copy(w_dn.at[aligned(me * f4, f4, LANES), :], pk.at[:, pl.ds(pc.dn0, pc.width)], sem).start()


def gather_ids(side, pc, tokens, gains, w_qkv, w_out, w_gu, w_dn):
    n_fsdp = pc.n_fsdp
    vmem, hbm = pl.BlockSpec(memory_space=pltpu.VMEM), pl.BlockSpec(memory_space=pl.ANY)
    dma = pltpu.SemaphoreType.DMA
    return pl.pallas_call(
        functools.partial(ids_kernel, side, pc),
        out_shape=(
            jax.ShapeDtypeStruct((n_fsdp,) + tokens.shape, tokens.dtype),
            jax.ShapeDtypeStruct((n_fsdp,) + gains.shape, gains.dtype),
            jax.ShapeDtypeStruct((pc.rows, pc.dn0), BF16),
            jax.ShapeDtypeStruct((pc.rows, pc.width), BF16)),
        in_specs=[vmem, vmem, hbm, hbm, hbm, hbm],
        out_specs=(vmem, vmem, hbm, hbm),
        scratch_shapes=[pltpu.VMEM((pc.rows, pc.total), BF16), dma((2,)), dma((2, n_fsdp)), dma((2, n_fsdp)), dma, dma((2,))],
        compiler_params=pltpu.CompilerParams(collective_id=0, has_side_effects=True),
        name='ids',
    )(tokens, gains, w_qkv, w_out, w_gu, w_dn)


def gather_kernel(n_tok, gid_ref, tgt_ref, table_ref, out_ref, buf, sems):
    width = table_ref.shape[2]
    n_step = n_tok // PICK

    def fetch(step, slot):
        for i in range(PICK):
            pltpu.make_async_copy(table_ref.at[gid_ref[step * PICK + i]], buf.at[slot, i], sems.at[slot]).start()

    for j in range(DEPTH - 1):
        fetch(j, j)

    def body(step, carry):
        slot = lax.rem(step, DEPTH)

        @pl.when(step + DEPTH - 1 < n_step)
        def _():
            fetch(step + DEPTH - 1, lax.rem(step + DEPTH - 1, DEPTH))
        arrived(buf.at[slot], sems.at[slot])
        rows = aligned(step * PICK, PICK, PICK)
        hot = (lax.broadcasted_iota(jnp.int32, (PICK, PICK * 8), 1) == tgt_ref[rows, :]).astype(BF16)
        got = jnp.dot(hot, buf[slot].reshape(PICK * 8, width), preferred_element_type=F32)
        out_ref[rows, :] = got.astype(BF16)
        return carry
    lax.fori_loop(0, n_step, body, 0)


def gather_table(ids, owned, table):
    n_tok = ids.shape[0]
    n_rows, width = table.shape
    gid = jnp.where(owned, ids // 8, jnp.arange(n_tok, dtype=jnp.int32) % (n_rows // 8))
    place = jnp.arange(n_tok, dtype=jnp.int32) % PICK
    tgt = jnp.where(owned, 8 * place + ids % 8, -1)[:, None]
    return pl.pallas_call(
        functools.partial(gather_kernel, n_tok),
        out_shape=jax.ShapeDtypeStruct((n_tok, width), BF16),
        in_specs=[pl.BlockSpec(memory_space=pltpu.SMEM), pl.BlockSpec(memory_space=pltpu.VMEM), pl.BlockSpec(memory_space=pl.ANY)],
        out_specs=pl.BlockSpec(memory_space=pltpu.VMEM),
        scratch_shapes=[pltpu.VMEM((DEPTH, PICK, 8, width), BF16), pltpu.SemaphoreType.DMA((DEPTH,))],
        compiler_params=pltpu.CompilerParams(vmem_limit_bytes=48 * 2**20),
        cost_estimate=pl.CostEstimate(flops=80 * 10**9, bytes_accessed=9 * n_tok * width * 2, transcendentals=0),
        name='rows',
    )(gid, tgt, table.reshape(n_rows // 8, 8, width))


def embed_kernel(side, pc, rows_ref, pe_ref, pd_ref, f0_ref, f1_ref, xa_ref, xb_ref, q_ref, te_ref, td_ref, tf_ref,
                 got, peer, rp, sb, pk, xo,
                 got_sem, pack_sem, own_sem, d2d_s, d2d_r, f_s, f_r, push_s, push_r,
                 peer_s, peer_r, rs_s, rs_r, home_sem, x_s, x_r):
    n_fsdp = pc.n_fsdp
    w = Where(side, n_fsdp)
    nz = w.nz
    far = nz // 2
    seq = got.shape[2]
    hw = got.shape[3]
    width = 2 * hw
    order = [far]
    for o in range(far - 1, 0, -1):
        order += [o, -o]
    order += [0]
    mine = aligned(w.c * hw, hw, LANES)
    other = aligned((1 - w.c) * hw, hw, LANES)
    for k in range(len(order)):
        dest = w.chip(order[k])
        pltpu.make_async_copy(rows_ref.at[dest, :, :, mine], got.at[dest], got_sem.at[k]).start()
    q_srcs = [ref.at[:, pl.ds(0, pc.qkv)] for ref in (pe_ref, f0_ref, f1_ref)]
    for j, src in enumerate(q_srcs):
        pltpu.make_async_copy(src, pk.at[j], pack_sem.at[j]).start()
    greet([w.partner()] + [w.along_z(dz, core) for dz in (1, -1) for core in (0, 1)] + [w.square(rel, core) for rel in (1, 2) for core in (0, 1)])
    dirs = (1, -1)

    for k in range(len(order)):
        dest = w.chip(order[k])
        remote(rows_ref.at[dest, :, :, other], peer.at[dest], peer_s.at[k], peer_r.at[k], w.partner()).start()

    here_q = (2 * w.z + w.c, 2 * w.chip(-1) + w.c, 2 * w.chip(1) + w.c)
    swaps = [(src, q_ref.at[here_q[j]]) for j, src in enumerate(q_srcs)]
    rest = pl.ds(pc.qkv, pc.dn0 - pc.qkv)
    swaps += [(pe_ref.at[:, rest], te_ref), (pd_ref, td_ref), (f0_ref.at[:, rest], tf_ref.at[0]), (f1_ref.at[:, rest], tf_ref.at[1])]
    own = [remote(src, dst, d2d_s.at[j], d2d_r.at[j], w.partner()) for j, (src, dst) in enumerate(swaps)]


    def pair(dz):
        return q_ref.at[pl.ds(2 * w.chip(dz), 2)]

    def single(dz, i):
        return q_ref.at[pl.ds(2 * w.chip(dz) + i, 1)]

    def push(ref, i, h):
        remote(ref, ref, push_s.at[i, h], push_r, w.partner()).start()

    local = []

    def forward(h):
        @pl.when(w.c == 1)
        def _():
            for i, dz in enumerate(dirs):
                if h == 1:
                    local[1 + i].wait()
                    own[1 + i].wait_recv()
                elif h < far:
                    arrived(pair(-dz * h), f_r.at[i, h])
                else:
                    arrived(single(-dz * h, i), f_r.at[i, h])
                if h < far - 1:
                    remote(pair(-dz * h), pair(-dz * h), f_s.at[i, h + 1], f_r.at[i, h + 1], w.along_z(dz, 1)).start()
                elif h == far - 1:
                    remote(single(-dz * h, i), single(-dz * h, i), f_s.at[i, h + 1], f_r.at[i, h + 1], w.along_z(dz, 1)).start()
                if h > 1:
                    push(pair(-dz * h) if h < far else single(-dz * h, i), i, h)

    def addto(dst, terms, q):
        def one(r, carry):
            rows = aligned(q * (seq // 2) + r * 32, 32, 32)
            val = terms[0](rows)
            for term in terms[1:]:
                val = val + term(rows)
            dst(rows, val)
            return carry
        lax.fori_loop(0, seq // 64, one, 0)

    def part(ref, q):
        return ref.at[pl.ds(q * (seq // 2), seq // 2)]

    def rs_stage(k, h):
        o = order[k]
        dest = w.chip(o)
        if h == 0:
            arrived(got.at[dest], got_sem.at[k])
            arrived(peer.at[dest], peer_r.at[k])
        if o == 0:
            return
        dist = abs(o)
        for i, dz in enumerate(dirs):
            if (o * dz < 0 and o != far) or (dist == far and h != i):
                continue
            for q in range(2):
                terms = [lambda r: got[dest, h, r, :], lambda r: peer[dest, h, r, :]]
                if dist < far - 1 or (dist == far - 1 and h == i):
                    arrived(part(rp.at[i, dist, h], q), rs_r.at[i, dist, h, q])
                    terms.append(lambda r, i=i: rp[i, dist, h, r, :])

                def put(r, val, i=i):
                    sb[i, dist - 1, h, r, :] = val
                addto(put, terms, q)
                remote(part(sb.at[i, dist - 1, h], q), part(rp.at[i, dist - 1, h], q), rs_s.at[i, dist - 1, h, q],
                       rs_r.at[i, dist - 1, h, q], w.along_z(dz, w.c)).start()

    def finish(h):
        for q in range(2):
            terms = [lambda r: got[w.z, h, r, :], lambda r: peer[w.z, h, r, :]]
            for i in range(2):
                arrived(part(rp.at[i, 0, h], q), rs_r.at[i, 0, h, q])
                terms.append(lambda r, i=i: rp[i, 0, h, r, :])

            def put(r, val):
                xo[h, r, :] = val
            addto(put, terms, q)
        dst = (xa_ref.at[0] if h == 0 else xb_ref).at[:, mine]

        @pl.when(w.c == 0)
        def _():
            pltpu.make_async_copy(xo.at[h], dst, home_sem.at[h]).start()

        @pl.when(w.c == 1)
        def _():
            remote(xo.at[h], dst, home_sem.at[h], x_r.at[0, h], w.partner()).start()

    sides = ((2, w.square(2, 0)), (1, w.square(1, 0)))
    spread = [remote(xo.at[0], xa_ref.at[rel, :, mine], x_s.at[j], x_r.at[rel, w.c], dev) for j, (rel, dev) in enumerate(sides)]
    col = [pl.ds(j * hw, hw) for j in range(2)]
    relay = [remote(xa_ref.at[rel, :, col[j]], xa_ref.at[3, :, col[j]], x_s.at[2 + j], x_r.at[3, j], sides[1 - j][1]) for j, (rel, _) in enumerate(sides)]

    for j in range(3):
        arrived(pk.at[j], pack_sem.at[j])
        local.append(pltpu.make_async_copy(pk.at[j], q_ref.at[here_q[j]], own_sem.at[j]))
    last = len(order) - 1
    for k in range(last + 1):
        rs_stage(k, 0)
        if k == 0:
            for cp in own[:3] + local:
                cp.start()
        if k == 2:
            for cp in own[3:]:
                cp.start()
            forward(1)
        if k == 5:
            forward(2)
    for k in range(3):
        rs_stage(k, 1)
    finish(0)
    for cp in spread:
        cp.start()
    for k in range(3, last + 1):
        rs_stage(k, 1)
        if k == 4:
            forward(3)
        if k == last - 1:
            @pl.when(w.c == 0)
            def _():
                for j, (rel, _) in enumerate(sides):
                    arrived(xa_ref.at[rel, :, col[j]], x_r.at[rel, j])
                    relay[j].start()
    forward(4)
    finish(1)

    for cp in own[:1] + own[3:]:
        cp.wait()
    for cp in own[1:3]:
        cp.wait_send()
    local[0].wait()
    for cp in spread:
        cp.wait_send()
    for k in range(len(order)):
        dest = w.chip(order[k])
        arrived(peer.at[dest], peer_s.at[k])
    for i in range(2):
        for dist in range(1, far + 1):
            for h in ((i,) if dist == far else (0, 1)):
                for q in range(2):
                    arrived(part(sb.at[i, dist - 1, h], q), rs_s.at[i, dist - 1, h, q])

    @pl.when(w.c == 1)
    def _():
        for i, dz in enumerate(dirs):
            for h in range(1, far + 1):
                ref = pair(-dz * h) if h < far else single(-dz * h, i)
                if h > 1:
                    arrived(ref, push_s.at[i, h])
                if h < far:
                    arrived(pair(-dz * h) if h < far - 1 else single(-dz * h, i), f_s.at[i, h + 1])

    @pl.when(w.c == 0)
    def _():
        arrived(q_ref.at[pl.ds(0, n_fsdp - 6)], push_r)
        for j in (1, 2):
            local[j].wait()
            own[j].wait_recv()
        arrived(xa_ref.at[0, :, col[1]], x_r.at[0, 0])
        arrived(xb_ref.at[:, col[1]], x_r.at[0, 1])
        arrived(xa_ref.at[2, :, col[1]], x_r.at[2, 1])
        arrived(xa_ref.at[1, :, col[0]], x_r.at[1, 0])
        for j in range(2):
            arrived(xa_ref.at[3, :, col[j]], x_r.at[3, j])
            relay[j].wait_send()
    for h in range(2):
        arrived(xo.at[h], home_sem.at[h])


def embed(side, pc, rows, pe, pd, f0, f1):
    seq, width = rows.shape[2], rows.shape[3]
    nz = pc.n_fsdp // 2
    far = nz // 2
    hbm = pl.BlockSpec(memory_space=pl.ANY)
    dma = pltpu.SemaphoreType.DMA
    return pl.pallas_call(
        functools.partial(embed_kernel, side, pc),
        out_shape=(
            jax.ShapeDtypeStruct((4, seq, width), BF16),
            jax.ShapeDtypeStruct((seq, width), BF16),
            jax.ShapeDtypeStruct((pc.n_fsdp, pc.rows, pc.qkv), BF16),
            jax.ShapeDtypeStruct((pc.rows, pc.dn0 - pc.qkv), BF16),
            jax.ShapeDtypeStruct(pd.shape, BF16),
            jax.ShapeDtypeStruct((2, pc.rows, pc.dn0 - pc.qkv), BF16)),
        in_specs=[hbm] * 5,
        out_specs=(hbm,) * 6,
        scratch_shapes=[
            pltpu.VMEM((nz, 2, seq, width // 2), BF16),
            pltpu.VMEM((nz, 2, seq, width // 2), BF16),
            pltpu.VMEM((2, far, 2, seq, width // 2), BF16),
            pltpu.VMEM((2, far, 2, seq, width // 2), BF16),
            pltpu.VMEM((3, pc.rows, pc.qkv), BF16),
            pltpu.VMEM((2, seq, width // 2), BF16),
            dma((nz,)), dma((3,)), dma((3,)), dma((7,)), dma((7,)),
            dma((2, far + 1)), dma((2, far + 1)), dma((2, far + 1)), dma,
            dma((nz,)), dma((nz,)),
            dma((2, far, 2, 2)), dma((2, far, 2, 2)),
            dma((2,)), dma((4,)), dma((4, 2)),
        ],
        compiler_params=pltpu.CompilerParams(collective_id=1, has_side_effects=True, vmem_limit_bytes=67043328),
        name='embed',
    )(rows, pe, pd, f0, f1)


def layer_kernel(side, pc, head_dim, x_ref, xb_ref, q_ref, pe_ref, pd_ref, f0_ref, f1_ref, te_ref, td_ref, tf_ref, g1_ref, g2_ref, cos_ref, sin_ref, out_ref, k_ref, v_ref, w_ref,
                 xa, ca, xm, wg, wd, mm, pp, r1, r2, qf, kvb,
                 lsem, xs_s, xs_r, cs_s, cs_r, ms_s, ms_r, kv_s, kv_r, p1_s, p1_r, p2_s, p2_r, o_s, o_l, o_r,
                 zs, zr, ps, wch):
    h2 = ca
    n_fsdp = pc.n_fsdp
    w = Where(side, n_fsdp)
    far = w.nz // 2
    seq, width = xa.shape[2], xa.shape[3]
    rows_b = 2 * seq
    half = pc.dn_w // 2
    n_chunk = len(pc.chunks)
    last_gu = 5
    greet([w.partner(), w.along_z(1, w.c), w.along_z(-1, w.c)] + [w.square(rel, core) for rel in (1, 2, 3) for core in (0, 1)])
    dirs = (1, -1)

    def slim(t, mine):
        off, cw = pc.chunks[t]
        return pl.ds(off - pc.dn0 if t >= pc.early else off - (0 if mine else pc.qkv), cw)

    def own_pieces(t):
        refs = (pe_ref, te_ref) if t < pc.early else (pd_ref, td_ref)
        return [refs[0].at[:, slim(t, True)], refs[1].at[:, slim(t, False)]]

    def near_pieces(t, i):
        return [(f0_ref, f1_ref)[i].at[:, slim(t, True)], tf_ref.at[i, :, slim(t, False)]]

    def stream():
        def cols(t):
            off, cw = pc.chunks[t]
            return pl.ds(off - pc.qkv, cw)

        def pair(t, dz):
            return w_ref.at[pl.ds(2 * w.chip(dz), 2), :, cols(t)]

        def single(t, dz, i):
            return w_ref.at[pl.ds(2 * w.chip(dz) + i, 1), :, cols(t)]

        def piece(t, h, i):
            dz = dirs[i]
            return pair(t, -dz * h) if h < far else single(t, -dz * h, i)

        sent = []

        def hop(t, h):
            if t < 1 or t >= n_chunk or (h == 0 and t < pc.early):
                return
            ready = h == 1 and t < pc.early
            for i in range(2):
                dz = dirs[i]
                if h > 0 and not ready:
                    arrived(piece(t, h, i), zr.at[t, i, h])
                if h == far:
                    continue
                ref = pair(t, -dz * h) if h < far - 1 else single(t, -dz * h, i)
                sems = (zs.at[t, i, h], zr.at[t, i, h + 1], w.along_z(dz, 1))
                if h == 0 or ready:
                    pieces = near_pieces(t, i) if ready else own_pieces(t)
                    for src, core in zip(pieces, (1, 0)):
                        remote(src, w_ref.at[2 * w.chip(-dz * h) + core, :, cols(t)], *sems).start()
                else:
                    remote(ref, ref, *sems).start()
                sent.append((ref, zs.at[t, i, h]))
            if h > 0 and not ready:
                for i in range(2):
                    ref = piece(t, h, i)
                    remote(ref, ref, ps.at[t, i, h], wch.at[t], w.partner()).start()
                    sent.append((ref, ps.at[t, i, h]))

        for s in range(n_chunk + far):
            for h in range(far, -1, -1):
                hop(s - h if h > 1 else s + 1 - h, h)
        for ref, sem in sent:
            arrived(ref, sem)
        kvw = 2 * (kvb.shape[2] // 4)
        for rel in range(4):
            arrived(k_ref.at[:, pl.ds(0, kvw)], kv_r.at[rel, 0])
            arrived(v_ref.at[:, pl.ds(0, kvw)], kv_r.at[rel, 1])
        for n in range(4):
            arrived(out_ref.at[:, pl.ds(n * pc.dn_w, pc.dn_w)], o_r.at[n])

    def compute():
        y, x = w.square(1, 0), w.square(2, 0)
        q4, kv4 = pc.q4, pc.kv4
        cols = {q: aligned((w.me ^ q) * pc.w4, pc.w4, LANES) for q in range(4)}
        sent = []

        def go(cp):
            cp.start()
            sent.append(cp)

        def load(t, dst, sem, first=True):
            off, cw = pc.chunks[t]
            c = pl.ds(off - pc.qkv, cw)
            near = t < pc.early
            if first:
                arrived(w_ref.at[pl.ds(0, n_fsdp - (6 if near else 2)), :, c], wch.at[t])
            for dz in range(-1, w.nz - 1):
                two = pl.ds(2 * w.chip(dz), 2)
                if dz == 0 or (near and dz in (1, -1)):
                    pieces = own_pieces(t) if dz == 0 else near_pieces(t, 0 if dz == -1 else 1)
                    for core, src in enumerate(pieces):
                        pltpu.make_async_copy(src, dst.at[2 * w.chip(dz) + core], sem).start()
                else:
                    pltpu.make_async_copy(w_ref.at[two, :, c], dst.at[two], sem).start()

        own = [pltpu.make_async_copy(x_ref, xa.at[:, 0], lsem.at[0]),
               pltpu.make_async_copy(xb_ref, xa.at[0, 1], lsem.at[2]),
               pltpu.make_async_copy(q_ref, wg.at[0, :, :, pl.ds(0, pc.qkv)], lsem.at[1])]
        for cp in own:
            cp.start()
        bits = [pl.ds(j * (seq // 2), seq // 2) for j in range(2)]
        for j, (rel, dev, q) in enumerate(((2, x, 0), (1, y, 1), (2, x, 1), (1, y, 0))):
            go(remote(xb_ref.at[bits[q]], xa.at[rel, 1, bits[q]], xs_s.at[j], xs_r.at[rel, q], dev))
        for cp in own:
            cp.wait()

        def norm_into(dst, slot, load_rows, gain_ref):
            def one(i, carry):
                rows = aligned(i * 16, 16, 16)
                val = load_rows(rows, i).astype(F32)
                inv = lax.rsqrt(jnp.mean(val * val, axis=-1, keepdims=True) + NORM_EPS)
                dst[slot, rows, :] = (val * inv * gain_ref[...]).astype(BF16)
                return carry
            lax.fori_loop(0, rows_b // 16, one, 0)

        per = seq // 16
        lane = lax.broadcasted_iota(jnp.int32, (seq, LANES), 1)
        low_head = (lane % head_dim) < head_dim // 2
        first_head = lane < head_dim
        n_pair = q4 // LANES
        pair_per_kv = n_pair // 2

        def rope(t):
            swapped = jnp.where(low_head, pltpu.roll(t, LANES - head_dim // 2, 1), pltpu.roll(t, head_dim // 2, 1))
            return t * cos_ref[...] + swapped * sin_ref[...]

        def attend(base, h):
            norm_into(mm, 0, lambda rows, i: xa[base + 2 * (i // per), h, aligned((i % per) * 16, 16, 16), :], g1_ref)

            def proj(nt, carry):
                c = aligned(nt * 256, 256, LANES)
                qf[:, c] = jnp.dot(mm[0], wg[0, :, :, c].reshape(width, 256), preferred_element_type=F32)
                return carry
            lax.fori_loop(0, pc.qkv // 256, proj, 0)

            def one_seq(u, carry):
                slot = base + 2 * u
                rows = aligned(u * seq, seq, seq)
                place = pl.ds(h * seq, seq)
                k_f = rope(qf[rows, pl.ds(q4, LANES)])
                v_f = qf[rows, pl.ds(q4 + kv4, LANES)]
                kvb[slot, place, pl.ds(0, LANES)] = k_f.astype(BF16)
                kvb[slot, place, pl.ds(LANES, LANES)] = v_f.astype(BF16)
                k_r, v_r = pltpu.roll(k_f, head_dim, 1), pltpu.roll(v_f, head_dim, 1)
                zero = jnp.zeros_like(k_f)
                row = lax.broadcasted_iota(jnp.int32, (pair_per_kv * seq, seq), 0) % seq
                causal = row >= lax.broadcasted_iota(jnp.int32, (pair_per_kv * seq, seq), 1)
                for g in range(2):
                    k_lo, k_hi = (k_f, k_r) if g == 0 else (k_r, k_f)
                    v_lo, v_hi = (v_f, v_r) if g == 0 else (v_r, v_f)
                    kk = jnp.concatenate([jnp.where(first_head, k_lo, zero), jnp.where(first_head, zero, k_hi)], axis=0).astype(BF16)
                    vv = jnp.concatenate([jnp.where(first_head, v_lo, zero), jnp.where(first_head, zero, v_hi)], axis=0).astype(BF16)
                    qs = jnp.concatenate([rope(qf[rows, pl.ds((g * pair_per_kv + p) * LANES, LANES)]).astype(BF16) for p in range(pair_per_kv)], axis=0)
                    sc = lax.dot_general(qs, kk, (((1,), (1,)), ((), ())), preferred_element_type=F32) * (head_dim ** -0.5)
                    probs = []
                    for e in range(2):
                        part = jnp.where(causal, sc[:, e * seq:(e + 1) * seq], -jnp.inf)
                        part = jnp.exp(part - jnp.max(part, axis=-1, keepdims=True))
                        probs.append((part / jnp.sum(part, axis=-1, keepdims=True)).astype(BF16))
                    ctx = jnp.dot(jnp.concatenate(probs, axis=1), vv, preferred_element_type=F32).astype(BF16)
                    for p in range(pair_per_kv):
                        lanes = aligned(w.me * pc.w4 + (g * pair_per_kv + p) * LANES, LANES, LANES)
                        ca[slot, place, lanes] = ctx[p * seq:(p + 1) * seq]
                return carry
            lax.fori_loop(0, 2, one_seq, 0)

        whole = pl.ds(0, rows_b)

        def spread(buf, slot, ss, rs, rows=whole, idx=()):
            mine = buf.at[slot, rows, cols[0]]
            go(remote(mine, buf.at[slot ^ 2, rows, cols[0]], ss.at[(slot,) + idx + (1,)], rs.at[(slot ^ 2,) + idx + (1,)], x))
            go(remote(mine, buf.at[slot ^ 1, rows, cols[0]], ss.at[(slot,) + idx + (0,)], rs.at[(slot ^ 1,) + idx + (0,)], y))

        def take(buf, slot, q, rs, rows=whole, idx=()):
            arrived(buf.at[slot, rows, cols[q]], rs.at[(slot,) + idx + (q - 1 if q < 3 else 2,)])

        def relay(buf, slot, q, ss, rs, rows=whole, idx=()):
            take(buf, slot, q, rs, rows, idx)
            ref = buf.at[slot, rows, cols[q]]
            to, dev = (slot ^ 1, y) if q == 2 else (slot ^ 2, x)
            go(remote(ref, buf.at[to, rows, cols[q]], ss.at[(to,) + idx + (2,)], rs.at[(to,) + idx + (2,)], dev))

        def send_kv(slot):
            mine = aligned(w.me * kv4, kv4, LANES)
            for core in range(2):
                for j, dst in enumerate((k_ref, v_ref)):
                    src = kvb.at[slot, pl.ds(core * seq, seq), pl.ds(j * kv4, kv4)]
                    if slot == 0 and core == 0:
                        cp = pltpu.make_async_copy(src, dst.at[:, mine], kv_s.at[slot, core, j])
                        cp.start()
                        local_kv.append(cp)
                    else:
                        go(remote(src, dst.at[:, mine], kv_s.at[slot, core, j], kv_r.at[slot, j], w.square(slot, core)))
        local_kv = []

        def here(slot, q):
            arrived(xa.at[slot, 1, bits[q]], xs_r.at[slot, q])

        seqs = [pl.ds(h * seq, seq) for h in range(2)]

        def send_ctx(base, h):
            for slot in (base, base + 2):
                spread(ca, slot, cs_s, cs_r, seqs[h], (h,))

        def relay_ctx(q, h):
            for slot in ((2, 0) if q == 2 else (0, 2)):
                relay(ca, slot, q, cs_s, cs_r, seqs[h], (h,))

        attend(0, 0)
        send_ctx(0, 0)
        here(2, 0)
        go(remote(xa.at[2, 1, bits[0]], xa.at[3, 1, bits[0]], xs_s.at[4], xs_r.at[3, 0], y))
        here(1, 1)
        go(remote(xa.at[1, 1, bits[1]], xa.at[3, 1, bits[1]], xs_s.at[5], xs_r.at[3, 1], x))
        attend(1, 0)
        send_ctx(1, 0)
        relay_ctx(2, 0)
        here(2, 1)
        attend(0, 1)
        send_ctx(0, 1)
        relay_ctx(1, 0)
        for slot, q in ((1, 0), (3, 0), (3, 1)):
            here(slot, q)
        attend(1, 1)
        send_ctx(1, 1)
        relay_ctx(2, 1)
        relay_ctx(1, 1)
        load(1, wd.at[0], lsem.at[0])
        for slot in range(4):
            send_kv(slot)
        arrived(wd.at[0], lsem.at[0])
        n_ctx = len(sent)

        def mid(slot):
            for q in (1, 2, 3):
                if q == 3 or slot in (1, 3):
                    for h in range(2):
                        take(ca, slot, q, cs_r, seqs[h], (h,))

            def one(nt, carry):
                c = aligned(nt * 256, 256, LANES)
                o = aligned(w.me * pc.w4 + nt * 256, 256, LANES)
                got = jnp.dot(ca[slot], wd[0, :, :, c].reshape(width, 256), preferred_element_type=F32)
                res = xa[slot, :, :, o].reshape(rows_b, 256).astype(F32)
                xm[slot, :, o] = (res + got).astype(BF16)
                return carry
            lax.fori_loop(0, pc.w4 // 256, one, 0)
            spread(xm, slot, ms_s, ms_r)

        mid(3)
        mid(1)
        mid(2)
        relay(xm, 1, 2, ms_s, ms_r)
        mid(0)
        relay(xm, 3, 2, ms_s, ms_r)
        relay(xm, 3, 1, ms_s, ms_r)
        relay(xm, 1, 1, ms_s, ms_r)
        for cp in sent[:n_ctx]:
            cp.wait_send()
        del sent[:n_ctx]
        gate_w = pc.gu_w // 2
        at = {0: 0, 2: 1, 1: 2, 3: 3}

        def gate_up(group, b):
            step = 4 * group + b
            if step < 7:
                load(2 + (b + 1) % 4, wg.at[(step + 1) % 2], lsem.at[1 + (step + 1) % 2], step < 3)
            arrived(wg.at[step % 2], lsem.at[1 + step % 2])

            def one(nt, carry):
                act = h2[pl.ds(2 * group, 2)].reshape(2 * rows_b, width)
                gate = jnp.dot(act, wg[step % 2, :, :, aligned(nt * 256, 256, LANES)].reshape(width, 256), preferred_element_type=F32)
                up = jnp.dot(act, wg[step % 2, :, :, aligned(gate_w + nt * 256, 256, LANES)].reshape(width, 256), preferred_element_type=F32)
                val = (jax.nn.silu(gate) * up).astype(BF16)
                mm[pl.ds(2 * group, 2), :, aligned(b * gate_w + nt * 256, 256, LANES)] = val.reshape(2, rows_b, 256)
                return carry
            lax.fori_loop(0, gate_w // 256, one, 0)

        load(2, wg.at[0], lsem.at[1])
        for group, slots in enumerate(((0, 2), (1, 3))):
            for slot in slots:
                for q in (1, 2, 3):
                    if q == 3 or slot in (0, 2):
                        take(xm, slot, q, ms_r)
                norm_into(h2, at[slot], lambda rows, i, slot=slot: xm[slot, rows, :], g2_ref)
            for b in range(4):
                gate_up(group, b)

        h0, h1 = pl.ds(0, half), pl.ds(half, half)
        first_sends, home = {}, []

        def phase1(n):
            for old in first_sends.get(n - 2, ()):
                old.wait_send()
            par = n % 2
            arrived(wd.at[par], lsem.at[3 + par])

            def one(j, carry):
                s, nt = j // (pc.dn_w // 256), j % (pc.dn_w // 256)
                c = aligned(nt * 256, 256, LANES)
                act = mm[pl.ds(2 * s, 2)].reshape(2 * rows_b, mm.shape[2])
                got = jnp.dot(act, wd[par, :, :, c].reshape(mm.shape[2], 256), preferred_element_type=F32)
                pp[par, pl.ds(2 * s, 2), :, c] = got.reshape(2, rows_b, 256)
                return carry
            lax.fori_loop(0, 2 * (pc.dn_w // 256), one, 0)
            first_sends[n] = []
            for path, dev, cc, rels in ((0, x, h0, (2, 3)), (1, y, h1, (1, 3))):
                for j, rel in enumerate(rels):
                    cp = remote(pp.at[par, at[rel], :, cc], r1.at[n, path, j], p1_s.at[n, path, j], p1_r.at[n, path, j], dev)
                    cp.start()
                    first_sends[n].append(cp)

        def phase2(n):
            par = n % 2
            for path, dev, cc, rel in ((0, y, h0, 1), (1, x, h1, 2)):
                arrived(r1.at[n, path, 1], p1_r.at[n, path, 1])
                r1[n, path, 1] = pp[par, at[rel], :, cc] + r1[n, path, 1]
                go(remote(r1.at[n, path, 1], r2.at[n, path], p2_s.at[n, path], p2_r.at[n, path], dev))
            for path, cc in ((0, h0), (1, h1)):
                arrived(r1.at[n, path, 0], p1_r.at[n, path, 0])
                r1[n, path, 0] = pp[par, 0, :, cc] + r1[n, path, 0]

        def phase3(n):
            for path in range(2):
                arrived(r2.at[n, path], p2_r.at[n, path])
                c = pl.ds(n * pc.dn_w + path * half, half)
                total = xm[0, :, c].astype(F32) + (r1[n, path, 0] + r2[n, path])
                xm[0, :, c] = total.astype(BF16)
            c = pl.ds(n * pc.dn_w, pc.dn_w)
            go(remote(xm.at[0, pl.ds(seq, seq), c], out_ref.at[:, c], o_s.at[n], o_r.at[n], w.partner()))
            cp = pltpu.make_async_copy(xm.at[0, pl.ds(0, seq), c], out_ref.at[:, c], o_l.at[n])
            cp.start()
            home.append(cp)

        for cp in sent:
            cp.wait_send()
        sent.clear()
        def load_down(n):
            load(last_gu + 1 + n, wd.at[n % 2], lsem.at[3 + n % 2])

        load_down(0)
        for n in range(4):
            phase1(n)
            if n >= 1:
                phase2(n - 1)
            if n >= 2:
                phase3(n - 2)
            if n < 3:
                load_down(n + 1)
        phase2(3)
        phase3(2)
        phase3(3)

        for cp in sent:
            cp.wait_send()
        for n in (2, 3):
            for cp in first_sends[n]:
                cp.wait_send()
        for cp in local_kv + home:
            cp.wait()
        for rel in (1, 2, 3):
            arrived(k_ref.at[:, pl.ds(0, kv4)], kv_r.at[rel, 0])
            arrived(v_ref.at[:, pl.ds(0, kv4)], kv_r.at[rel, 1])

    pl.when(w.c == 1)(stream)
    pl.when(w.c == 0)(compute)


def layer(side, pc, head_dim, x, xb, q_all, near, g1, g2, cos_tab, sin_tab):
    _, seq, width = x.shape
    rows_b = 2 * seq
    kv_width = 4 * pc.kv4
    n_chunk = len(pc.chunks)
    far = pc.n_fsdp // 4
    ff4 = pc.f4 * pc.n_fsdp
    half = pc.dn_w // 2
    hbm = pl.BlockSpec(memory_space=pl.ANY)
    vmem = pl.BlockSpec(memory_space=pltpu.VMEM)
    dma = pltpu.SemaphoreType.DMA
    return pl.pallas_call(
        functools.partial(layer_kernel, side, pc, head_dim),
        out_shape=(
            jax.ShapeDtypeStruct((seq, width), BF16),
            jax.ShapeDtypeStruct((seq, kv_width), BF16),
            jax.ShapeDtypeStruct((seq, kv_width), BF16),
            jax.ShapeDtypeStruct((pc.n_fsdp, pc.rows, pc.late), BF16)),
        in_specs=[hbm] * (3 + len(near)) + [vmem, vmem, vmem, vmem],
        out_specs=(hbm, hbm, hbm, hbm),
        scratch_shapes=[
            pltpu.VMEM((4, 2, seq, width), BF16),
            pltpu.VMEM((4, rows_b, width), BF16),
            pltpu.VMEM((4, rows_b, width), BF16),
            pltpu.VMEM((2, pc.n_fsdp, pc.rows, pc.gu_w), BF16),
            pltpu.VMEM((2, pc.n_fsdp, pc.rows, pc.dn_w), BF16),
            pltpu.VMEM((4, rows_b, max(ff4, width)), BF16),
            pltpu.VMEM((2, 4, rows_b, pc.dn_w), F32),
            pltpu.VMEM((4, 2, 2, rows_b, half), F32),
            pltpu.VMEM((4, 2, rows_b, half), F32),
            pltpu.VMEM((rows_b, pc.qkv), F32),
            pltpu.VMEM((4, rows_b, 2 * pc.kv4), BF16),
            dma((5,)),
            dma((6,)), dma((4, 2)),
            dma((4, 2, 3)), dma((4, 2, 3)),
            dma((4, 3)), dma((4, 3)),
            dma((4, 2, 2)), dma((4, 2)),
            dma((4, 2, 2)), dma((4, 2, 2)),
            dma((4, 2)), dma((4, 2)),
            dma((4,)), dma((4,)), dma((4,)),
            dma((n_chunk, 2, far + 1)), dma((n_chunk, 2, far + 1)), dma((n_chunk, 2, far + 1)), dma((n_chunk,)),
        ],
        compiler_params=pltpu.CompilerParams(collective_id=2, has_side_effects=True, vmem_limit_bytes=67043328),
        name='layer',
    )(x, xb, q_all, *near, g1, g2, cos_tab, sin_tab)


def solution(mesh):
    batch_axes = ('dp', 'fsdp')
    row_spec = P('fsdp', None)
    n_dp = mesh.shape['dp']
    n_fsdp = mesh.shape['fsdp']
    side = math.isqrt(n_dp)

    def device_step(tokens, embed_table, norm_attn, w_qkv, w_out, norm_mlp, w_gate_up, w_down, rope_scale):
        seq = tokens.shape[1]
        shard_rows, width = embed_table.shape
        head_dim = 2 * rope_scale.shape[0]
        rows = w_out.shape[0]
        q_width = rows * n_fsdp
        kv_width = (w_qkv.shape[1] - q_width) // 2
        pc = Pieces(rows, q_width // 4, kv_width // 4, width // 4, w_down.shape[0] // 4, n_fsdp, width)

        gains = jnp.stack([norm_attn, norm_mlp]).astype(F32)
        ids, gains, pe, pd = gather_ids(side, pc, tokens, gains, w_qkv, w_out, w_gate_up, w_down)
        def first_hop(piece, dz):
            return lax.ppermute(piece, 'fsdp', [(i, (i + 2 * dz) % n_fsdp) for i in range(n_fsdp)])

        f0, f1 = first_hop(pe, 1), first_hop(pe, -1)
        ids = ids.reshape(-1) - lax.axis_index('fsdp') * shard_rows
        owned = (ids >= 0) & (ids < shard_rows)
        table_rows = gather_table(ids, owned, embed_table)
        g1 = gains[:, 0].reshape(1, width)
        g2 = gains[:, 1].reshape(1, width)

        freq_expo = jnp.arange(head_dim // 2, dtype=F32) * (2.0 / head_dim)
        inv_freq = 1.0 / (rope_scale * jnp.power(ROPE_THETA, freq_expo))
        angles = jnp.arange(seq, dtype=F32)[:, None] * inv_freq[None, :]
        cos_tab, sin_tab = jnp.cos(angles), jnp.sin(angles)
        reps = LANES // head_dim
        cos_tab = jnp.concatenate([cos_tab, cos_tab] * reps, axis=1)
        sin_tab = jnp.concatenate([-sin_tab, sin_tab] * reps, axis=1)

        table_rows = table_rows.reshape(n_fsdp // 2, 2, seq, width)
        x, xb, q_all, te, td, tf = embed(side, pc, table_rows, pe, pd, f0, f1)
        out, k, v, _ = layer(side, pc, head_dim, x, xb, q_all, (pe, pd, f0, f1, te, td, tf), g1, g2, cos_tab, sin_tab)
        heads = (1, seq, kv_width // head_dim, head_dim)
        return out[None], k.reshape(heads), v.reshape(heads)

    return jax.shard_map(
        device_step,
        mesh=mesh,
        in_specs=(P(batch_axes, None), row_spec, P('fsdp'), row_spec, row_spec, P('fsdp'), row_spec, row_spec, P(None)),
        out_specs=(P(batch_axes, None, None), P(batch_axes, None, None, None), P(batch_axes, None, None, None)),
        check_vma=False,
    )
```

```python
import functools
import math

import jax
import jax.numpy as jnp
from jax import lax
from jax.experimental import pallas as pl
from jax.experimental.pallas import tpu as pltpu
from jax.sharding import PartitionSpec as P

NORM_EPS = 1e-5
ROPE_THETA = 10000.0
PICK = 32
DEPTH = 4
LANES = 128
MESH = pl.DeviceIdType.MESH
BF16 = jnp.bfloat16
F32 = jnp.float32


def aligned(start, size, step):
    return pl.ds(pl.multiple_of(start, step), size)


class Where:
    def __init__(self, side, n_fsdp):
        self.side = side
        self.nz = n_fsdp // 2
        self.dp = lax.axis_index('dp')
        self.f = lax.axis_index('fsdp')
        self.z = self.f // 2
        self.c = self.f % 2
        self.px = self.dp // side
        self.py = self.dp % side
        self.me = 2 * (self.px % 2) + self.py % 2

    def chip(self, dz):
        return lax.rem(self.z + dz + self.nz, self.nz)

    def along_z(self, dz, core):
        return (self.dp, 2 * self.chip(dz) + core)

    def partner(self):
        return (self.dp, 2 * self.z + 1 - self.c)

    def square(self, rel, core):
        px = self.px + (1 - 2 * (self.px % 2)) if rel & 2 else self.px
        py = self.py + (1 - 2 * (self.py % 2)) if rel & 1 else self.py
        return (px * self.side + py, 2 * self.z + core)


def greet(devices):
    barrier = pltpu.get_barrier_semaphore()
    for dev in devices:
        pl.semaphore_signal(barrier, inc=1, device_id=dev, device_id_type=MESH)
    pl.semaphore_wait(barrier, len(devices))


def remote(src, dst, ssem, rsem, dev):
    return pltpu.make_async_remote_copy(src_ref=src, dst_ref=dst, send_sem=ssem, recv_sem=rsem, device_id=dev, device_id_type=MESH)


def arrived(ref, sem):
    pltpu.make_async_copy(ref, ref, sem).wait()


def ids_kernel(side, pc, tok_ref, gain_ref, w_qkv, w_out, w_gu, w_dn, ids_ref, gains_ref, pe_ref, pd_ref,
               pk, lsem, ssem, rsem, pack_sem, store_sem):
    n_fsdp = pc.n_fsdp
    w = Where(side, n_fsdp)
    pack_copies(pc, w.me, pk, w_qkv, w_out, w_gu, w_dn, pack_sem)
    greet([(w.dp, lax.rem(w.f + k, n_fsdp)) for k in range(1, n_fsdp)])
    own = [pltpu.make_async_copy(tok_ref, ids_ref.at[w.f], lsem.at[0]),
           pltpu.make_async_copy(gain_ref, gains_ref.at[w.f], lsem.at[1])]
    for cp in own:
        cp.start()
    sent = []
    for k in range(1, n_fsdp):
        dev = (w.dp, lax.rem(w.f + k, n_fsdp))
        for j, (src, dst) in enumerate(((tok_ref, ids_ref), (gain_ref, gains_ref))):
            cp = remote(src, dst.at[w.f], ssem.at[j, k], rsem.at[j, k], dev)
            cp.start()
            sent.append(cp)
    arrived(pk, pack_sem)
    lo = 0
    stores = []
    for j, ref in enumerate((pe_ref, pd_ref)):
        stores.append(pltpu.make_async_copy(pk.at[:, pl.ds(lo, ref.shape[1])], ref, store_sem.at[j]))
        stores[-1].start()
        lo += ref.shape[1]
    for cp in own + stores:
        cp.wait()
    for cp in sent:
        cp.wait_send()
    for k in range(1, n_fsdp):
        src = lax.rem(w.f - k + n_fsdp, n_fsdp)
        arrived(ids_ref.at[src], rsem.at[0, k])
        arrived(gains_ref.at[src], rsem.at[1, k])


class Pieces:
    def __init__(self, rows, q4, kv4, w4, f4, n_fsdp, width):
        self.rows = rows
        self.q4, self.kv4, self.w4, self.f4 = q4, kv4, w4, f4
        self.n_fsdp = n_fsdp
        self.width = width
        self.qkv = q4 + 2 * kv4
        self.gu0 = self.qkv + w4
        self.gu_w = 2 * f4 * n_fsdp // 4
        self.dn0 = self.gu0 + 4 * self.gu_w
        self.n_dn = 8
        self.dn_w = width // self.n_dn
        self.total = self.dn0 + width
        self.late = self.total - self.qkv
        self.chunks = [(0, self.qkv), (self.qkv, w4)]
        self.chunks += [(self.gu0 + b * self.gu_w, self.gu_w) for b in range(4)]
        self.chunks += [(self.dn0 + n * self.dn_w, self.dn_w) for n in range(self.n_dn)]
        self.early = 6


def pack_copies(pc, me, pk, w_qkv, w_out, w_gu, w_dn, sem):
    q4, kv4, w4, f4 = pc.q4, pc.kv4, pc.w4, pc.f4
    first = [
        (w_qkv.at[:, aligned(me * q4, q4, LANES)], pk.at[:, pl.ds(0, q4)]),
        (w_qkv.at[:, aligned(4 * q4 + me * kv4, kv4, LANES)], pk.at[:, pl.ds(q4, kv4)]),
        (w_qkv.at[:, aligned(4 * q4 + 4 * kv4 + me * kv4, kv4, LANES)], pk.at[:, pl.ds(q4 + kv4, kv4)]),
    ]
    for src, dst in first:
        pltpu.make_async_copy(src, dst, sem).start()
    pltpu.make_async_copy(w_out.at[:, aligned(me * w4, w4, LANES)], pk.at[:, pl.ds(pc.qkv, w4)], sem).start()
    ff = 4 * f4 * pc.n_fsdp
    for d in range(pc.n_fsdp):
        b, k = d // 4, d % 4
        for part in range(2):
            src = w_gu.at[:, aligned(part * ff + d * 4 * f4 + me * f4, f4, LANES)]
            dst = pk.at[:, pl.ds(pc.gu0 + b * pc.gu_w + part * (pc.gu_w // 2) + k * f4, f4)]
            pltpu.make_async_copy(src, dst, sem).start()
    pltpu.make_async_copy(w_dn.at[aligned(me * f4, f4, LANES), :], pk.at[:, pl.ds(pc.dn0, pc.width)], sem).start()


def gather_ids(side, pc, tokens, gains, w_qkv, w_out, w_gu, w_dn):
    n_fsdp = pc.n_fsdp
    vmem, hbm = pl.BlockSpec(memory_space=pltpu.VMEM), pl.BlockSpec(memory_space=pl.ANY)
    dma = pltpu.SemaphoreType.DMA
    return pl.pallas_call(
        functools.partial(ids_kernel, side, pc),
        out_shape=(
            jax.ShapeDtypeStruct((n_fsdp,) + tokens.shape, tokens.dtype),
            jax.ShapeDtypeStruct((n_fsdp,) + gains.shape, gains.dtype),
            jax.ShapeDtypeStruct((pc.rows, pc.dn0), BF16),
            jax.ShapeDtypeStruct((pc.rows, pc.width), BF16)),
        in_specs=[vmem, vmem, hbm, hbm, hbm, hbm],
        out_specs=(vmem, vmem, hbm, hbm),
        scratch_shapes=[pltpu.VMEM((pc.rows, pc.total), BF16), dma((2,)), dma((2, n_fsdp)), dma((2, n_fsdp)), dma, dma((2,))],
        compiler_params=pltpu.CompilerParams(collective_id=0, has_side_effects=True),
        name='ids',
    )(tokens, gains, w_qkv, w_out, w_gu, w_dn)


def gather_kernel(n_tok, gid_ref, tgt_ref, table_ref, out_ref, buf, sems):
    width = table_ref.shape[2]
    n_step = n_tok // PICK

    def fetch(step, slot):
        for i in range(PICK):
            pltpu.make_async_copy(table_ref.at[gid_ref[step * PICK + i]], buf.at[slot, i], sems.at[slot]).start()

    for j in range(DEPTH - 1):
        fetch(j, j)

    def body(step, carry):
        slot = lax.rem(step, DEPTH)

        @pl.when(step + DEPTH - 1 < n_step)
        def _():
            fetch(step + DEPTH - 1, lax.rem(step + DEPTH - 1, DEPTH))
        arrived(buf.at[slot], sems.at[slot])
        rows = aligned(step * PICK, PICK, PICK)
        hot = (lax.broadcasted_iota(jnp.int32, (PICK, PICK * 8), 1) == tgt_ref[rows, :]).astype(BF16)
        got = jnp.dot(hot, buf[slot].reshape(PICK * 8, width), preferred_element_type=F32)
        out_ref[rows, :] = got.astype(BF16)
        return carry
    lax.fori_loop(0, n_step, body, 0)


def gather_table(ids, owned, table):
    n_tok = ids.shape[0]
    n_rows, width = table.shape
    gid = jnp.where(owned, ids // 8, jnp.arange(n_tok, dtype=jnp.int32) % (n_rows // 8))
    place = jnp.arange(n_tok, dtype=jnp.int32) % PICK
    tgt = jnp.where(owned, 8 * place + ids % 8, -1)[:, None]
    return pl.pallas_call(
        functools.partial(gather_kernel, n_tok),
        out_shape=jax.ShapeDtypeStruct((n_tok, width), BF16),
        in_specs=[pl.BlockSpec(memory_space=pltpu.SMEM), pl.BlockSpec(memory_space=pltpu.VMEM), pl.BlockSpec(memory_space=pl.ANY)],
        out_specs=pl.BlockSpec(memory_space=pltpu.VMEM),
        scratch_shapes=[pltpu.VMEM((DEPTH, PICK, 8, width), BF16), pltpu.SemaphoreType.DMA((DEPTH,))],
        compiler_params=pltpu.CompilerParams(vmem_limit_bytes=48 * 2**20),
        cost_estimate=pl.CostEstimate(flops=80 * 10**9, bytes_accessed=9 * n_tok * width * 2, transcendentals=0),
        name='rows',
    )(gid, tgt, table.reshape(n_rows // 8, 8, width))


def embed_kernel(side, pc, rows_ref, pe_ref, pd_ref, f0_ref, f1_ref, xa_ref, xb_ref, q_ref, te_ref, td_ref, tf_ref,
                 got, peer, rp, sb, pk, xo,
                 got_sem, pack_sem, own_sem, d2d_s, d2d_r, f_s, f_r, push_s, push_r,
                 peer_s, peer_r, rs_s, rs_r, home_sem, x_s, x_r):
    n_fsdp = pc.n_fsdp
    w = Where(side, n_fsdp)
    nz = w.nz
    far = nz // 2
    seq = got.shape[2]
    hw = got.shape[3]
    width = 2 * hw
    order = [far]
    for o in range(far - 1, 0, -1):
        order += [o, -o]
    order += [0]
    mine = aligned(w.c * hw, hw, LANES)
    other = aligned((1 - w.c) * hw, hw, LANES)
    for k in range(len(order)):
        dest = w.chip(order[k])
        pltpu.make_async_copy(rows_ref.at[dest, :, :, mine], got.at[dest], got_sem.at[k]).start()
    q_srcs = [ref.at[:, pl.ds(0, pc.qkv)] for ref in (pe_ref, f0_ref, f1_ref)]
    for j, src in enumerate(q_srcs):
        pltpu.make_async_copy(src, pk.at[j], pack_sem.at[j]).start()
    greet([w.partner()] + [w.along_z(dz, core) for dz in (1, -1) for core in (0, 1)] + [w.square(rel, core) for rel in (1, 2) for core in (0, 1)])
    dirs = (1, -1)

    for k in range(len(order)):
        dest = w.chip(order[k])
        remote(rows_ref.at[dest, :, :, other], peer.at[dest], peer_s.at[k], peer_r.at[k], w.partner()).start()

    here_q = (2 * w.z + w.c, 2 * w.chip(-1) + w.c, 2 * w.chip(1) + w.c)
    swaps = [(src, q_ref.at[here_q[j]]) for j, src in enumerate(q_srcs)]
    rest = pl.ds(pc.qkv, pc.dn0 - pc.qkv)
    swaps += [(pe_ref.at[:, rest], te_ref), (pd_ref, td_ref), (f0_ref.at[:, rest], tf_ref.at[0]), (f1_ref.at[:, rest], tf_ref.at[1])]
    own = [remote(src, dst, d2d_s.at[j], d2d_r.at[j], w.partner()) for j, (src, dst) in enumerate(swaps)]


    def pair(dz):
        return q_ref.at[pl.ds(2 * w.chip(dz), 2)]

    def single(dz, i):
        return q_ref.at[pl.ds(2 * w.chip(dz) + i, 1)]

    def push(ref, i, h):
        remote(ref, ref, push_s.at[i, h], push_r, w.partner()).start()

    local = []

    def forward(h):
        @pl.when(w.c == 1)
        def _():
            for i, dz in enumerate(dirs):
                if h == 1:
                    local[1 + i].wait()
                    own[1 + i].wait_recv()
                elif h < far:
                    arrived(pair(-dz * h), f_r.at[i, h])
                else:
                    arrived(single(-dz * h, i), f_r.at[i, h])
                if h < far - 1:
                    remote(pair(-dz * h), pair(-dz * h), f_s.at[i, h + 1], f_r.at[i, h + 1], w.along_z(dz, 1)).start()
                elif h == far - 1:
                    remote(single(-dz * h, i), single(-dz * h, i), f_s.at[i, h + 1], f_r.at[i, h + 1], w.along_z(dz, 1)).start()
                if h > 1:
                    push(pair(-dz * h) if h < far else single(-dz * h, i), i, h)

    def addto(dst, terms, q):
        def one(r, carry):
            rows = aligned(q * (seq // 2) + r * 32, 32, 32)
            val = terms[0](rows)
            for term in terms[1:]:
                val = val + term(rows)
            dst(rows, val)
            return carry
        lax.fori_loop(0, seq // 64, one, 0)

    def part(ref, q):
        return ref.at[pl.ds(q * (seq // 2), seq // 2)]

    def rs_stage(k, h):
        o = order[k]
        dest = w.chip(o)
        if h == 0:
            arrived(got.at[dest], got_sem.at[k])
            arrived(peer.at[dest], peer_r.at[k])
        if o == 0:
            return
        dist = abs(o)
        for i, dz in enumerate(dirs):
            if (o * dz < 0 and o != far) or (dist == far and h != i):
                continue
            for q in range(2):
                terms = [lambda r: got[dest, h, r, :], lambda r: peer[dest, h, r, :]]
                if dist < far - 1 or (dist == far - 1 and h == i):
                    arrived(part(rp.at[i, dist, h], q), rs_r.at[i, dist, h, q])
                    terms.append(lambda r, i=i: rp[i, dist, h, r, :])

                def put(r, val, i=i):
                    sb[i, dist - 1, h, r, :] = val
                addto(put, terms, q)
                remote(part(sb.at[i, dist - 1, h], q), part(rp.at[i, dist - 1, h], q), rs_s.at[i, dist - 1, h, q],
                       rs_r.at[i, dist - 1, h, q], w.along_z(dz, w.c)).start()

    def finish(h):
        for q in range(2):
            terms = [lambda r: got[w.z, h, r, :], lambda r: peer[w.z, h, r, :]]
            for i in range(2):
                arrived(part(rp.at[i, 0, h], q), rs_r.at[i, 0, h, q])
                terms.append(lambda r, i=i: rp[i, 0, h, r, :])

            def put(r, val):
                xo[h, r, :] = val
            addto(put, terms, q)
        dst = (xa_ref.at[0] if h == 0 else xb_ref).at[:, mine]

        @pl.when(w.c == 0)
        def _():
            pltpu.make_async_copy(xo.at[h], dst, home_sem.at[h]).start()

        @pl.when(w.c == 1)
        def _():
            remote(xo.at[h], dst, home_sem.at[h], x_r.at[0, h], w.partner()).start()

    sides = ((2, w.square(2, 0)), (1, w.square(1, 0)))
    spread = [remote(xo.at[0], xa_ref.at[rel, :, mine], x_s.at[j], x_r.at[rel, w.c], dev) for j, (rel, dev) in enumerate(sides)]
    col = [pl.ds(j * hw, hw) for j in range(2)]
    relay = [remote(xa_ref.at[rel, :, col[j]], xa_ref.at[3, :, col[j]], x_s.at[2 + j], x_r.at[3, j], sides[1 - j][1]) for j, (rel, _) in enumerate(sides)]

    for j in range(3):
        arrived(pk.at[j], pack_sem.at[j])
        local.append(pltpu.make_async_copy(pk.at[j], q_ref.at[here_q[j]], own_sem.at[j]))
    last = len(order) - 1
    for k in range(last + 1):
        rs_stage(k, 0)
        if k == 0:
            for cp in own[:3] + local:
                cp.start()
        if k == 2:
            for cp in own[3:]:
                cp.start()
            forward(1)
        if k == 5:
            forward(2)
    for k in range(3):
        rs_stage(k, 1)
    finish(0)
    for cp in spread:
        cp.start()
    for k in range(3, last + 1):
        rs_stage(k, 1)
        if k == 4:
            forward(3)
        if k == last - 1:
            @pl.when(w.c == 0)
            def _():
                for j, (rel, _) in enumerate(sides):
                    arrived(xa_ref.at[rel, :, col[j]], x_r.at[rel, j])
                    relay[j].start()
    forward(4)
    finish(1)

    for cp in own[:1] + own[3:]:
        cp.wait()
    for cp in own[1:3]:
        cp.wait_send()
    local[0].wait()
    for cp in spread:
        cp.wait_send()
    for k in range(len(order)):
        dest = w.chip(order[k])
        arrived(peer.at[dest], peer_s.at[k])
    for i in range(2):
        for dist in range(1, far + 1):
            for h in ((i,) if dist == far else (0, 1)):
                for q in range(2):
                    arrived(part(sb.at[i, dist - 1, h], q), rs_s.at[i, dist - 1, h, q])

    @pl.when(w.c == 1)
    def _():
        for i, dz in enumerate(dirs):
            for h in range(1, far + 1):
                ref = pair(-dz * h) if h < far else single(-dz * h, i)
                if h > 1:
                    arrived(ref, push_s.at[i, h])
                if h < far:
                    arrived(pair(-dz * h) if h < far - 1 else single(-dz * h, i), f_s.at[i, h + 1])

    @pl.when(w.c == 0)
    def _():
        arrived(q_ref.at[pl.ds(0, n_fsdp - 6)], push_r)
        for j in (1, 2):
            local[j].wait()
            own[j].wait_recv()
        arrived(xa_ref.at[0, :, col[1]], x_r.at[0, 0])
        arrived(xb_ref.at[:, col[1]], x_r.at[0, 1])
        arrived(xa_ref.at[2, :, col[1]], x_r.at[2, 1])
        arrived(xa_ref.at[1, :, col[0]], x_r.at[1, 0])
        for j in range(2):
            arrived(xa_ref.at[3, :, col[j]], x_r.at[3, j])
            relay[j].wait_send()
    for h in range(2):
        arrived(xo.at[h], home_sem.at[h])


def embed(side, pc, rows, pe, pd, f0, f1):
    seq, width = rows.shape[2], rows.shape[3]
    nz = pc.n_fsdp // 2
    far = nz // 2
    hbm = pl.BlockSpec(memory_space=pl.ANY)
    dma = pltpu.SemaphoreType.DMA
    return pl.pallas_call(
        functools.partial(embed_kernel, side, pc),
        out_shape=(
            jax.ShapeDtypeStruct((4, seq, width), BF16),
            jax.ShapeDtypeStruct((seq, width), BF16),
            jax.ShapeDtypeStruct((pc.n_fsdp, pc.rows, pc.qkv), BF16),
            jax.ShapeDtypeStruct((pc.rows, pc.dn0 - pc.qkv), BF16),
            jax.ShapeDtypeStruct(pd.shape, BF16),
            jax.ShapeDtypeStruct((2, pc.rows, pc.dn0 - pc.qkv), BF16)),
        in_specs=[hbm] * 5,
        out_specs=(hbm,) * 6,
        scratch_shapes=[
            pltpu.VMEM((nz, 2, seq, width // 2), BF16),
            pltpu.VMEM((nz, 2, seq, width // 2), BF16),
            pltpu.VMEM((2, far, 2, seq, width // 2), BF16),
            pltpu.VMEM((2, far, 2, seq, width // 2), BF16),
            pltpu.VMEM((3, pc.rows, pc.qkv), BF16),
            pltpu.VMEM((2, seq, width // 2), BF16),
            dma((nz,)), dma((3,)), dma((3,)), dma((7,)), dma((7,)),
            dma((2, far + 1)), dma((2, far + 1)), dma((2, far + 1)), dma,
            dma((nz,)), dma((nz,)),
            dma((2, far, 2, 2)), dma((2, far, 2, 2)),
            dma((2,)), dma((4,)), dma((4, 2)),
        ],
        compiler_params=pltpu.CompilerParams(collective_id=1, has_side_effects=True, vmem_limit_bytes=67043328),
        name='embed',
    )(rows, pe, pd, f0, f1)


def layer_kernel(side, pc, head_dim, x_ref, xb_ref, q_ref, pe_ref, pd_ref, f0_ref, f1_ref, te_ref, td_ref, tf_ref, g1_ref, g2_ref, cos_ref, sin_ref, out_ref, k_ref, v_ref, w_ref,
                 xa, ca, xm, wg, wd, mm, pp, r1, r2, qf, kvb,
                 lsem, xs_s, xs_r, cs_s, cs_r, ms_s, ms_r, kv_s, kv_r, p1_s, p1_r, p2_s, p2_r, o_s, o_l, o_r,
                 zs, zr, ps, wch):
    h2 = ca
    n_fsdp = pc.n_fsdp
    w = Where(side, n_fsdp)
    far = w.nz // 2
    seq, width = xa.shape[2], xa.shape[3]
    rows_b = 2 * seq
    half = pc.dn_w // 2
    n_chunk = len(pc.chunks)
    last_gu = 5
    greet([w.partner(), w.along_z(1, w.c), w.along_z(-1, w.c)] + [w.square(rel, core) for rel in (1, 2, 3) for core in (0, 1)])
    dirs = (1, -1)

    def slim(t, mine):
        off, cw = pc.chunks[t]
        return pl.ds(off - pc.dn0 if t >= pc.early else off - (0 if mine else pc.qkv), cw)

    def own_pieces(t):
        refs = (pe_ref, te_ref) if t < pc.early else (pd_ref, td_ref)
        return [refs[0].at[:, slim(t, True)], refs[1].at[:, slim(t, False)]]

    def near_pieces(t, i):
        return [(f0_ref, f1_ref)[i].at[:, slim(t, True)], tf_ref.at[i, :, slim(t, False)]]

    def stream():
        def cols(t):
            off, cw = pc.chunks[t]
            return pl.ds(off - pc.qkv, cw)

        def pair(t, dz):
            return w_ref.at[pl.ds(2 * w.chip(dz), 2), :, cols(t)]

        def single(t, dz, i):
            return w_ref.at[pl.ds(2 * w.chip(dz) + i, 1), :, cols(t)]

        def piece(t, h, i):
            dz = dirs[i]
            return pair(t, -dz * h) if h < far else single(t, -dz * h, i)

        sent = []

        def hop(t, h):
            if t < 1 or t >= n_chunk or (h == 0 and t < pc.early):
                return
            ready = h == 1 and t < pc.early
            for i in range(2):
                dz = dirs[i]
                if h > 0 and not ready:
                    arrived(piece(t, h, i), zr.at[t, i, h])
                if h == far:
                    continue
                ref = pair(t, -dz * h) if h < far - 1 else single(t, -dz * h, i)
                sems = (zs.at[t, i, h], zr.at[t, i, h + 1], w.along_z(dz, 1))
                if h == 0 or ready:
                    pieces = near_pieces(t, i) if ready else own_pieces(t)
                    for src, core in zip(pieces, (1, 0)):
                        remote(src, w_ref.at[2 * w.chip(-dz * h) + core, :, cols(t)], *sems).start()
                else:
                    remote(ref, ref, *sems).start()
                sent.append((ref, zs.at[t, i, h]))
            if h > 0 and not ready:
                for i in range(2):
                    ref = piece(t, h, i)
                    remote(ref, ref, ps.at[t, i, h], wch.at[t], w.partner()).start()
                    sent.append((ref, ps.at[t, i, h]))

        for s in range(n_chunk + far):
            for h in range(far, -1, -1):
                hop(s - h if h > 1 else s + 1 - h, h)
        for ref, sem in sent:
            arrived(ref, sem)
        kvw = 2 * (kvb.shape[2] // 4)
        for rel in range(4):
            arrived(k_ref.at[:, pl.ds(0, kvw)], kv_r.at[rel, 0])
            arrived(v_ref.at[:, pl.ds(0, kvw)], kv_r.at[rel, 1])
        for n in range(pc.n_dn):
            arrived(out_ref.at[:, pl.ds(n * pc.dn_w, pc.dn_w)], o_r.at[n])

    def compute():
        y, x = w.square(1, 0), w.square(2, 0)
        q4, kv4 = pc.q4, pc.kv4
        cols = {q: aligned((w.me ^ q) * pc.w4, pc.w4, LANES) for q in range(4)}
        sent = []

        def go(cp):
            cp.start()
            sent.append(cp)

        def load(t, dst, sem, first=True):
            off, cw = pc.chunks[t]
            c = pl.ds(off - pc.qkv, cw)
            near = t < pc.early
            if first:
                arrived(w_ref.at[pl.ds(0, n_fsdp - (6 if near else 2)), :, c], wch.at[t])
            for dz in range(-1, w.nz - 1):
                two = pl.ds(2 * w.chip(dz), 2)
                if dz == 0 or (near and dz in (1, -1)):
                    pieces = own_pieces(t) if dz == 0 else near_pieces(t, 0 if dz == -1 else 1)
                    for core, src in enumerate(pieces):
                        pltpu.make_async_copy(src, dst.at[2 * w.chip(dz) + core], sem).start()
                else:
                    pltpu.make_async_copy(w_ref.at[two, :, c], dst.at[two], sem).start()

        own = [pltpu.make_async_copy(x_ref, xa.at[:, 0], lsem.at[0]),
               pltpu.make_async_copy(xb_ref, xa.at[0, 1], lsem.at[2]),
               pltpu.make_async_copy(q_ref, wg.at[0, :, :, pl.ds(0, pc.qkv)], lsem.at[1])]
        for cp in own:
            cp.start()
        bits = [pl.ds(j * (seq // 2), seq // 2) for j in range(2)]
        for j, (rel, dev, q) in enumerate(((2, x, 0), (1, y, 1), (2, x, 1), (1, y, 0))):
            go(remote(xb_ref.at[bits[q]], xa.at[rel, 1, bits[q]], xs_s.at[j], xs_r.at[rel, q], dev))
        for cp in own:
            cp.wait()

        def norm_into(dst, slot, load_rows, gain_ref):
            def one(i, carry):
                rows = aligned(i * 16, 16, 16)
                val = load_rows(rows, i).astype(F32)
                inv = lax.rsqrt(jnp.mean(val * val, axis=-1, keepdims=True) + NORM_EPS)
                dst[slot, rows, :] = (val * inv * gain_ref[...]).astype(BF16)
                return carry
            lax.fori_loop(0, rows_b // 16, one, 0)

        per = seq // 16
        lane = lax.broadcasted_iota(jnp.int32, (seq, LANES), 1)
        low_head = (lane % head_dim) < head_dim // 2
        first_head = lane < head_dim
        n_pair = q4 // LANES
        pair_per_kv = n_pair // 2

        def rope(t):
            swapped = jnp.where(low_head, pltpu.roll(t, LANES - head_dim // 2, 1), pltpu.roll(t, head_dim // 2, 1))
            return t * cos_ref[...] + swapped * sin_ref[...]

        def attend(base, h):
            norm_into(mm, 0, lambda rows, i: xa[base + 2 * (i // per), h, aligned((i % per) * 16, 16, 16), :], g1_ref)

            def proj(nt, carry):
                c = aligned(nt * 256, 256, LANES)
                qf[:, c] = jnp.dot(mm[0], wg[0, :, :, c].reshape(width, 256), preferred_element_type=F32)
                return carry
            lax.fori_loop(0, pc.qkv // 256, proj, 0)

            def one_seq(u, carry):
                slot = base + 2 * u
                rows = aligned(u * seq, seq, seq)
                place = pl.ds(h * seq, seq)
                k_f = rope(qf[rows, pl.ds(q4, LANES)])
                v_f = qf[rows, pl.ds(q4 + kv4, LANES)]
                kvb[slot, place, pl.ds(0, LANES)] = k_f.astype(BF16)
                kvb[slot, place, pl.ds(LANES, LANES)] = v_f.astype(BF16)
                k_r, v_r = pltpu.roll(k_f, head_dim, 1), pltpu.roll(v_f, head_dim, 1)
                zero = jnp.zeros_like(k_f)
                row = lax.broadcasted_iota(jnp.int32, (pair_per_kv * seq, seq), 0) % seq
                causal = row >= lax.broadcasted_iota(jnp.int32, (pair_per_kv * seq, seq), 1)
                for g in range(2):
                    k_lo, k_hi = (k_f, k_r) if g == 0 else (k_r, k_f)
                    v_lo, v_hi = (v_f, v_r) if g == 0 else (v_r, v_f)
                    kk = jnp.concatenate([jnp.where(first_head, k_lo, zero), jnp.where(first_head, zero, k_hi)], axis=0).astype(BF16)
                    vv = jnp.concatenate([jnp.where(first_head, v_lo, zero), jnp.where(first_head, zero, v_hi)], axis=0).astype(BF16)
                    qs = jnp.concatenate([rope(qf[rows, pl.ds((g * pair_per_kv + p) * LANES, LANES)]).astype(BF16) for p in range(pair_per_kv)], axis=0)
                    sc = lax.dot_general(qs, kk, (((1,), (1,)), ((), ())), preferred_element_type=F32) * (head_dim ** -0.5)
                    probs = []
                    for e in range(2):
                        part = jnp.where(causal, sc[:, e * seq:(e + 1) * seq], -jnp.inf)
                        part = jnp.exp(part - jnp.max(part, axis=-1, keepdims=True))
                        probs.append((part / jnp.sum(part, axis=-1, keepdims=True)).astype(BF16))
                    ctx = jnp.dot(jnp.concatenate(probs, axis=1), vv, preferred_element_type=F32).astype(BF16)
                    for p in range(pair_per_kv):
                        lanes = aligned(w.me * pc.w4 + (g * pair_per_kv + p) * LANES, LANES, LANES)
                        ca[slot, place, lanes] = ctx[p * seq:(p + 1) * seq]
                return carry
            lax.fori_loop(0, 2, one_seq, 0)

        whole = pl.ds(0, rows_b)

        def spread(buf, slot, ss, rs, rows=whole, idx=()):
            mine = buf.at[slot, rows, cols[0]]
            go(remote(mine, buf.at[slot ^ 2, rows, cols[0]], ss.at[(slot,) + idx + (1,)], rs.at[(slot ^ 2,) + idx + (1,)], x))
            go(remote(mine, buf.at[slot ^ 1, rows, cols[0]], ss.at[(slot,) + idx + (0,)], rs.at[(slot ^ 1,) + idx + (0,)], y))

        def take(buf, slot, q, rs, rows=whole, idx=()):
            arrived(buf.at[slot, rows, cols[q]], rs.at[(slot,) + idx + (q - 1 if q < 3 else 2,)])

        def relay(buf, slot, q, ss, rs, rows=whole, idx=()):
            take(buf, slot, q, rs, rows, idx)
            ref = buf.at[slot, rows, cols[q]]
            to, dev = (slot ^ 1, y) if q == 2 else (slot ^ 2, x)
            go(remote(ref, buf.at[to, rows, cols[q]], ss.at[(to,) + idx + (2,)], rs.at[(to,) + idx + (2,)], dev))

        def send_kv(slot):
            mine = aligned(w.me * kv4, kv4, LANES)
            for core in range(2):
                for j, dst in enumerate((k_ref, v_ref)):
                    src = kvb.at[slot, pl.ds(core * seq, seq), pl.ds(j * kv4, kv4)]
                    if slot == 0 and core == 0:
                        cp = pltpu.make_async_copy(src, dst.at[:, mine], kv_s.at[slot, core, j])
                        cp.start()
                        local_kv.append(cp)
                    else:
                        go(remote(src, dst.at[:, mine], kv_s.at[slot, core, j], kv_r.at[slot, j], w.square(slot, core)))
        local_kv = []

        def here(slot, q):
            arrived(xa.at[slot, 1, bits[q]], xs_r.at[slot, q])

        seqs = [pl.ds(h * seq, seq) for h in range(2)]

        def send_ctx(base, h):
            for slot in (base, base + 2):
                spread(ca, slot, cs_s, cs_r, seqs[h], (h,))

        def relay_ctx(q, h):
            for slot in ((2, 0) if q == 2 else (0, 2)):
                relay(ca, slot, q, cs_s, cs_r, seqs[h], (h,))

        attend(0, 0)
        send_ctx(0, 0)
        here(2, 0)
        go(remote(xa.at[2, 1, bits[0]], xa.at[3, 1, bits[0]], xs_s.at[4], xs_r.at[3, 0], y))
        here(1, 1)
        go(remote(xa.at[1, 1, bits[1]], xa.at[3, 1, bits[1]], xs_s.at[5], xs_r.at[3, 1], x))
        attend(1, 0)
        send_ctx(1, 0)
        relay_ctx(2, 0)
        here(2, 1)
        attend(0, 1)
        send_ctx(0, 1)
        relay_ctx(1, 0)
        for slot, q in ((1, 0), (3, 0), (3, 1)):
            here(slot, q)
        attend(1, 1)
        send_ctx(1, 1)
        relay_ctx(2, 1)
        relay_ctx(1, 1)
        load(1, wd.at[0], lsem.at[0])
        for slot in range(4):
            send_kv(slot)
        arrived(wd.at[0], lsem.at[0])
        n_ctx = len(sent)

        def mid(slot):
            for q in (1, 2, 3):
                if q == 3 or slot in (1, 3):
                    for h in range(2):
                        take(ca, slot, q, cs_r, seqs[h], (h,))

            def one(nt, carry):
                c = aligned(nt * 256, 256, LANES)
                o = aligned(w.me * pc.w4 + nt * 256, 256, LANES)
                got = jnp.dot(ca[slot], wd[0, :, :, c].reshape(width, 256), preferred_element_type=F32)
                res = xa[slot, :, :, o].reshape(rows_b, 256).astype(F32)
                xm[slot, :, o] = (res + got).astype(BF16)
                return carry
            lax.fori_loop(0, pc.w4 // 256, one, 0)
            spread(xm, slot, ms_s, ms_r)

        mid(3)
        mid(1)
        mid(2)
        relay(xm, 1, 2, ms_s, ms_r)
        mid(0)
        relay(xm, 3, 2, ms_s, ms_r)
        relay(xm, 3, 1, ms_s, ms_r)
        relay(xm, 1, 1, ms_s, ms_r)
        for cp in sent[:n_ctx]:
            cp.wait_send()
        del sent[:n_ctx]
        gate_w = pc.gu_w // 2
        at = {0: 0, 2: 1, 1: 2, 3: 3}

        def gate_up(group, b):
            def one(nt, carry):
                act = h2[pl.ds(2 * group, 2)].reshape(2 * rows_b, width)
                gate = jnp.dot(act, wg[b % 2, :, :, aligned(nt * 256, 256, LANES)].reshape(width, 256), preferred_element_type=F32)
                up = jnp.dot(act, wg[b % 2, :, :, aligned(gate_w + nt * 256, 256, LANES)].reshape(width, 256), preferred_element_type=F32)
                val = (jax.nn.silu(gate) * up).astype(BF16)
                mm[pl.ds(2 * group, 2), :, aligned(b * gate_w + nt * 256, 256, LANES)] = val.reshape(2, rows_b, 256)
                return carry
            lax.fori_loop(0, gate_w // 256, one, 0)

        def load_gate(b):
            load(2 + b, wg.at[b % 2], lsem.at[1 + b % 2])

        def gate_here(b):
            arrived(wg.at[b % 2], lsem.at[1 + b % 2])

        def normed(group):
            for slot in ((0, 2), (1, 3))[group]:
                for q in (1, 2, 3):
                    if q == 3 or slot in (0, 2):
                        take(xm, slot, q, ms_r)
                norm_into(h2, at[slot], lambda rows, i: xm[slot, rows, :], g2_ref)

        load_gate(0)
        normed(0)
        gate_here(0)
        gate_up(0, 0)
        load_gate(1)
        normed(1)
        gate_up(1, 0)
        load_gate(2)
        gate_here(1)
        gate_up(0, 1)
        gate_up(1, 1)
        gate_here(2)
        gate_up(0, 2)
        gate_up(1, 2)
        load_gate(3)
        gate_here(3)
        gate_up(0, 3)
        gate_up(1, 3)

        h0, h1 = pl.ds(0, half), pl.ds(half, half)
        first_sends, home = {}, []

        def phase1(n):
            for old in first_sends.get(n - 2, ()):
                old.wait_send()
            par = n % 2
            arrived(wd.at[par, :, :, pl.ds(0, pc.dn_w)], lsem.at[3 + par])

            def one(j, carry):
                s, nt = j // (pc.dn_w // 256), j % (pc.dn_w // 256)
                c = aligned(nt * 256, 256, LANES)
                act = mm[pl.ds(2 * s, 2)].reshape(2 * rows_b, mm.shape[2])
                got = jnp.dot(act, wd[par, :, :, c].reshape(mm.shape[2], 256), preferred_element_type=F32)
                pp[par, pl.ds(2 * s, 2), :, c] = got.reshape(2, rows_b, 256)
                return carry
            lax.fori_loop(0, 2 * (pc.dn_w // 256), one, 0)
            first_sends[n] = []
            for path, dev, cc, rels in ((0, x, h0, (2, 3)), (1, y, h1, (1, 3))):
                for j, rel in enumerate(rels):
                    cp = remote(pp.at[par, at[rel], :, cc], r1.at[n, path, j], p1_s.at[n, path, j], p1_r.at[n, path, j], dev)
                    cp.start()
                    first_sends[n].append(cp)

        def phase2(n):
            par = n % 2
            for path, dev, cc, rel in ((0, y, h0, 1), (1, x, h1, 2)):
                arrived(r1.at[n, path, 1], p1_r.at[n, path, 1])
                r1[n, path, 1] = pp[par, at[rel], :, cc] + r1[n, path, 1]
                go(remote(r1.at[n, path, 1], r2.at[n, path], p2_s.at[n, path], p2_r.at[n, path], dev))
            for path, cc in ((0, h0), (1, h1)):
                arrived(r1.at[n, path, 0], p1_r.at[n, path, 0])
                r1[n, path, 0] = pp[par, 0, :, cc] + r1[n, path, 0]

        def phase3(n):
            for path in range(2):
                arrived(r2.at[n, path], p2_r.at[n, path])
                c = pl.ds(n * pc.dn_w + path * half, half)
                total = xm[0, :, c].astype(F32) + (r1[n, path, 0] + r2[n, path])
                xm[0, :, c] = total.astype(BF16)
            c = pl.ds(n * pc.dn_w, pc.dn_w)
            go(remote(xm.at[0, pl.ds(seq, seq), c], out_ref.at[:, c], o_s.at[n], o_r.at[n], w.partner()))
            cp = pltpu.make_async_copy(xm.at[0, pl.ds(0, seq), c], out_ref.at[:, c], o_l.at[n])
            cp.start()
            home.append(cp)

        for cp in sent:
            cp.wait_send()
        sent.clear()
        def load_down(n):
            load(last_gu + 1 + n, wd.at[n % 2, :, :, pl.ds(0, pc.dn_w)], lsem.at[3 + n % 2])

        load_down(0)
        last = pc.n_dn - 1
        for n in range(pc.n_dn):
            phase1(n)
            if n >= 1:
                phase2(n - 1)
            if n >= 2:
                phase3(n - 2)
            if n < last:
                load_down(n + 1)
        phase2(last)
        phase3(last - 1)
        phase3(last)

        for cp in sent:
            cp.wait_send()
        for n in (last - 1, last):
            for cp in first_sends[n]:
                cp.wait_send()
        for cp in local_kv + home:
            cp.wait()
        for rel in (1, 2, 3):
            arrived(k_ref.at[:, pl.ds(0, kv4)], kv_r.at[rel, 0])
            arrived(v_ref.at[:, pl.ds(0, kv4)], kv_r.at[rel, 1])

    pl.when(w.c == 1)(stream)
    pl.when(w.c == 0)(compute)


def layer(side, pc, head_dim, x, xb, q_all, near, g1, g2, cos_tab, sin_tab):
    _, seq, width = x.shape
    rows_b = 2 * seq
    kv_width = 4 * pc.kv4
    n_chunk = len(pc.chunks)
    far = pc.n_fsdp // 4
    ff4 = pc.f4 * pc.n_fsdp
    half = pc.dn_w // 2
    hbm = pl.BlockSpec(memory_space=pl.ANY)
    vmem = pl.BlockSpec(memory_space=pltpu.VMEM)
    dma = pltpu.SemaphoreType.DMA
    return pl.pallas_call(
        functools.partial(layer_kernel, side, pc, head_dim),
        out_shape=(
            jax.ShapeDtypeStruct((seq, width), BF16),
            jax.ShapeDtypeStruct((seq, kv_width), BF16),
            jax.ShapeDtypeStruct((seq, kv_width), BF16),
            jax.ShapeDtypeStruct((pc.n_fsdp, pc.rows, pc.late), BF16)),
        in_specs=[hbm] * (3 + len(near)) + [vmem, vmem, vmem, vmem],
        out_specs=(hbm, hbm, hbm, hbm),
        scratch_shapes=[
            pltpu.VMEM((4, 2, seq, width), BF16),
            pltpu.VMEM((4, rows_b, width), BF16),
            pltpu.VMEM((4, rows_b, width), BF16),
            pltpu.VMEM((2, pc.n_fsdp, pc.rows, pc.gu_w), BF16),
            pltpu.VMEM((2, pc.n_fsdp, pc.rows, pc.w4), BF16),
            pltpu.VMEM((4, rows_b, max(ff4, width)), BF16),
            pltpu.VMEM((2, 4, rows_b, pc.dn_w), F32),
            pltpu.VMEM((pc.n_dn, 2, 2, rows_b, half), F32),
            pltpu.VMEM((pc.n_dn, 2, rows_b, half), F32),
            pltpu.VMEM((rows_b, pc.qkv), F32),
            pltpu.VMEM((4, rows_b, 2 * pc.kv4), BF16),
            dma((5,)),
            dma((6,)), dma((4, 2)),
            dma((4, 2, 3)), dma((4, 2, 3)),
            dma((4, 3)), dma((4, 3)),
            dma((4, 2, 2)), dma((4, 2)),
            dma((pc.n_dn, 2, 2)), dma((pc.n_dn, 2, 2)),
            dma((pc.n_dn, 2)), dma((pc.n_dn, 2)),
            dma((pc.n_dn,)), dma((pc.n_dn,)), dma((pc.n_dn,)),
            dma((n_chunk, 2, far + 1)), dma((n_chunk, 2, far + 1)), dma((n_chunk, 2, far + 1)), dma((n_chunk,)),
        ],
        compiler_params=pltpu.CompilerParams(collective_id=2, has_side_effects=True, vmem_limit_bytes=67043328),
        name='layer',
    )(x, xb, q_all, *near, g1, g2, cos_tab, sin_tab)


def solution(mesh):
    batch_axes = ('dp', 'fsdp')
    row_spec = P('fsdp', None)
    n_dp = mesh.shape['dp']
    n_fsdp = mesh.shape['fsdp']
    side = math.isqrt(n_dp)

    def device_step(tokens, embed_table, norm_attn, w_qkv, w_out, norm_mlp, w_gate_up, w_down, rope_scale):
        seq = tokens.shape[1]
        shard_rows, width = embed_table.shape
        head_dim = 2 * rope_scale.shape[0]
        rows = w_out.shape[0]
        q_width = rows * n_fsdp
        kv_width = (w_qkv.shape[1] - q_width) // 2
        pc = Pieces(rows, q_width // 4, kv_width // 4, width // 4, w_down.shape[0] // 4, n_fsdp, width)

        gains = jnp.stack([norm_attn, norm_mlp]).astype(F32)
        ids, gains, pe, pd = gather_ids(side, pc, tokens, gains, w_qkv, w_out, w_gate_up, w_down)
        def first_hop(piece, dz):
            return lax.ppermute(piece, 'fsdp', [(i, (i + 2 * dz) % n_fsdp) for i in range(n_fsdp)])

        f0, f1 = first_hop(pe, 1), first_hop(pe, -1)
        ids = ids.reshape(-1) - lax.axis_index('fsdp') * shard_rows
        owned = (ids >= 0) & (ids < shard_rows)
        table_rows = gather_table(ids, owned, embed_table)
        g1 = gains[:, 0].reshape(1, width)
        g2 = gains[:, 1].reshape(1, width)

        freq_expo = jnp.arange(head_dim // 2, dtype=F32) * (2.0 / head_dim)
        inv_freq = 1.0 / (rope_scale * jnp.power(ROPE_THETA, freq_expo))
        angles = jnp.arange(seq, dtype=F32)[:, None] * inv_freq[None, :]
        cos_tab, sin_tab = jnp.cos(angles), jnp.sin(angles)
        reps = LANES // head_dim
        cos_tab = jnp.concatenate([cos_tab, cos_tab] * reps, axis=1)
        sin_tab = jnp.concatenate([-sin_tab, sin_tab] * reps, axis=1)

        table_rows = table_rows.reshape(n_fsdp // 2, 2, seq, width)
        x, xb, q_all, te, td, tf = embed(side, pc, table_rows, pe, pd, f0, f1)
        out, k, v, _ = layer(side, pc, head_dim, x, xb, q_all, (pe, pd, f0, f1, te, td, tf), g1, g2, cos_tab, sin_tab)
        heads = (1, seq, kv_width // head_dim, head_dim)
        return out[None], k.reshape(heads), v.reshape(heads)

    return jax.shard_map(
        device_step,
        mesh=mesh,
        in_specs=(P(batch_axes, None), row_spec, P('fsdp'), row_spec, row_spec, P('fsdp'), row_spec, row_spec, P(None)),
        out_specs=(P(batch_axes, None, None), P(batch_axes, None, None, None), P(batch_axes, None, None, None)),
        check_vma=False,
    )
```

```python
import functools
import math

import jax
import jax.numpy as jnp
from jax import lax
from jax.experimental import pallas as pl
from jax.experimental.pallas import tpu as pltpu
from jax.sharding import PartitionSpec as P

NORM_EPS = 1e-5
ROPE_THETA = 10000.0
PICK = 32
DEPTH = 4
LANES = 128
MESH = pl.DeviceIdType.MESH
BF16 = jnp.bfloat16
F32 = jnp.float32


def aligned(start, size, step):
    return pl.ds(pl.multiple_of(start, step), size)


class Where:
    def __init__(self, side, n_fsdp):
        self.side = side
        self.nz = n_fsdp // 2
        self.dp = lax.axis_index('dp')
        self.f = lax.axis_index('fsdp')
        self.z = self.f // 2
        self.c = self.f % 2
        self.px = self.dp // side
        self.py = self.dp % side
        self.me = 2 * (self.px % 2) + self.py % 2

    def chip(self, dz):
        return lax.rem(self.z + dz + self.nz, self.nz)

    def along_z(self, dz, core):
        return (self.dp, 2 * self.chip(dz) + core)

    def partner(self):
        return (self.dp, 2 * self.z + 1 - self.c)

    def square(self, rel, core):
        px = self.px + (1 - 2 * (self.px % 2)) if rel & 2 else self.px
        py = self.py + (1 - 2 * (self.py % 2)) if rel & 1 else self.py
        return (px * self.side + py, 2 * self.z + core)


def greet(devices):
    barrier = pltpu.get_barrier_semaphore()
    for dev in devices:
        pl.semaphore_signal(barrier, inc=1, device_id=dev, device_id_type=MESH)
    pl.semaphore_wait(barrier, len(devices))


def remote(src, dst, ssem, rsem, dev):
    return pltpu.make_async_remote_copy(src_ref=src, dst_ref=dst, send_sem=ssem, recv_sem=rsem, device_id=dev, device_id_type=MESH)


def arrived(ref, sem):
    pltpu.make_async_copy(ref, ref, sem).wait()


def ids_kernel(side, pc, tok_ref, gain_ref, w_qkv, w_out, w_gu, w_dn, ids_ref, gains_ref, pe_ref, pd_ref,
               pk, lsem, ssem, rsem, pack_sem, store_sem):
    n_fsdp = pc.n_fsdp
    w = Where(side, n_fsdp)
    pack_copies(pc, w.me, pk, w_qkv, w_out, w_gu, w_dn, pack_sem)
    greet([(w.dp, lax.rem(w.f + k, n_fsdp)) for k in range(1, n_fsdp)])
    own = [pltpu.make_async_copy(tok_ref, ids_ref.at[w.f], lsem.at[0]),
           pltpu.make_async_copy(gain_ref, gains_ref.at[w.f], lsem.at[1])]
    for cp in own:
        cp.start()
    sent = []
    for k in range(1, n_fsdp):
        dev = (w.dp, lax.rem(w.f + k, n_fsdp))
        for j, (src, dst) in enumerate(((tok_ref, ids_ref), (gain_ref, gains_ref))):
            cp = remote(src, dst.at[w.f], ssem.at[j, k], rsem.at[j, k], dev)
            cp.start()
            sent.append(cp)
    arrived(pk, pack_sem)
    lo = 0
    stores = []
    for j, ref in enumerate((pe_ref, pd_ref)):
        stores.append(pltpu.make_async_copy(pk.at[:, pl.ds(lo, ref.shape[1])], ref, store_sem.at[j]))
        stores[-1].start()
        lo += ref.shape[1]
    for cp in own + stores:
        cp.wait()
    for cp in sent:
        cp.wait_send()
    for k in range(1, n_fsdp):
        src = lax.rem(w.f - k + n_fsdp, n_fsdp)
        arrived(ids_ref.at[src], rsem.at[0, k])
        arrived(gains_ref.at[src], rsem.at[1, k])


class Pieces:
    def __init__(self, rows, q4, kv4, w4, f4, n_fsdp, width):
        self.rows = rows
        self.q4, self.kv4, self.w4, self.f4 = q4, kv4, w4, f4
        self.n_fsdp = n_fsdp
        self.width = width
        self.qkv = q4 + 2 * kv4
        self.gu0 = self.qkv + w4
        self.gu_w = 2 * f4 * n_fsdp // 4
        self.dn0 = self.gu0 + 4 * self.gu_w
        self.n_dn = 8
        self.dn_w = width // self.n_dn
        self.total = self.dn0 + width
        self.late = self.total - self.qkv
        self.chunks = [(0, self.qkv), (self.qkv, w4)]
        self.chunks += [(self.gu0 + b * self.gu_w, self.gu_w) for b in range(4)]
        self.chunks += [(self.dn0 + n * self.dn_w, self.dn_w) for n in range(self.n_dn)]
        self.early = 6


def pack_copies(pc, me, pk, w_qkv, w_out, w_gu, w_dn, sem):
    q4, kv4, w4, f4 = pc.q4, pc.kv4, pc.w4, pc.f4
    first = [
        (w_qkv.at[:, aligned(me * q4, q4, LANES)], pk.at[:, pl.ds(0, q4)]),
        (w_qkv.at[:, aligned(4 * q4 + me * kv4, kv4, LANES)], pk.at[:, pl.ds(q4, kv4)]),
        (w_qkv.at[:, aligned(4 * q4 + 4 * kv4 + me * kv4, kv4, LANES)], pk.at[:, pl.ds(q4 + kv4, kv4)]),
    ]
    for src, dst in first:
        pltpu.make_async_copy(src, dst, sem).start()
    pltpu.make_async_copy(w_out.at[:, aligned(me * w4, w4, LANES)], pk.at[:, pl.ds(pc.qkv, w4)], sem).start()
    ff = 4 * f4 * pc.n_fsdp
    for d in range(pc.n_fsdp):
        b, k = d // 4, d % 4
        for part in range(2):
            src = w_gu.at[:, aligned(part * ff + d * 4 * f4 + me * f4, f4, LANES)]
            dst = pk.at[:, pl.ds(pc.gu0 + b * pc.gu_w + part * (pc.gu_w // 2) + k * f4, f4)]
            pltpu.make_async_copy(src, dst, sem).start()
    pltpu.make_async_copy(w_dn.at[aligned(me * f4, f4, LANES), :], pk.at[:, pl.ds(pc.dn0, pc.width)], sem).start()


def gather_ids(side, pc, tokens, gains, w_qkv, w_out, w_gu, w_dn):
    n_fsdp = pc.n_fsdp
    vmem, hbm = pl.BlockSpec(memory_space=pltpu.VMEM), pl.BlockSpec(memory_space=pl.ANY)
    dma = pltpu.SemaphoreType.DMA
    return pl.pallas_call(
        functools.partial(ids_kernel, side, pc),
        out_shape=(
            jax.ShapeDtypeStruct((n_fsdp,) + tokens.shape, tokens.dtype),
            jax.ShapeDtypeStruct((n_fsdp,) + gains.shape, gains.dtype),
            jax.ShapeDtypeStruct((pc.rows, pc.dn0), BF16),
            jax.ShapeDtypeStruct((pc.rows, pc.width), BF16)),
        in_specs=[vmem, vmem, hbm, hbm, hbm, hbm],
        out_specs=(vmem, vmem, hbm, hbm),
        scratch_shapes=[pltpu.VMEM((pc.rows, pc.total), BF16), dma((2,)), dma((2, n_fsdp)), dma((2, n_fsdp)), dma, dma((2,))],
        compiler_params=pltpu.CompilerParams(collective_id=0, has_side_effects=True),
        name='ids',
    )(tokens, gains, w_qkv, w_out, w_gu, w_dn)


def gather_kernel(n_tok, gid_ref, tgt_ref, table_ref, out_ref, buf, sems):
    width = table_ref.shape[2]
    n_step = n_tok // PICK

    def fetch(step, slot):
        for i in range(PICK):
            pltpu.make_async_copy(table_ref.at[gid_ref[step * PICK + i]], buf.at[slot, i], sems.at[slot]).start()

    for j in range(DEPTH - 1):
        fetch(j, j)

    def body(step, carry):
        slot = lax.rem(step, DEPTH)

        @pl.when(step + DEPTH - 1 < n_step)
        def _():
            fetch(step + DEPTH - 1, lax.rem(step + DEPTH - 1, DEPTH))
        arrived(buf.at[slot], sems.at[slot])
        rows = aligned(step * PICK, PICK, PICK)
        hot = (lax.broadcasted_iota(jnp.int32, (PICK, PICK * 8), 1) == tgt_ref[rows, :]).astype(BF16)
        got = jnp.dot(hot, buf[slot].reshape(PICK * 8, width), preferred_element_type=F32)
        out_ref[rows, :] = got.astype(BF16)
        return carry
    lax.fori_loop(0, n_step, body, 0)


def gather_table(ids, owned, table):
    n_tok = ids.shape[0]
    n_rows, width = table.shape
    gid = jnp.where(owned, ids // 8, jnp.arange(n_tok, dtype=jnp.int32) % (n_rows // 8))
    place = jnp.arange(n_tok, dtype=jnp.int32) % PICK
    tgt = jnp.where(owned, 8 * place + ids % 8, -1)[:, None]
    return pl.pallas_call(
        functools.partial(gather_kernel, n_tok),
        out_shape=jax.ShapeDtypeStruct((n_tok, width), BF16),
        in_specs=[pl.BlockSpec(memory_space=pltpu.SMEM), pl.BlockSpec(memory_space=pltpu.VMEM), pl.BlockSpec(memory_space=pl.ANY)],
        out_specs=pl.BlockSpec(memory_space=pltpu.VMEM),
        scratch_shapes=[pltpu.VMEM((DEPTH, PICK, 8, width), BF16), pltpu.SemaphoreType.DMA((DEPTH,))],
        compiler_params=pltpu.CompilerParams(vmem_limit_bytes=48 * 2**20),
        cost_estimate=pl.CostEstimate(flops=80 * 10**9, bytes_accessed=9 * n_tok * width * 2, transcendentals=0),
        name='rows',
    )(gid, tgt, table.reshape(n_rows // 8, 8, width))


def embed_kernel(side, pc, rows_ref, pe_ref, pd_ref, f0_ref, f1_ref, xa_ref, xb_ref, q_ref, te_ref, td_ref, tf_ref,
                 got, peer, rp, sb, pk, xo,
                 got_sem, pack_sem, own_sem, d2d_s, d2d_r, f_s, f_r, push_s, push_r,
                 peer_s, peer_r, rs_s, rs_r, home_sem, x_s, x_r):
    n_fsdp = pc.n_fsdp
    w = Where(side, n_fsdp)
    nz = w.nz
    far = nz // 2
    seq = got.shape[2]
    hw = got.shape[3]
    width = 2 * hw
    order = [far]
    for o in range(far - 1, 0, -1):
        order += [o, -o]
    order += [0]
    mine = aligned(w.c * hw, hw, LANES)
    other = aligned((1 - w.c) * hw, hw, LANES)
    for k in range(len(order)):
        dest = w.chip(order[k])
        pltpu.make_async_copy(rows_ref.at[dest, :, :, mine], got.at[dest], got_sem.at[k]).start()
    q_srcs = [ref.at[:, pl.ds(0, pc.qkv)] for ref in (pe_ref, f0_ref, f1_ref)]
    for j, src in enumerate(q_srcs):
        pltpu.make_async_copy(src, pk.at[j], pack_sem.at[j]).start()
    greet([w.partner()] + [w.along_z(dz, core) for dz in (1, -1) for core in (0, 1)] + [w.square(rel, core) for rel in (1, 2) for core in (0, 1)])
    dirs = (1, -1)

    for k in range(len(order)):
        dest = w.chip(order[k])
        remote(rows_ref.at[dest, :, :, other], peer.at[dest], peer_s.at[k], peer_r.at[k], w.partner()).start()

    here_q = (2 * w.z + w.c, 2 * w.chip(-1) + w.c, 2 * w.chip(1) + w.c)
    swaps = [(src, q_ref.at[here_q[j]]) for j, src in enumerate(q_srcs)]
    rest = pl.ds(pc.qkv, pc.dn0 - pc.qkv)
    swaps += [(pe_ref.at[:, rest], te_ref), (pd_ref, td_ref), (f0_ref.at[:, rest], tf_ref.at[0]), (f1_ref.at[:, rest], tf_ref.at[1])]
    own = [remote(src, dst, d2d_s.at[j], d2d_r.at[j], w.partner()) for j, (src, dst) in enumerate(swaps)]


    def pair(dz):
        return q_ref.at[pl.ds(2 * w.chip(dz), 2)]

    def single(dz, i):
        return q_ref.at[pl.ds(2 * w.chip(dz) + i, 1)]

    def push(ref, i, h):
        remote(ref, ref, push_s.at[i, h], push_r, w.partner()).start()

    local = []

    def forward(h):
        @pl.when(w.c == 1)
        def _():
            for i, dz in enumerate(dirs):
                if h == 1:
                    local[1 + i].wait()
                    own[1 + i].wait_recv()
                elif h < far:
                    arrived(pair(-dz * h), f_r.at[i, h])
                else:
                    arrived(single(-dz * h, i), f_r.at[i, h])
                if h < far - 1:
                    remote(pair(-dz * h), pair(-dz * h), f_s.at[i, h + 1], f_r.at[i, h + 1], w.along_z(dz, 1)).start()
                elif h == far - 1:
                    remote(single(-dz * h, i), single(-dz * h, i), f_s.at[i, h + 1], f_r.at[i, h + 1], w.along_z(dz, 1)).start()
                if h > 1:
                    push(pair(-dz * h) if h < far else single(-dz * h, i), i, h)

    def addto(dst, terms, q):
        def one(r, carry):
            rows = aligned(q * (seq // 2) + r * 32, 32, 32)
            val = terms[0](rows)
            for term in terms[1:]:
                val = val + term(rows)
            dst(rows, val)
            return carry
        lax.fori_loop(0, seq // 64, one, 0)

    def part(ref, q):
        return ref.at[pl.ds(q * (seq // 2), seq // 2)]

    def rs_stage(k, h):
        o = order[k]
        dest = w.chip(o)
        if h == 0:
            arrived(got.at[dest], got_sem.at[k])
            arrived(peer.at[dest], peer_r.at[k])
        if o == 0:
            return
        dist = abs(o)
        for i, dz in enumerate(dirs):
            if (o * dz < 0 and o != far) or (dist == far and h != i):
                continue
            for q in range(2):
                terms = [lambda r: got[dest, h, r, :], lambda r: peer[dest, h, r, :]]
                if dist < far - 1 or (dist == far - 1 and h == i):
                    arrived(part(rp.at[i, dist, h], q), rs_r.at[i, dist, h, q])
                    terms.append(lambda r, i=i: rp[i, dist, h, r, :])

                def put(r, val, i=i):
                    sb[i, dist - 1, h, r, :] = val
                addto(put, terms, q)
                remote(part(sb.at[i, dist - 1, h], q), part(rp.at[i, dist - 1, h], q), rs_s.at[i, dist - 1, h, q],
                       rs_r.at[i, dist - 1, h, q], w.along_z(dz, w.c)).start()

    def finish(h):
        for q in range(2):
            terms = [lambda r: got[w.z, h, r, :], lambda r: peer[w.z, h, r, :]]
            for i in range(2):
                arrived(part(rp.at[i, 0, h], q), rs_r.at[i, 0, h, q])
                terms.append(lambda r, i=i: rp[i, 0, h, r, :])

            def put(r, val):
                xo[h, r, :] = val
            addto(put, terms, q)
        dst = (xa_ref.at[0] if h == 0 else xb_ref).at[:, mine]

        @pl.when(w.c == 0)
        def _():
            pltpu.make_async_copy(xo.at[h], dst, home_sem.at[h]).start()

        @pl.when(w.c == 1)
        def _():
            remote(xo.at[h], dst, home_sem.at[h], x_r.at[0, h], w.partner()).start()

    sides = ((2, w.square(2, 0)), (1, w.square(1, 0)))
    spread = [remote(xo.at[0], xa_ref.at[rel, :, mine], x_s.at[j], x_r.at[rel, w.c], dev) for j, (rel, dev) in enumerate(sides)]
    col = [pl.ds(j * hw, hw) for j in range(2)]
    relay = [remote(xa_ref.at[rel, :, col[j]], xa_ref.at[3, :, col[j]], x_s.at[2 + j], x_r.at[3, j], sides[1 - j][1]) for j, (rel, _) in enumerate(sides)]

    for j in range(3):
        arrived(pk.at[j], pack_sem.at[j])
        local.append(pltpu.make_async_copy(pk.at[j], q_ref.at[here_q[j]], own_sem.at[j]))
    last = len(order) - 1
    for k in range(last + 1):
        rs_stage(k, 0)
        if k == 0:
            for cp in own[:3] + local:
                cp.start()
        if k == 2:
            for cp in own[3:]:
                cp.start()
            forward(1)
        if k == 5:
            forward(2)
    for k in range(3):
        rs_stage(k, 1)
    finish(0)
    for cp in spread:
        cp.start()
    for k in range(3, last + 1):
        rs_stage(k, 1)
        if k == 4:
            forward(3)
        if k == last - 1:
            @pl.when(w.c == 0)
            def _():
                for j, (rel, _) in enumerate(sides):
                    arrived(xa_ref.at[rel, :, col[j]], x_r.at[rel, j])
                    relay[j].start()
    forward(4)
    finish(1)

    for cp in own[:1] + own[3:]:
        cp.wait()
    for cp in own[1:3]:
        cp.wait_send()
    local[0].wait()
    for cp in spread:
        cp.wait_send()
    for k in range(len(order)):
        dest = w.chip(order[k])
        arrived(peer.at[dest], peer_s.at[k])
    for i in range(2):
        for dist in range(1, far + 1):
            for h in ((i,) if dist == far else (0, 1)):
                for q in range(2):
                    arrived(part(sb.at[i, dist - 1, h], q), rs_s.at[i, dist - 1, h, q])

    @pl.when(w.c == 1)
    def _():
        for i, dz in enumerate(dirs):
            for h in range(1, far + 1):
                ref = pair(-dz * h) if h < far else single(-dz * h, i)
                if h > 1:
                    arrived(ref, push_s.at[i, h])
                if h < far:
                    arrived(pair(-dz * h) if h < far - 1 else single(-dz * h, i), f_s.at[i, h + 1])

    @pl.when(w.c == 0)
    def _():
        arrived(q_ref.at[pl.ds(0, n_fsdp - 6)], push_r)
        for j in (1, 2):
            local[j].wait()
            own[j].wait_recv()
        arrived(xa_ref.at[0, :, col[1]], x_r.at[0, 0])
        arrived(xb_ref.at[:, col[1]], x_r.at[0, 1])
        arrived(xa_ref.at[2, :, col[1]], x_r.at[2, 1])
        arrived(xa_ref.at[1, :, col[0]], x_r.at[1, 0])
        for j in range(2):
            arrived(xa_ref.at[3, :, col[j]], x_r.at[3, j])
            relay[j].wait_send()
    for h in range(2):
        arrived(xo.at[h], home_sem.at[h])


def embed(side, pc, rows, pe, pd, f0, f1):
    seq, width = rows.shape[2], rows.shape[3]
    nz = pc.n_fsdp // 2
    far = nz // 2
    hbm = pl.BlockSpec(memory_space=pl.ANY)
    dma = pltpu.SemaphoreType.DMA
    return pl.pallas_call(
        functools.partial(embed_kernel, side, pc),
        out_shape=(
            jax.ShapeDtypeStruct((4, seq, width), BF16),
            jax.ShapeDtypeStruct((seq, width), BF16),
            jax.ShapeDtypeStruct((pc.n_fsdp, pc.rows, pc.qkv), BF16),
            jax.ShapeDtypeStruct((pc.rows, pc.dn0 - pc.qkv), BF16),
            jax.ShapeDtypeStruct(pd.shape, BF16),
            jax.ShapeDtypeStruct((2, pc.rows, pc.dn0 - pc.qkv), BF16)),
        in_specs=[hbm] * 5,
        out_specs=(hbm,) * 6,
        scratch_shapes=[
            pltpu.VMEM((nz, 2, seq, width // 2), BF16),
            pltpu.VMEM((nz, 2, seq, width // 2), BF16),
            pltpu.VMEM((2, far, 2, seq, width // 2), BF16),
            pltpu.VMEM((2, far, 2, seq, width // 2), BF16),
            pltpu.VMEM((3, pc.rows, pc.qkv), BF16),
            pltpu.VMEM((2, seq, width // 2), BF16),
            dma((nz,)), dma((3,)), dma((3,)), dma((7,)), dma((7,)),
            dma((2, far + 1)), dma((2, far + 1)), dma((2, far + 1)), dma,
            dma((nz,)), dma((nz,)),
            dma((2, far, 2, 2)), dma((2, far, 2, 2)),
            dma((2,)), dma((4,)), dma((4, 2)),
        ],
        compiler_params=pltpu.CompilerParams(collective_id=1, has_side_effects=True, vmem_limit_bytes=67043328),
        name='embed',
    )(rows, pe, pd, f0, f1)


def layer_kernel(side, pc, head_dim, x_ref, xb_ref, q_ref, pe_ref, pd_ref, f0_ref, f1_ref, te_ref, td_ref, tf_ref, g1_ref, g2_ref, cos_ref, sin_ref, out_ref, k_ref, v_ref, w_ref,
                 xa, ca, xm, wg, wd, mm, pp, r1, r2, qf, kvb,
                 lsem, xs_s, xs_r, cs_s, cs_r, ms_s, ms_r, kv_s, kv_r, p1_s, p1_r, p2_s, p2_r, o_s, o_l, o_r,
                 zs, zr, ps, wch):
    h2 = ca
    n_fsdp = pc.n_fsdp
    w = Where(side, n_fsdp)
    far = w.nz // 2
    seq, width = xa.shape[2], xa.shape[3]
    rows_b = 2 * seq
    half = pc.dn_w // 2
    n_chunk = len(pc.chunks)
    last_gu = 5
    greet([w.partner(), w.along_z(1, w.c), w.along_z(-1, w.c)] + [w.square(rel, core) for rel in (1, 2, 3) for core in (0, 1)])
    dirs = (1, -1)

    def slim(t, mine):
        off, cw = pc.chunks[t]
        return pl.ds(off - pc.dn0 if t >= pc.early else off - (0 if mine else pc.qkv), cw)

    def own_pieces(t):
        refs = (pe_ref, te_ref) if t < pc.early else (pd_ref, td_ref)
        return [refs[0].at[:, slim(t, True)], refs[1].at[:, slim(t, False)]]

    def near_pieces(t, i):
        return [(f0_ref, f1_ref)[i].at[:, slim(t, True)], tf_ref.at[i, :, slim(t, False)]]

    def stream():
        def cols(t):
            off, cw = pc.chunks[t]
            return pl.ds(off - pc.qkv, cw)

        def pair(t, dz):
            return w_ref.at[pl.ds(2 * w.chip(dz), 2), :, cols(t)]

        def single(t, dz, i):
            return w_ref.at[pl.ds(2 * w.chip(dz) + i, 1), :, cols(t)]

        def piece(t, h, i):
            dz = dirs[i]
            return pair(t, -dz * h) if h < far else single(t, -dz * h, i)

        sent = []

        def hop(t, h):
            if t < 1 or t >= n_chunk or (h == 0 and t < pc.early):
                return
            ready = h == 1 and t < pc.early
            for i in range(2):
                dz = dirs[i]
                if h > 0 and not ready:
                    arrived(piece(t, h, i), zr.at[t, i, h])
                if h == far:
                    continue
                ref = pair(t, -dz * h) if h < far - 1 else single(t, -dz * h, i)
                sems = (zs.at[t, i, h], zr.at[t, i, h + 1], w.along_z(dz, 1))
                if h == 0 or ready:
                    pieces = near_pieces(t, i) if ready else own_pieces(t)
                    for src, core in zip(pieces, (1, 0)):
                        remote(src, w_ref.at[2 * w.chip(-dz * h) + core, :, cols(t)], *sems).start()
                else:
                    remote(ref, ref, *sems).start()
                sent.append((ref, zs.at[t, i, h]))
            if h > 0 and not ready:
                for i in range(2):
                    ref = piece(t, h, i)
                    remote(ref, ref, ps.at[t, i, h], wch.at[t], w.partner()).start()
                    sent.append((ref, ps.at[t, i, h]))

        for s in range(n_chunk + far):
            for h in range(far, -1, -1):
                hop(s - h if h > 1 else s + 1 - h, h)
        for ref, sem in sent:
            arrived(ref, sem)
        kvw = 2 * (kvb.shape[2] // 4)
        for rel in range(4):
            arrived(k_ref.at[:, pl.ds(0, kvw)], kv_r.at[rel, 0])
            arrived(v_ref.at[:, pl.ds(0, kvw)], kv_r.at[rel, 1])
        for n in range(pc.n_dn):
            arrived(out_ref.at[:, pl.ds(n * pc.dn_w, pc.dn_w)], o_r.at[n])

    def compute():
        y, x = w.square(1, 0), w.square(2, 0)
        q4, kv4 = pc.q4, pc.kv4
        cols = {q: aligned((w.me ^ q) * pc.w4, pc.w4, LANES) for q in range(4)}
        sent = []

        def go(cp):
            cp.start()
            sent.append(cp)

        def load(t, dst, sem, first=True):
            off, cw = pc.chunks[t]
            c = pl.ds(off - pc.qkv, cw)
            near = t < pc.early
            if first:
                arrived(w_ref.at[pl.ds(0, n_fsdp - (6 if near else 2)), :, c], wch.at[t])
            for dz in range(-1, w.nz - 1):
                two = pl.ds(2 * w.chip(dz), 2)
                if dz == 0 or (near and dz in (1, -1)):
                    pieces = own_pieces(t) if dz == 0 else near_pieces(t, 0 if dz == -1 else 1)
                    for core, src in enumerate(pieces):
                        pltpu.make_async_copy(src, dst.at[2 * w.chip(dz) + core], sem).start()
                else:
                    pltpu.make_async_copy(w_ref.at[two, :, c], dst.at[two], sem).start()

        own = [pltpu.make_async_copy(x_ref, xa.at[:, 0], lsem.at[0]),
               pltpu.make_async_copy(xb_ref, xa.at[0, 1], lsem.at[2]),
               pltpu.make_async_copy(q_ref, wg.at[0, :, :, pl.ds(0, pc.qkv)], lsem.at[1])]
        for cp in own:
            cp.start()
        bits = [pl.ds(j * (seq // 2), seq // 2) for j in range(2)]
        for j, (rel, dev, q) in enumerate(((2, x, 0), (1, y, 1), (2, x, 1), (1, y, 0))):
            go(remote(xb_ref.at[bits[q]], xa.at[rel, 1, bits[q]], xs_s.at[j], xs_r.at[rel, q], dev))
        for cp in own:
            cp.wait()

        def norm_into(dst, slot, load_rows, gain_ref):
            def one(i, carry):
                rows = aligned(i * 16, 16, 16)
                val = load_rows(rows, i).astype(F32)
                inv = lax.rsqrt(jnp.mean(val * val, axis=-1, keepdims=True) + NORM_EPS)
                dst[slot, rows, :] = (val * inv * gain_ref[...]).astype(BF16)
                return carry
            lax.fori_loop(0, rows_b // 16, one, 0)

        per = seq // 16
        lane = lax.broadcasted_iota(jnp.int32, (seq, LANES), 1)
        low_head = (lane % head_dim) < head_dim // 2
        first_head = lane < head_dim
        n_pair = q4 // LANES
        pair_per_kv = n_pair // 2

        def rope(t):
            swapped = jnp.where(low_head, pltpu.roll(t, LANES - head_dim // 2, 1), pltpu.roll(t, head_dim // 2, 1))
            return t * cos_ref[...] + swapped * sin_ref[...]

        def attend(base, h):
            norm_into(mm, 0, lambda rows, i: xa[base + 2 * (i // per), h, aligned((i % per) * 16, 16, 16), :], g1_ref)

            def proj(nt, carry):
                c = aligned(nt * 256, 256, LANES)
                qf[:, c] = jnp.dot(mm[0], wg[0, :, :, c].reshape(width, 256), preferred_element_type=F32)
                return carry
            lax.fori_loop(0, pc.qkv // 256, proj, 0)

            def one_seq(u, carry):
                slot = base + 2 * u
                rows = aligned(u * seq, seq, seq)
                place = pl.ds(h * seq, seq)
                k_f = rope(qf[rows, pl.ds(q4, LANES)])
                v_f = qf[rows, pl.ds(q4 + kv4, LANES)]
                kvb[slot, place, pl.ds(0, LANES)] = k_f.astype(BF16)
                kvb[slot, place, pl.ds(LANES, LANES)] = v_f.astype(BF16)
                k_r, v_r = pltpu.roll(k_f, head_dim, 1), pltpu.roll(v_f, head_dim, 1)
                zero = jnp.zeros_like(k_f)
                row = lax.broadcasted_iota(jnp.int32, (pair_per_kv * seq, seq), 0) % seq
                causal = row >= lax.broadcasted_iota(jnp.int32, (pair_per_kv * seq, seq), 1)
                for g in range(2):
                    k_lo, k_hi = (k_f, k_r) if g == 0 else (k_r, k_f)
                    v_lo, v_hi = (v_f, v_r) if g == 0 else (v_r, v_f)
                    kk = jnp.concatenate([jnp.where(first_head, k_lo, zero), jnp.where(first_head, zero, k_hi)], axis=0).astype(BF16)
                    vv = jnp.concatenate([jnp.where(first_head, v_lo, zero), jnp.where(first_head, zero, v_hi)], axis=0).astype(BF16)
                    qs = jnp.concatenate([rope(qf[rows, pl.ds((g * pair_per_kv + p) * LANES, LANES)]).astype(BF16) for p in range(pair_per_kv)], axis=0)
                    sc = lax.dot_general(qs, kk, (((1,), (1,)), ((), ())), preferred_element_type=F32) * (head_dim ** -0.5)
                    probs = []
                    for e in range(2):
                        part = jnp.where(causal, sc[:, e * seq:(e + 1) * seq], -jnp.inf)
                        part = jnp.exp(part - jnp.max(part, axis=-1, keepdims=True))
                        probs.append((part / jnp.sum(part, axis=-1, keepdims=True)).astype(BF16))
                    ctx = jnp.dot(jnp.concatenate(probs, axis=1), vv, preferred_element_type=F32).astype(BF16)
                    for p in range(pair_per_kv):
                        lanes = aligned(w.me * pc.w4 + (g * pair_per_kv + p) * LANES, LANES, LANES)
                        ca[slot, place, lanes] = ctx[p * seq:(p + 1) * seq]
                return carry
            lax.fori_loop(0, 2, one_seq, 0)

        whole = pl.ds(0, rows_b)

        def spread(buf, slot, ss, rs, rows=whole, idx=()):
            mine = buf.at[slot, rows, cols[0]]
            go(remote(mine, buf.at[slot ^ 2, rows, cols[0]], ss.at[(slot,) + idx + (1,)], rs.at[(slot ^ 2,) + idx + (1,)], x))
            go(remote(mine, buf.at[slot ^ 1, rows, cols[0]], ss.at[(slot,) + idx + (0,)], rs.at[(slot ^ 1,) + idx + (0,)], y))

        def take(buf, slot, q, rs, rows=whole, idx=()):
            arrived(buf.at[slot, rows, cols[q]], rs.at[(slot,) + idx + (q - 1 if q < 3 else 2,)])

        def relay(buf, slot, q, ss, rs, rows=whole, idx=()):
            take(buf, slot, q, rs, rows, idx)
            ref = buf.at[slot, rows, cols[q]]
            to, dev = (slot ^ 1, y) if q == 2 else (slot ^ 2, x)
            go(remote(ref, buf.at[to, rows, cols[q]], ss.at[(to,) + idx + (2,)], rs.at[(to,) + idx + (2,)], dev))

        def send_kv(slot):
            mine = aligned(w.me * kv4, kv4, LANES)
            for core in range(2):
                for j, dst in enumerate((k_ref, v_ref)):
                    src = kvb.at[slot, pl.ds(core * seq, seq), pl.ds(j * kv4, kv4)]
                    if slot == 0 and core == 0:
                        cp = pltpu.make_async_copy(src, dst.at[:, mine], kv_s.at[slot, core, j])
                        cp.start()
                        local_kv.append(cp)
                    else:
                        go(remote(src, dst.at[:, mine], kv_s.at[slot, core, j], kv_r.at[slot, j], w.square(slot, core)))
        local_kv = []

        def here(slot, q):
            arrived(xa.at[slot, 1, bits[q]], xs_r.at[slot, q])

        seqs = [pl.ds(h * seq, seq) for h in range(2)]

        def send_ctx(base, h):
            for slot in (base, base + 2):
                spread(ca, slot, cs_s, cs_r, seqs[h], (h,))

        def relay_ctx(q, h):
            for slot in ((2, 0) if q == 2 else (0, 2)):
                relay(ca, slot, q, cs_s, cs_r, seqs[h], (h,))

        def mid(slot, h):
            for q in (1, 2, 3):
                if q == 3 or slot in (1, 3):
                    take(ca, slot, q, cs_r, seqs[h], (h,))

            def one(nt, carry):
                c = aligned(nt * 256, 256, LANES)
                o = aligned(w.me * pc.w4 + nt * 256, 256, LANES)
                got = jnp.dot(ca[slot, seqs[h], :], wd[0, :, :, c].reshape(width, 256), preferred_element_type=F32)
                xm[slot, seqs[h], o] = (xa[slot, h, :, o].astype(F32) + got).astype(BF16)
                return carry
            lax.fori_loop(0, pc.w4 // 256, one, 0)
            spread(xm, slot, ms_s, ms_r, seqs[h], (h,))

        def relay_mid(slot, q, h):
            relay(xm, slot, q, ms_s, ms_r, seqs[h], (h,))

        attend(0, 0)
        send_ctx(0, 0)
        here(2, 0)
        go(remote(xa.at[2, 1, bits[0]], xa.at[3, 1, bits[0]], xs_s.at[4], xs_r.at[3, 0], y))
        here(1, 1)
        go(remote(xa.at[1, 1, bits[1]], xa.at[3, 1, bits[1]], xs_s.at[5], xs_r.at[3, 1], x))
        attend(1, 0)
        send_ctx(1, 0)
        relay_ctx(2, 0)
        here(2, 1)
        attend(0, 1)
        send_ctx(0, 1)
        relay_ctx(1, 0)
        for slot, q in ((1, 0), (3, 0), (3, 1)):
            here(slot, q)
        attend(1, 1)
        send_ctx(1, 1)
        relay_ctx(2, 1)
        load(1, wd.at[0], lsem.at[0])
        arrived(wd.at[0], lsem.at[0])
        for slot in (3, 1, 2, 0):
            mid(slot, 0)
        relay_ctx(1, 1)
        for slot in range(4):
            send_kv(slot)
        n_ctx = len(sent)

        mid(3, 1)
        mid(1, 1)
        for slot, q in ((1, 2), (3, 2), (3, 1), (1, 1)):
            relay_mid(slot, q, 0)
        mid(2, 1)
        mid(0, 1)
        for slot, q in ((1, 2), (3, 2), (3, 1), (1, 1)):
            relay_mid(slot, q, 1)
        for cp in sent[:n_ctx]:
            cp.wait_send()
        del sent[:n_ctx]
        gate_w = pc.gu_w // 2
        at = {0: 0, 2: 1, 1: 2, 3: 3}

        def gate_up(group, b):
            def one(nt, carry):
                act = h2[pl.ds(2 * group, 2)].reshape(2 * rows_b, width)
                gate = jnp.dot(act, wg[b % 2, :, :, aligned(nt * 256, 256, LANES)].reshape(width, 256), preferred_element_type=F32)
                up = jnp.dot(act, wg[b % 2, :, :, aligned(gate_w + nt * 256, 256, LANES)].reshape(width, 256), preferred_element_type=F32)
                val = (jax.nn.silu(gate) * up).astype(BF16)
                mm[pl.ds(2 * group, 2), :, aligned(b * gate_w + nt * 256, 256, LANES)] = val.reshape(2, rows_b, 256)
                return carry
            lax.fori_loop(0, gate_w // 256, one, 0)

        def load_gate(b):
            load(2 + b, wg.at[b % 2], lsem.at[1 + b % 2])

        def gate_here(b):
            arrived(wg.at[b % 2], lsem.at[1 + b % 2])

        def normed(group):
            for slot in ((0, 2), (1, 3))[group]:
                for q in (1, 2, 3):
                    if q == 3 or slot in (0, 2):
                        for h in range(2):
                            take(xm, slot, q, ms_r, seqs[h], (h,))
                norm_into(h2, at[slot], lambda rows, i: xm[slot, rows, :], g2_ref)

        load_gate(0)
        normed(0)
        gate_here(0)
        gate_up(0, 0)
        load_gate(1)
        normed(1)
        gate_up(1, 0)
        load_gate(2)
        gate_here(1)
        gate_up(0, 1)
        gate_up(1, 1)
        gate_here(2)
        gate_up(0, 2)
        gate_up(1, 2)
        load_gate(3)
        gate_here(3)
        gate_up(0, 3)
        gate_up(1, 3)

        h0, h1 = pl.ds(0, half), pl.ds(half, half)
        first_sends, home = {}, []

        def phase1(n):
            for old in first_sends.get(n - 2, ()):
                old.wait_send()
            par = n % 2
            arrived(wd.at[par, :, :, pl.ds(0, pc.dn_w)], lsem.at[3 + par])

            def one(j, carry):
                s, nt = j // (pc.dn_w // 256), j % (pc.dn_w // 256)
                c = aligned(nt * 256, 256, LANES)
                act = mm[pl.ds(2 * s, 2)].reshape(2 * rows_b, mm.shape[2])
                got = jnp.dot(act, wd[par, :, :, c].reshape(mm.shape[2], 256), preferred_element_type=F32)
                pp[par, pl.ds(2 * s, 2), :, c] = got.reshape(2, rows_b, 256)
                return carry
            lax.fori_loop(0, 2 * (pc.dn_w // 256), one, 0)
            first_sends[n] = []
            for path, dev, cc, rels in ((0, x, h0, (2, 3)), (1, y, h1, (1, 3))):
                for j, rel in enumerate(rels):
                    cp = remote(pp.at[par, at[rel], :, cc], r1.at[n, path, j], p1_s.at[n, path, j], p1_r.at[n, path, j], dev)
                    cp.start()
                    first_sends[n].append(cp)

        def phase2(n):
            par = n % 2
            for path, dev, cc, rel in ((0, y, h0, 1), (1, x, h1, 2)):
                arrived(r1.at[n, path, 1], p1_r.at[n, path, 1])
                r1[n, path, 1] = pp[par, at[rel], :, cc] + r1[n, path, 1]
                go(remote(r1.at[n, path, 1], r2.at[n, path], p2_s.at[n, path], p2_r.at[n, path], dev))
            for path, cc in ((0, h0), (1, h1)):
                arrived(r1.at[n, path, 0], p1_r.at[n, path, 0])
                r1[n, path, 0] = pp[par, 0, :, cc] + r1[n, path, 0]

        def phase3(n):
            for path in range(2):
                arrived(r2.at[n, path], p2_r.at[n, path])
                c = pl.ds(n * pc.dn_w + path * half, half)
                total = xm[0, :, c].astype(F32) + (r1[n, path, 0] + r2[n, path])
                xm[0, :, c] = total.astype(BF16)
            c = pl.ds(n * pc.dn_w, pc.dn_w)
            go(remote(xm.at[0, pl.ds(seq, seq), c], out_ref.at[:, c], o_s.at[n], o_r.at[n], w.partner()))
            cp = pltpu.make_async_copy(xm.at[0, pl.ds(0, seq), c], out_ref.at[:, c], o_l.at[n])
            cp.start()
            home.append(cp)

        for cp in sent:
            cp.wait_send()
        sent.clear()
        def load_down(n):
            load(last_gu + 1 + n, wd.at[n % 2, :, :, pl.ds(0, pc.dn_w)], lsem.at[3 + n % 2])

        load_down(0)
        last = pc.n_dn - 1
        for n in range(pc.n_dn):
            phase1(n)
            if n >= 1:
                phase2(n - 1)
            if n >= 2:
                phase3(n - 2)
            if n < last:
                load_down(n + 1)
        phase2(last)
        phase3(last - 1)
        phase3(last)

        for cp in sent:
            cp.wait_send()
        for n in (last - 1, last):
            for cp in first_sends[n]:
                cp.wait_send()
        for cp in local_kv + home:
            cp.wait()
        for rel in (1, 2, 3):
            arrived(k_ref.at[:, pl.ds(0, kv4)], kv_r.at[rel, 0])
            arrived(v_ref.at[:, pl.ds(0, kv4)], kv_r.at[rel, 1])

    pl.when(w.c == 1)(stream)
    pl.when(w.c == 0)(compute)


def layer(side, pc, head_dim, x, xb, q_all, near, g1, g2, cos_tab, sin_tab):
    _, seq, width = x.shape
    rows_b = 2 * seq
    kv_width = 4 * pc.kv4
    n_chunk = len(pc.chunks)
    far = pc.n_fsdp // 4
    ff4 = pc.f4 * pc.n_fsdp
    half = pc.dn_w // 2
    hbm = pl.BlockSpec(memory_space=pl.ANY)
    vmem = pl.BlockSpec(memory_space=pltpu.VMEM)
    dma = pltpu.SemaphoreType.DMA
    return pl.pallas_call(
        functools.partial(layer_kernel, side, pc, head_dim),
        out_shape=(
            jax.ShapeDtypeStruct((seq, width), BF16),
            jax.ShapeDtypeStruct((seq, kv_width), BF16),
            jax.ShapeDtypeStruct((seq, kv_width), BF16),
            jax.ShapeDtypeStruct((pc.n_fsdp, pc.rows, pc.late), BF16)),
        in_specs=[hbm] * (3 + len(near)) + [vmem, vmem, vmem, vmem],
        out_specs=(hbm, hbm, hbm, hbm),
        scratch_shapes=[
            pltpu.VMEM((4, 2, seq, width), BF16),
            pltpu.VMEM((4, rows_b, width), BF16),
            pltpu.VMEM((4, rows_b, width), BF16),
            pltpu.VMEM((2, pc.n_fsdp, pc.rows, pc.gu_w), BF16),
            pltpu.VMEM((2, pc.n_fsdp, pc.rows, pc.w4), BF16),
            pltpu.VMEM((4, rows_b, max(ff4, width)), BF16),
            pltpu.VMEM((2, 4, rows_b, pc.dn_w), F32),
            pltpu.VMEM((pc.n_dn, 2, 2, rows_b, half), F32),
            pltpu.VMEM((pc.n_dn, 2, rows_b, half), F32),
            pltpu.VMEM((rows_b, pc.qkv), F32),
            pltpu.VMEM((4, rows_b, 2 * pc.kv4), BF16),
            dma((5,)),
            dma((6,)), dma((4, 2)),
            dma((4, 2, 3)), dma((4, 2, 3)),
            dma((4, 2, 3)), dma((4, 2, 3)),
            dma((4, 2, 2)), dma((4, 2)),
            dma((pc.n_dn, 2, 2)), dma((pc.n_dn, 2, 2)),
            dma((pc.n_dn, 2)), dma((pc.n_dn, 2)),
            dma((pc.n_dn,)), dma((pc.n_dn,)), dma((pc.n_dn,)),
            dma((n_chunk, 2, far + 1)), dma((n_chunk, 2, far + 1)), dma((n_chunk, 2, far + 1)), dma((n_chunk,)),
        ],
        compiler_params=pltpu.CompilerParams(collective_id=2, has_side_effects=True, vmem_limit_bytes=67043328),
        name='layer',
    )(x, xb, q_all, *near, g1, g2, cos_tab, sin_tab)


def solution(mesh):
    batch_axes = ('dp', 'fsdp')
    row_spec = P('fsdp', None)
    n_dp = mesh.shape['dp']
    n_fsdp = mesh.shape['fsdp']
    side = math.isqrt(n_dp)

    def device_step(tokens, embed_table, norm_attn, w_qkv, w_out, norm_mlp, w_gate_up, w_down, rope_scale):
        seq = tokens.shape[1]
        shard_rows, width = embed_table.shape
        head_dim = 2 * rope_scale.shape[0]
        rows = w_out.shape[0]
        q_width = rows * n_fsdp
        kv_width = (w_qkv.shape[1] - q_width) // 2
        pc = Pieces(rows, q_width // 4, kv_width // 4, width // 4, w_down.shape[0] // 4, n_fsdp, width)

        gains = jnp.stack([norm_attn, norm_mlp]).astype(F32)
        ids, gains, pe, pd = gather_ids(side, pc, tokens, gains, w_qkv, w_out, w_gate_up, w_down)
        def first_hop(piece, dz):
            return lax.ppermute(piece, 'fsdp', [(i, (i + 2 * dz) % n_fsdp) for i in range(n_fsdp)])

        f0, f1 = first_hop(pe, 1), first_hop(pe, -1)
        ids = ids.reshape(-1) - lax.axis_index('fsdp') * shard_rows
        owned = (ids >= 0) & (ids < shard_rows)
        table_rows = gather_table(ids, owned, embed_table)
        g1 = gains[:, 0].reshape(1, width)
        g2 = gains[:, 1].reshape(1, width)

        freq_expo = jnp.arange(head_dim // 2, dtype=F32) * (2.0 / head_dim)
        inv_freq = 1.0 / (rope_scale * jnp.power(ROPE_THETA, freq_expo))
        angles = jnp.arange(seq, dtype=F32)[:, None] * inv_freq[None, :]
        cos_tab, sin_tab = jnp.cos(angles), jnp.sin(angles)
        reps = LANES // head_dim
        cos_tab = jnp.concatenate([cos_tab, cos_tab] * reps, axis=1)
        sin_tab = jnp.concatenate([-sin_tab, sin_tab] * reps, axis=1)

        table_rows = table_rows.reshape(n_fsdp // 2, 2, seq, width)
        x, xb, q_all, te, td, tf = embed(side, pc, table_rows, pe, pd, f0, f1)
        out, k, v, _ = layer(side, pc, head_dim, x, xb, q_all, (pe, pd, f0, f1, te, td, tf), g1, g2, cos_tab, sin_tab)
        heads = (1, seq, kv_width // head_dim, head_dim)
        return out[None], k.reshape(heads), v.reshape(heads)

    return jax.shard_map(
        device_step,
        mesh=mesh,
        in_specs=(P(batch_axes, None), row_spec, P('fsdp'), row_spec, row_spec, P('fsdp'), row_spec, row_spec, P(None)),
        out_specs=(P(batch_axes, None, None), P(batch_axes, None, None, None), P(batch_axes, None, None, None)),
        check_vma=False,
    )
```
